32 devices in a mesh: wall: 8 (over y, x, core), span: 4 (over z).
Axes of the slice: x: 2, y: 2, z: 4, core: 2. Of those that a mesh axis runs over, the one named last changes fastest.
Arguments:
- velocity_old: float32 [3, 128, 64, 128], P(None, 'wall', 'span'), may hold values from -12 to 12, as said below
- heights: float32 [16], replicated, may hold values from 0.04 to 0.25
- owner_device: int32 [16384, 1], P(('wall', 'span')), may hold values from 0 to 7, as said below
- owner_element: int32 [16384, 1], P(('wall', 'span')), may hold values from 0 to 63, as said below
- ref_coords: float32 [3, 16384], P(None, ('wall', 'span')), may hold values from -1 to 1
- roughness: float32 [16384], P(('wall', 'span')), may hold values from 0.0001 to 0.01
Outputs:
- velocity_new: float32 [3, 128, 64, 128], P(None, 'wall', 'span')
- neumann: float32 [2, 16384], P(None, ('wall', 'span'))
The draws below stay inside these ranges and needn't reach their ends.
Inputs may be any that keep to these rules, and one draw needn't show every extreme that they name: `velocity_old`: values at coinciding nodes of neighbouring elements are equal. `owner_device`: the owner is the streamwise index w of the point's own device, or w + 1 or w - 1 modulo 8. Among the rows of one device at most 128 name w + 1 and at most 128 name w - 1; some device has exactly 128 for w + 1 and some device exactly 128 for w - 1. `owner_element`: the element index is (ex * 2 + ez) * 16 + ey with ex = i // 8 and ez = j // 8 of the wall point; ey < 2 for points of the first wall, ey >= 14 for the second.
All inputs are finite; a program needn't handle non-finite values.
Results may differ from the reference program's by a relative error of at most 0.0003.
Values sent between devices are 32-bit elements; how exact they have to be, the bound alone decides.
A program may use at most 128 MiB of HBM per device.

```python
import math
import jax
import jax.numpy as jnp
import numpy as np
from jax import lax

ORDER = 7
QN = 8
EXD = 2
EZD = 2
EY = 16
NEAR = 2
ITERS = 3
XLOC = 16
ZLOC = 16
YNODES = 128
XNODES = 128
ZNODES = 64
P_DEV = 512
WALLPTS = 16384
CAP = 128
N_WALL = 8
N_SPAN = 4
DEVICES = 32


def draw_velocity_old(key, part):
    unique_x = XNODES // QN * ORDER
    unique_z = ZNODES // QN * ORDER
    unique_y = EY * ORDER + 1
    index_x = (jnp.arange(XNODES) // QN * ORDER + jnp.arange(XNODES) % QN) % unique_x
    index_z = (jnp.arange(ZNODES) // QN * ORDER + jnp.arange(ZNODES) % QN) % unique_z
    index_y = jnp.arange(YNODES) // QN * ORDER + jnp.arange(YNODES) % QN
    shape_grid = (3, unique_x, unique_z, unique_y)
    values_grid = jax.random.truncated_normal(key, -4.0, 4.0, shape_grid, jnp.float32)
    rising = jnp.exp(jnp.log(3.0) * jnp.arange(unique_x, dtype=jnp.float32) / unique_x)
    values_grid = values_grid * rising[None, :, None, None]
    values_grid = jnp.take(values_grid, index_x, axis=1)
    values_grid = jnp.take(values_grid, index_z, axis=2)
    return jnp.take(values_grid, index_y, axis=3)


def draw_owner_device(key, part):
    block_keys = jax.random.split(jax.random.fold_in(key, 21), DEVICES)
    ranks = jax.vmap(lambda single: jax.random.permutation(single, P_DEV))(block_keys).astype(jnp.int32)
    blocks = jnp.arange(DEVICES, dtype=jnp.int32)
    count_next = jax.random.randint(jax.random.fold_in(key, 22), (DEVICES,), CAP // 3, CAP + 1)
    count_prev = jax.random.randint(jax.random.fold_in(key, 23), (DEVICES,), CAP // 3, CAP + 1)
    full_next = jax.random.randint(jax.random.fold_in(key, 24), (), 0, DEVICES)
    full_prev = jax.random.randint(jax.random.fold_in(key, 25), (), 0, DEVICES)
    count_next = jnp.where(blocks == full_next, CAP, count_next)
    count_prev = jnp.where(blocks == full_prev, CAP, count_prev)
    offset = jnp.where(ranks < count_next[:, None], 1, jnp.where(ranks < (count_next + count_prev)[:, None], -1, 0))
    own_wall = (blocks // N_SPAN)[:, None]
    owner = (own_wall + offset + N_WALL) % N_WALL
    return owner.astype(jnp.int32).reshape(WALLPTS, 1)


def draw_owner_element(key, part):
    position = jnp.arange(WALLPTS, dtype=jnp.int32) % P_DEV
    side_flag = position // (P_DEV // 2)
    node_i = position // ZLOC % XLOC
    node_j = position % ZLOC
    elem_x = node_i // QN
    elem_z = node_j // QN
    layer = jax.random.randint(jax.random.fold_in(key, 13), (WALLPTS,), 0, NEAR)
    elem_y = jnp.where(side_flag == 1, EY - 1 - layer, layer)
    return ((elem_x * EZD + elem_z) * EY + elem_y).astype(jnp.int32).reshape(WALLPTS, 1)


def levels(rng, shape, cuts, low, high):
    level = 1.0
    for axis_at, parts in cuts:
        steps = jax.random.uniform(jax.random.fold_in(jax.random.fold_in(rng, 6), axis_at), (parts,), jnp.float32, low / len(cuts), high / len(cuts))
        level = level * jnp.repeat(jnp.exp(steps), shape[axis_at] // parts).reshape((-1,) + (1,) * (len(shape) - 1 - axis_at))
    return level


def setup_inputs(seed: int = 0) -> dict:
    keys = jax.random.split(jax.random.key(seed), 7)
    return {
        "velocity_old": draw_velocity_old(jax.random.fold_in(keys[6], 71), 0),
        "heights": jnp.clip(jnp.exp(jax.random.uniform(keys[1], (EY,), jnp.float32, math.log(0.04), math.log(0.25))), 0.04, 0.25),
        "owner_device": draw_owner_device(jax.random.fold_in(keys[6], 71), 0),
        "owner_element": draw_owner_element(jax.random.fold_in(keys[6], 71), 0),
        "ref_coords": jnp.clip(jax.random.uniform(keys[4], (3, WALLPTS), jnp.float32, -1.0, 1.0) * levels(keys[4], (3, WALLPTS), ((1, 32),), -0.4, 0.0), -1.0, 1.0),
        "roughness": jnp.clip(jnp.exp(math.log(0.01) - 4.6051702 * jax.random.uniform(keys[5], (WALLPTS,), jnp.float32) ** levels(keys[5], (WALLPTS,), ((0, 32),), -0.2, 0.2)), 0.0001, 0.01),
    }


GLL_NODES = (-1.0, -0.8717401485096066, -0.5917001814331423, -0.2092992179024789, 0.2092992179024789, 0.5917001814331423, 0.8717401485096066, 1.0)
GLL_WEIGHTS = (0.03571428571428571, 0.2107042271435061, 0.3411226924835044, 0.4124587946587038, 0.4124587946587038, 0.3411226924835044, 0.2107042271435061, 0.03571428571428571)
viscosity = 0.02
inverse_step = 20.0
karman = 0.41
sample_height = 0.1
speed_floor = 0.01
element_dx = 0.05
element_dz = 0.13
precise = lax.Precision.HIGHEST

def stiffness_table():
    points = np.array(GLL_NODES)
    weights = np.array(GLL_WEIGHTS)
    previous = np.ones(8)
    current = points.copy()
    for degree in range(1, 7):
        previous, current = (current, ((2 * degree + 1) * points * current - degree * previous) / (degree + 1))
    derivative = np.zeros((8, 8))
    for target in range(8):
        for source in range(8):
            if target != source:
                derivative[target, source] = current[target] / current[source] / (points[target] - points[source])
    derivative[0, 0] = -14.0
    derivative[7, 7] = 14.0
    return derivative.T @ (weights[:, None] * derivative)

def lagrange(coord):
    points = np.array(GLL_NODES)
    gaps_table = points[:, None] - points[None, :] + np.eye(8)
    scale_row = jnp.asarray(1.0 / np.prod(gaps_table, axis=1), jnp.float32)
    gaps = coord[:, None] - jnp.asarray(points, jnp.float32)[None, :]
    filled = jnp.where(jnp.asarray(np.eye(8) > 0.5)[None], jnp.float32(1.0), gaps[:, None, :])
    return jnp.prod(filled, axis=2) * scale_row[None, :]

def face_weights(length, open_ends):
    values = np.ones(length)
    position = np.arange(length) % 8
    values[(position == 0) | (position == 7)] = 0.5
    if open_ends:
        values[0] = 1.0
        values[-1] = 1.0
    return values

def join_faces(core, before, after, axis):
    count = core.shape[axis] // 8
    blocks = core.reshape(core.shape[:axis] + (count, 8) + core.shape[axis + 1:])
    first = lax.slice_in_dim(blocks, 0, 1, axis=axis + 1)
    last = lax.slice_in_dim(blocks, 7, 8, axis=axis + 1)
    before_b = jnp.expand_dims(before, axis + 1)
    after_b = jnp.expand_dims(after, axis + 1)
    prev_last = jnp.concatenate([before_b, lax.slice_in_dim(last, 0, count - 1, axis=axis)], axis)
    next_first = jnp.concatenate([lax.slice_in_dim(first, 1, count, axis=axis), after_b], axis)
    middle = lax.slice_in_dim(blocks, 1, 7, axis=axis + 1)
    joined = jnp.concatenate([first + prev_last, middle, last + next_first], axis + 1)
    return joined.reshape(core.shape)

def assemble(field):
    joined_x = join_faces(field, field[:, -1:], field[:, :1], 1)
    joined_z = join_faces(joined_x, joined_x[:, :, -1:], joined_x[:, :, :1], 2)
    border = jnp.zeros(joined_z.shape[:3] + (1,), jnp.float32)
    return join_faces(joined_z, border, border, 3)

def reference(velocity_old, heights, owner_device, owner_element, ref_coords, roughness):
    weights = np.array(GLL_WEIGHTS)
    stiffness = jnp.asarray(stiffness_table(), jnp.float32)
    length_x, length_z, length_y = (velocity_old.shape[1], velocity_old.shape[2], velocity_old.shape[3])
    count_x, count_z, count_y = (length_x // 8, length_z // 8, length_y // 8)
    mass_x = jnp.asarray(np.tile(0.5 * element_dx * weights, count_x), jnp.float32)
    mass_z = jnp.asarray(np.tile(0.5 * element_dz * weights, count_z), jnp.float32)
    mass_y = (0.5 * heights[:, None] * jnp.asarray(weights, jnp.float32)[None, :]).reshape(length_y)
    mass_all = mass_x[:, None, None] * mass_z[None, :, None] * mass_y[None, None, :]
    inverse_count = jnp.asarray(face_weights(length_x, False)[:, None, None] * face_weights(length_z, False)[None, :, None] * face_weights(length_y, True)[None, None, :], jnp.float32)
    blocks = (2.0 / heights)[:, None, None] * stiffness[None]

    def operate(field):
        along_x = jnp.einsum('ab,cebzy->ceazy', stiffness * (2.0 / element_dx), field.reshape(3, count_x, 8, length_z, length_y), precision=precise).reshape(field.shape)
        along_z = jnp.einsum('ab,cxeby->cxeay', stiffness * (2.0 / element_dz), field.reshape(3, length_x, count_z, 8, length_y), precision=precise).reshape(field.shape)
        along_y = jnp.einsum('eab,cxzeb->cxzea', blocks, field.reshape(3, length_x, length_z, count_y, 8), precision=precise).reshape(field.shape)
        mass_xb = mass_x[None, :, None, None]
        mass_zb = mass_z[None, None, :, None]
        mass_yb = mass_y[None, None, None, :]
        local = viscosity * (along_x * mass_zb * mass_yb + mass_xb * along_z * mass_yb + mass_xb * mass_zb * along_y) + inverse_step * mass_all[None] * field
        return assemble(local)
    element_rows = velocity_old.reshape(3, count_x, 8, count_z, 8, count_y, 8).transpose(1, 3, 5, 0, 2, 4, 6).reshape(count_x * count_z * count_y, 3 * 512)
    points = jnp.arange(WALLPTS, dtype=jnp.int32)
    span_index = points // P_DEV % N_SPAN
    local_elem = owner_element[:, 0]
    elem_x = owner_device[:, 0] * EXD + local_elem // (EZD * EY)
    elem_z = span_index * EZD + local_elem // EY % EZD
    elem_y = local_elem % EY
    row_ids = ((elem_x * count_z + elem_z) * count_y + elem_y).astype(jnp.int32)

    def evaluate(pieces):
        rows_here, coords = pieces
        values = element_rows[rows_here].reshape(rows_here.shape[0], 3, 8, 8, 8)
        return jnp.einsum('gcabd,ga,gb,gd->gc', values, lagrange(coords[:, 0]), lagrange(coords[:, 1]), lagrange(coords[:, 2]), precision=precise)
    sampled = lax.map(evaluate, (row_ids.reshape(DEVICES, P_DEV), ref_coords.T.reshape(DEVICES, P_DEV, 3))).reshape(WALLPTS, 3)
    stream = sampled[:, 0]
    spanwise = sampled[:, 2]
    wall_speed = jnp.sqrt(stream * stream + spanwise * spanwise + speed_floor)
    drag_coeff = (karman / jnp.log(sample_height / roughness)) ** 2
    neumann = -(drag_coeff * wall_speed / viscosity)[None, :] * jnp.stack([stream, spanwise])
    traction = (viscosity * neumann).reshape(2, N_WALL, N_SPAN, 2, XLOC, ZLOC).transpose(0, 3, 1, 4, 2, 5).reshape(2, 2, length_x, length_z)
    traction = traction * (mass_x[:, None] * mass_z[None, :])[None, None]
    zero_plane = jnp.zeros((1, length_x, length_z), jnp.float32)
    bottom = jnp.concatenate([traction[0:1, 0], zero_plane, traction[1:2, 0]], axis=0)
    top_wall = jnp.concatenate([traction[0:1, 1], zero_plane, traction[1:2, 1]], axis=0)
    forcing = inverse_step * mass_all[None] * velocity_old
    forcing = forcing.at[:, :, :, 0].add(bottom).at[:, :, :, -1].add(top_wall)
    right_side = assemble(forcing)

    def weighted(first, second):
        return lax.optimization_barrier(jnp.sum(first * second * inverse_count[None], axis=(1, 2, 3)))

    def spread(values):
        return values[:, None, None, None]
    solution = jnp.zeros_like(right_side)
    residual = right_side
    direction = residual
    norm_now = weighted(residual, residual)
    for sweep in range(ITERS):
        applied = operate(direction)
        step_size = norm_now / weighted(direction, applied)
        solution = solution + spread(step_size) * direction
        residual = residual - spread(step_size) * applied
        norm_next = weighted(residual, residual)
        direction = residual + spread(norm_next / norm_now) * direction
        norm_now = norm_next
    return (solution, neumann)
```

```python
import functools

import jax
import jax.numpy as jnp
import numpy as np
from jax import lax
from jax.experimental import pallas as pl
from jax.experimental.pallas import tpu as pltpu
from jax.sharding import PartitionSpec as P

GLL_NODES = (
    -1.0,
    -0.8717401485096066,
    -0.5917001814331423,
    -0.2092992179024789,
    0.2092992179024789,
    0.5917001814331423,
    0.8717401485096066,
    1.0,
)
GLL_WEIGHTS = (
    0.03571428571428571,
    0.2107042271435061,
    0.3411226924835044,
    0.4124587946587038,
    0.4124587946587038,
    0.3411226924835044,
    0.2107042271435061,
    0.03571428571428571,
)
viscosity = 0.02
inverse_step = 20.0
karman = 0.41
sample_height = 0.1
speed_floor = 0.01
element_dx = 0.05
element_dz = 0.13
NEAR = 2
ROUNDS = 2
REACH = 2
TERMS = (
    (0, 0, 0),
    (1, 1, 2),
    (1, 2, 1),
    (2, 2, 2),
    (3, 3, 6),
    (3, 4, 5),
    (3, 5, 4),
    (3, 6, 3),
    (4, 4, 6),
    (4, 6, 4),
    (5, 5, 6),
    (5, 6, 5),
    (6, 6, 6),
)
SINGLE_STAGE = 64
VMEM_LIMIT = 32 * 2**20
MESH = pl.DeviceIdType.MESH
F32 = jnp.float32
BF16 = jnp.bfloat16


def stiffness_table():
    points = np.array(GLL_NODES)
    weights = np.array(GLL_WEIGHTS)
    previous = np.ones(8)
    current = points.copy()
    for degree in range(1, 7):
        previous, current = (
            current,
            ((2 * degree + 1) * points * current - degree * previous) / (degree + 1),
        )
    derivative = np.zeros((8, 8))
    for target in range(8):
        for source in range(8):
            if target != source:
                derivative[target, source] = (
                    current[target] / current[source] / (points[target] - points[source])
                )
    derivative[0, 0] = -14.0
    derivative[7, 7] = 14.0
    return derivative.T @ (weights[:, None] * derivative)


def join_matrix(length):
    joined = np.eye(length)
    for left in range(7, length - 1, 8):
        joined[left, left + 1] = 1.0
        joined[left + 1, left] = 1.0
    return joined


def face_weights(length, open_ends):
    values = np.ones(length)
    position = np.arange(length) % 8
    values[(position == 0) | (position == 7)] = 0.5
    if open_ends:
        values[0] = 1.0
        values[-1] = 1.0
    return values


def split_np(matrix):
    single = jnp.asarray(matrix, F32)
    high = single.astype(BF16)
    low = (jnp.asarray(matrix, F32) - high.astype(F32)).astype(BF16)
    return high, low


def tables(length_x, length_z, length_y):
    weights = np.array(GLL_WEIGHTS)
    stiffness = stiffness_table()
    count_x, count_z, count_y = length_x // 8, length_z // 8, length_y // 8
    mass_x = np.tile(0.5 * element_dx * weights, count_x)
    mass_z = np.tile(0.5 * element_dz * weights, count_z)
    stiff_x = np.kron(np.eye(count_x), stiffness * (2.0 / element_dx))
    stiff_z = np.kron(np.eye(count_z), stiffness * (2.0 / element_dz))
    mass_xz = np.kron(mass_x, mass_z)
    join_xz = np.kron(join_matrix(length_x), join_matrix(length_z))
    join_y = join_matrix(length_y)
    plane = viscosity * (
        np.kron(stiff_x, np.diag(mass_z)) + np.kron(np.diag(mass_x), stiff_z)
    ) + inverse_step * np.diag(mass_xz)
    plane = join_xz @ plane
    mass_plane = join_xz @ np.diag(mass_xz)
    both = np.concatenate([plane, mass_plane], axis=1)
    lines_mass = np.tile(0.5 * weights, count_y)[:, None] * join_y
    lines_stiff = viscosity * 2.0 * (np.kron(np.eye(count_y), stiffness) @ join_y)
    lines = np.stack([lines_mass, lines_stiff])
    ring_x = join_matrix(length_x) @ mass_x
    ring_z = join_matrix(length_z) @ mass_z
    ring_x[0] *= 2.0
    ring_x[-1] *= 2.0
    ring_z[0] *= 2.0
    ring_z[-1] *= 2.0
    assembled = inverse_step * np.kron(ring_x, ring_z)
    inner_x = face_weights(length_x, True)
    inner_z = face_weights(length_z, True)
    outer_x = face_weights(length_x, False)
    outer_z = face_weights(length_z, False)
    weight_y = face_weights(length_y, True)
    columns = np.stack(
        [
            assembled[:, None] * np.ones(length_y)[None],
            np.kron(outer_x, outer_z)[:, None] * weight_y[None],
            np.kron(inner_x, inner_z)[:, None] * weight_y[None],
        ]
    )
    reach = 2 * REACH + 1

    def words(length, mass, stiff, extra):
        size = reach * length
        join = join_matrix(size)
        light = join @ np.diag(np.tile(mass, reach))
        heavy = viscosity * join @ np.kron(np.eye(size // 8), stiff) + extra * light
        chains = [
            light,
            heavy @ light,
            light @ light,
            heavy @ heavy @ light,
            heavy @ light @ light,
            light @ heavy @ light,
            light @ light @ light,
        ]
        middle = REACH * length
        chains = [chain[middle : middle + length] for chain in chains]
        return np.concatenate(chains + [np.zeros((128 - 7 * length, size))], axis=0)

    words_x = words(length_x, mass_x, stiffness * (2.0 / element_dx), 0.0)
    words_z = words(length_z, mass_z, stiffness * (2.0 / element_dz), inverse_step)
    pad = np.zeros((128, 128 - reach * length_z))
    words_z = np.concatenate([words_z, pad], axis=1)
    return both, lines, columns, words_x, words_z


def split(value):
    high = value.astype(BF16)
    low = (value - high.astype(F32)).astype(BF16)
    return high, low


def dot3(left, right, dims):
    def one(a, b):
        return lax.dot_general(a, b, (dims, ((), ())), preferred_element_type=F32)

    return one(left[0], right[0]) + (one(left[0], right[1]) + one(left[1], right[0]))


NN = ((1,), (0,))
NT = ((1,), (1,))
TN = ((0,), (0,))
DIRS = ((1, 1), (1, -1), (-1, 1), (-1, -1))


def lagrange_rows(coord):
    points = np.array(GLL_NODES)
    scale = 1.0 / np.prod(points[:, None] - points[None, :] + np.eye(8), axis=1)
    shape = (8, coord.shape[1])
    node = lax.broadcasted_iota(jnp.int32, shape, 0)
    total = jnp.zeros(shape, F32)
    for a in range(8):
        total = jnp.where(node == a, F32(scale[a]), total)
    for b in range(8):
        total = total * jnp.where(node == b, F32(1.0), coord - F32(points[b]))
    return total


def kernel(
    n_wall,
    n_span,
    sizes,
    vel_in,
    heights_in,
    owner_in,
    element_in,
    coords_in,
    roughness_in,
    plane_hi_in,
    plane_lo_in,
    lines_in,
    columns_in,
    words_x_in,
    words_z_in,
    field,
    factors,
    neumann,
    vel,
    heights,
    owner,
    element,
    coords,
    roughness,
    plane_hi,
    plane_lo,
    lines,
    columns,
    words_x,
    words_z,
    load_sem,
    near,
    near_got,
    local,
    face_send,
    face_got,
    parts,
    sum_send,
    wall_got,
    span_got,
    pull_send,
    pull_got,
    pull_ss,
    pull_rs,
    near_ss,
    near_rs,
    face_ss,
    face_rs,
    wall_ss,
    wall_rs,
    span_ss,
    span_rs,
):
    length_x, length_z, length_y = sizes
    rows = length_x * length_z
    count_z, count_y = length_z // 8, length_y // 8
    w = lax.axis_index("wall")
    s = lax.axis_index("span")

    def at(dx, dz):
        return (lax.rem(w + (dx + n_wall), n_wall), lax.rem(s + (dz + n_span), n_span))

    loads = [
        pltpu.make_async_copy(source, target, load_sem.at[index])
        for index, (source, target) in enumerate(
            (
                (vel_in, vel),
                (heights_in, heights),
                (lines_in, lines),
                (coords_in, coords),
                (owner_in, owner),
                (element_in, element),
                (columns_in, columns),
                (roughness_in, roughness),
                (plane_hi_in, plane_hi),
                (plane_lo_in, plane_lo),
                (words_x_in, words_x),
                (words_z_in, words_z),
            )
        )
    ]
    for load in loads:
        load.start()

    single = n_wall * n_span <= SINGLE_STAGE
    if single:
        greeted = [divmod(k, n_span) for k in range(1, n_wall * n_span)]
    else:
        greeted = [(k, 0) for k in range(1, n_wall)] + [(0, k) for k in range(1, n_span)]
        greeted += sorted(
            {
                ((dx + n_wall) % n_wall, (dz + n_span) % n_span)
                for dx in range(-REACH, REACH + 1)
                for dz in range(-REACH, REACH + 1)
            }
            - {(0, 0)}
            - set(greeted)
        )
    barrier = pltpu.get_barrier_semaphore()
    for dx, dz in greeted:
        pl.semaphore_signal(barrier, inc=1, device_id=at(dx, dz), device_id_type=MESH)

    loads[0].wait()
    lane = lax.broadcasted_iota(jnp.int32, (64, length_y), 1)
    groups = (length_x // 8) * count_z
    for index, comp in enumerate((0, 2)):
        packed = jnp.zeros((64, length_y), F32)
        for group in range(groups):
            ex, ez = group // count_z, group % count_z
            block = vel[comp, pl.ds(ex * 8, 8), pl.ds(ez * 8, 8), :].reshape(64, length_y)
            moved = pltpu.roll(block, (group * 32 + 16) % length_y, 1)
            packed = jnp.where(lane // 32 == group, moved, packed)
        near[index] = packed
    for load in loads[1:]:
        load.wait()

    layer_of = lax.broadcasted_iota(jnp.int32, (length_y, count_y), 0) // 8
    layer = lax.broadcasted_iota(jnp.int32, (length_y, count_y), 1)
    height_row = heights[...]
    height = jnp.sum(jnp.where(layer_of == layer, height_row, 0.0), axis=1, keepdims=True)
    lines_mass = height * lines[0]
    lines_hi, lines_lo = split(jnp.concatenate([lines_mass, lines[1] / height], axis=1))
    bound = jnp.max(0.1535 * height_row + 0.000182 / height_row, axis=1, keepdims=True)
    shifts = (0.15 * bound, 0.85 * bound)

    mass_row = jnp.sum(lines_mass, axis=0, keepdims=True)
    scale = columns[0] * mass_row
    for c in range(3):
        field[0, c] = vel[c].reshape(rows, length_y) * scale

    def remote(src, dst, ss, rs, where):
        return pltpu.make_async_remote_copy(
            src_ref=src,
            dst_ref=dst,
            send_sem=ss,
            recv_sem=rs,
            device_id=where,
            device_id_type=MESH,
        )

    face_rows = []
    for slot, (dx, dz) in enumerate(((1, 0), (-1, 0), (0, 1), (0, -1)) + DIRS):
        size = 3 * (1 if dx and dz else length_z if dx else length_x)
        face_rows.append((sum(entry[1] for entry in face_rows), size, dx, dz))
    face_total = sum(entry[1] for entry in face_rows)

    def corner(dx, dz):
        return (rows - length_z if dx == 1 else 0) + (length_z - 1 if dz == 1 else 0)

    def face_part(slot, c, dx, dz):
        first, size = face_rows[slot][0] + c * (face_rows[slot][1] // 3), face_rows[slot][1] // 3
        if dx and dz:
            rows_of = pl.ds(corner(dx, dz), 1)
        elif dx:
            rows_of = pl.ds(rows - length_z if dx == 1 else 0, length_z)
        else:
            rows_of = pl.ds(length_z - 1 if dz == 1 else 0, length_x, stride=length_z)
        return pl.ds(first, size), rows_of

    def send_faces(turn):
        for c in range(3):
            for slot, (_, _, dx, dz) in enumerate(face_rows):
                packed_rows, rows_of = face_part(slot, c, dx, dz)
                face_send[turn, packed_rows, :] = local[turn, c, rows_of, :]
        if turn == 0:
            pl.semaphore_wait(barrier, len(greeted))
            for copy in near_copies:
                copy.start()
        for first, size, dx, dz in face_rows:
            part = (turn, pl.ds(first, size), slice(None))
            remote(
                face_send.at[part], face_got.at[part], face_ss.at[turn], face_rs.at[turn], at(dx, dz)
            ).start()

    def settle(ss, rs, ref):
        for semaphore in (rs, ss):
            pltpu.make_async_copy(ref, ref, semaphore).wait()

    def add_faces(turn):
        settle(face_ss.at[turn], face_rs.at[turn], face_got.at[turn, pl.ds(0, face_total), :])
        for c in range(3):
            for slot, (_, _, dx, dz) in enumerate(face_rows):
                packed_rows, rows_of = face_part(slot, c, -dx, -dz)
                field[turn + 1, c, rows_of, :] = (
                    field[turn + 1, c, rows_of, :] + face_got[turn, packed_rows, :]
                )

    def inner(quantity, c, product):
        parts[quantity * 8 + c : quantity * 8 + c + 1, :] = jnp.sum(
            product, axis=0, keepdims=True
        )

    def operate(source, target):
        flat = field[source].reshape(3 * rows, length_y)
        lined = dot3(split(flat), (lines_hi, lines_lo), NN)
        wide = jnp.concatenate(
            [
                jnp.concatenate(
                    [
                        lined[c * rows : (c + 1) * rows, :length_y],
                        lined[c * rows : (c + 1) * rows, length_y:],
                    ],
                    axis=0,
                )
                for c in range(3)
            ],
            axis=1,
        )
        result = dot3((plane_hi[...], plane_lo[...]), split(wide), NN)
        for c in range(3):
            local[target, c] = result[:, c * length_y : (c + 1) * length_y]

    slots = {(0, 0): 0, (0, 1): 1, (1, 1): 2, (0, 2): 3, (1, 2): 4, (2, 2): 5}

    def inner_products(newest):
        for c in range(3):
            weighted = field[newest, c] * columns[1]
            for other in range(newest + 1):
                inner(slots[(other, newest)], c, weighted * field[other, c])

    near_copies = []
    for slot, dx in enumerate((1, -1)):
        copy = remote(near, near_got.at[slot], near_ss, near_rs, at(dx, 0))
        near_copies.append(copy)

    operate(0, 0)
    send_faces(0)
    for c in range(3):
        field[1, c] = local[0, c]
    parts[...] = jnp.zeros_like(parts)

    points = owner.shape[1]
    row_x = lagrange_rows(coords[0:1, :])
    row_z = lagrange_rows(coords[1:2, :])
    row_y = lagrange_rows(coords[2:3, :])
    cross = jnp.concatenate([row_x[a : a + 1] * row_z for a in range(8)], axis=0)
    distance = lax.rem(owner[...] - w + n_wall, n_wall)
    from_next = distance == 1
    from_prev = distance == n_wall - 1
    own = jnp.logical_not(jnp.logical_or(from_next, from_prev))
    spread = jnp.concatenate(
        [jnp.where(mask, cross, 0.0) for mask in (own, from_prev, from_next)], axis=0
    )
    n_row = lax.broadcasted_iota(jnp.int32, (length_y, points), 0)
    within = (n_row % 32) // 8
    layer_y = jnp.where(within < NEAR, within + (count_y - NEAR), within - NEAR)
    wanted = (n_row // 32) * count_y + layer_y == element[...]
    along = jnp.where(wanted, jnp.concatenate([row_y] * (length_y // 8), axis=0), 0.0)
    spread = split(spread)

    settle(near_ss, near_rs, near_got)

    sampled = []
    for index in range(2):
        sources = jnp.concatenate(
            [near[index], near_got[0, index], near_got[1, index]], axis=0
        )
        values = dot3(split(sources), spread, TN)
        sampled.append(jnp.sum(values * along, axis=0, keepdims=True))
    stream, spanwise = sampled
    speed = jnp.sqrt(stream * stream + spanwise * spanwise + speed_floor)
    drag = karman / jnp.log(sample_height / roughness[...])
    factor = -(drag * drag * speed / viscosity)
    gradient = (factor * stream, factor * spanwise)
    neumann[0:1, :] = gradient[0]
    neumann[1:2, :] = gradient[1]

    planes = []
    for index in range(2):
        pull = viscosity * gradient[index]
        planes += [pull[:, :rows], pull[:, rows:]]
    node = lax.broadcasted_iota(jnp.int32, (length_x, rows), 1) // length_z
    node_row = lax.broadcasted_iota(jnp.int32, (length_x, rows), 0)
    masked = jnp.concatenate([jnp.where(node == node_row, plane, 0.0) for plane in planes], axis=0)
    pick_row = lax.broadcasted_iota(jnp.int32, (rows, 128), 0)
    pick_lane = lax.broadcasted_iota(jnp.int32, (rows, 128), 1)
    pick = jnp.where(lax.rem(pick_row, length_z) == pick_lane, 1.0, 0.0).astype(BF16)
    masked_hi, masked_lo = split(masked)
    flat = jnp.dot(masked_hi, pick, preferred_element_type=F32) + jnp.dot(
        masked_lo, pick, preferred_element_type=F32
    )
    bundle = flat[0:8]
    tiles = 4 * length_x // 8
    for tile in range(1, tiles):
        bundle = bundle + pltpu.roll(flat[tile * 8 : tile * 8 + 8], tile * length_z, 1)
    pull_send[...] = bundle
    reach = 2 * REACH + 1
    folded = n_span == 2 * REACH
    offsets = [
        (dx, dz)
        for dx in range(-REACH, REACH + 1)
        for dz in range(-REACH, REACH + 1)
        if (dx, dz) != (0, 0) and not (folded and dz == REACH)
    ]
    for dx, dz in sorted(offsets, key=lambda pair: -abs(pair[0]) - abs(pair[1])):
        slot = (REACH - dx) * reach + (REACH - dz)
        remote(pull_send, pull_got.at[slot], pull_ss, pull_rs, at(dx, dz)).start()

    add_faces(0)
    operate(1, 1)
    send_faces(1)
    for c in range(3):
        field[2, c] = local[1, c]
    lines_rows = jnp.concatenate([lines_mass, lines[1] / height], axis=1)
    ends = [lines_rows[0:1], lines_rows[length_y - 1 : length_y]]
    once = [(end[:, :length_y], end[:, length_y:]) for end in ends]
    twice = dot3(
        split(jnp.concatenate([once[0][0], once[0][1], once[1][0], once[1][1]] * 2, axis=0)),
        (lines_hi, lines_lo),
        NN,
    )
    one_lane = lax.broadcasted_iota(jnp.int32, (1, length_y), 1)
    zero = jnp.zeros((1, length_y), F32)
    images = []
    for side in range(2):
        tip = jnp.where(one_lane == side * (length_y - 1), 1.0, 0.0)
        by_mass, by_stiff = twice[2 * side : 2 * side + 1], twice[2 * side + 1 : 2 * side + 2]
        rows_of = [
            (tip, zero, zero),
            (zero, once[side][0], zero),
            (zero, once[side][1], zero),
            (zero, zero, by_mass[:, :length_y]),
            (zero, zero, by_stiff[:, :length_y]),
            (zero, zero, by_mass[:, length_y:]),
            (zero, zero, by_stiff[:, length_y:]),
        ]
        for entry in rows_of:
            image = jnp.concatenate(entry, axis=1)
            images.append(jnp.broadcast_to(image, (length_z, 3 * length_y)))
        images.append(jnp.zeros((128 - 7 * length_z, 3 * length_y), F32))
    images = split(jnp.concatenate(images, axis=0))
    words_x_parts = split(words_x[...])
    words_z_parts = split(words_z[...])

    settle(pull_ss, pull_rs, pull_got.at[pl.ds(0, len(offsets))])
    small_lane = lax.broadcasted_iota(jnp.int32, (8, 128), 1) // length_z
    spans = []
    for ix in range(reach):
        pieces = [
            bundle
            if (ix, iz) == (REACH, REACH)
            else pull_got[ix * reach + (reach - 1 if folded and iz == 0 else iz)]
            for iz in range(reach)
        ]
        for tile in range(tiles):
            line = jnp.zeros((8, 128), F32)
            for iz in range(reach):
                shift = ((iz - tile) * length_z) % 128
                moved = pltpu.roll(pieces[iz], shift, 1) if shift else pieces[iz]
                line = jnp.where(small_lane == iz, moved, line)
            spans.append(line)
    along_z = dot3(split(jnp.concatenate(spans, axis=0)), words_z_parts, NT)
    by_plane = []
    for plane in range(4):
        by_plane.append(
            jnp.concatenate(
                [
                    along_z[(ix * 4 + plane) * length_x : (ix * 4 + plane + 1) * length_x]
                    for ix in range(reach)
                ],
                axis=0,
            )
        )
    both_ways = dot3(words_x_parts, split(jnp.concatenate(by_plane, axis=1)), NN)
    block_lane = lax.broadcasted_iota(jnp.int32, (length_x, 128), 1) // length_z
    keep_row = lax.rem(lax.broadcasted_iota(jnp.int32, (rows, 256), 0), length_z)
    keep_lane = lax.rem(lax.broadcasted_iota(jnp.int32, (rows, 256), 1), length_z)
    tractions = []
    for index in range(2):
        blocks = []
        for side in range(2):
            plane = index * 2 + side
            total = jnp.zeros((length_x, 128), F32)
            for block, word_x, word_z in TERMS:
                piece = both_ways[
                    word_x * length_x : (word_x + 1) * length_x, plane * 128 : plane * 128 + 128
                ]
                shift = ((block - word_z) * length_z) % 128
                moved = pltpu.roll(piece, shift, 1) if shift else piece
                total = total + jnp.where(block_lane == block, moved, 0.0)
            blocks.append(total)
        wide = jnp.concatenate(blocks, axis=1)
        tall = jnp.concatenate(
            [jnp.broadcast_to(wide[x : x + 1], (length_z, 256)) for x in range(length_x)], axis=0
        )
        tall = jnp.where(keep_row == keep_lane, tall, 0.0)
        tractions.append(dot3(split(tall), images, NN))
    add_faces(1)
    t1, t2 = shifts
    for c in range(3):
        chain = [field[level, c] for level in range(3)]
        if c != 1:
            taus = tractions[c // 2]
            chain = [
                chain[level] + taus[:, level * length_y : (level + 1) * length_y]
                for level in range(3)
            ]
        v1 = chain[1] - t1 * chain[0]
        field[0, c] = chain[0]
        field[1, c] = v1
        field[2, c] = chain[2] - t1 * chain[1] - t2 * v1
    operate(2, 2)
    for newest in range(3):
        inner_products(newest)
    for c in range(3):
        inner(6, c, field[2, c] * columns[2] * local[2, c])

    total_rows = parts.shape[0]
    r_iota = lax.broadcasted_iota(jnp.int32, (total_rows, 128), 0)
    l_iota = lax.broadcasted_iota(jnp.int32, (total_rows, 128), 1)
    diagonal = r_iota == l_iota
    summed = jnp.sum(parts[...], axis=1, keepdims=True)
    row = jnp.sum(jnp.where(diagonal, summed, 0.0), axis=0, keepdims=True)

    def gather_sum(stage, row, count, got, ss, rs, place):
        sum_send[stage : stage + 1, :] = row
        for k in range(1, count):
            remote(
                sum_send.at[pl.ds(stage, 1), :], got.at[pl.ds(k - 1, 1), :], ss, rs, place(k)
            ).start()
        settle(ss, rs, got)
        return row + jnp.sum(got[...], axis=0, keepdims=True)

    if single:
        every = n_wall * n_span
        row = gather_sum(
            0, row, every, wall_got, wall_ss, wall_rs, lambda k: at(k // n_span, k % n_span)
        )
    else:
        row = gather_sum(0, row, n_wall, wall_got, wall_ss, wall_rs, lambda k: at(k, 0))
        row = gather_sum(1, row, n_span, span_got, span_ss, span_rs, lambda k: at(0, k))
    totals = jnp.sum(jnp.where(diagonal, row, 0.0), axis=1, keepdims=True)
    m00, m01, m11, m02, m12, m22, e22 = [totals[q * 8 : q * 8 + 8, :] for q in range(7)]
    t1, t2 = shifts
    a00 = m01 + t1 * m00
    a01 = m11 + t1 * m01
    a02 = m12 + t1 * m02
    a11 = m12 + t2 * m11
    a12 = m22 + t2 * m12
    l10 = a01 / a00
    l20 = a02 / a00
    d1 = a11 - l10 * a01
    u12 = a12 - l10 * a02
    l21 = u12 / d1
    d2 = e22 - l20 * a02 - l21 * u12
    y1 = m01 - l10 * m00
    y2 = m02 - l20 * m00 - l21 * y1
    x2 = y2 / d2
    x1 = y1 / d1 - l21 * x2
    x0 = m00 / a00 - l10 * x1 - l20 * x2
    for index, value in enumerate((x0, x1, x2)):
        factors[index] = jnp.broadcast_to(value, (8, 128))


def combine(field, factors, neumann_in, out, neumann, stage, sems):
    small = pltpu.make_async_copy(neumann_in, neumann, sems.at[3])
    small.start()
    copies = []
    for c in range(3):
        result = factors[0, c : c + 1] * field[0, c]
        for level in range(1, 3):
            result += factors[level, c : c + 1] * field[level, c]
        stage[c] = result.reshape(stage.shape[1:])
        copy = pltpu.make_async_copy(stage.at[c], out.at[c], sems.at[c])
        copy.start()
        copies.append(copy)
    for copy in copies:
        copy.wait()
    small.wait()


def body(n_wall, n_span, velocity_old, heights, owner_device, owner_element, ref_coords, roughness):
    sizes = velocity_old.shape[1:]
    length_x, length_z, length_y = sizes
    rows = length_x * length_z
    points = owner_device.shape[0]
    both, lines, columns, words_x, words_z = tables(*sizes)
    plane_hi, plane_lo = split_np(both)
    every = n_wall * n_span
    first = every if every <= SINGLE_STAGE else n_wall
    faces = -(-(6 * (length_x + length_z) + 12) // 8) * 8
    vmem = pl.BlockSpec(memory_space=pltpu.VMEM)
    hbm = pl.BlockSpec(memory_space=pltpu.HBM)
    operands = (
        velocity_old,
        heights.reshape(1, -1),
        owner_device.reshape(1, -1),
        owner_element.reshape(1, -1),
        ref_coords,
        roughness.reshape(1, -1),
        plane_hi,
        plane_lo,
        jnp.asarray(lines, F32),
        jnp.asarray(columns, F32),
        jnp.asarray(words_x, F32),
        jnp.asarray(words_z, F32),
    )
    dma = pltpu.SemaphoreType.DMA
    field, factors, neumann = pl.pallas_call(
        functools.partial(kernel, n_wall, n_span, sizes),
        out_shape=(
            pltpu.VMEM((3, 3, rows, length_y), F32),
            pltpu.VMEM((3, 8, 128), F32),
            pltpu.VMEM((2, points), F32),
        ),
        in_specs=[hbm] * 12,
        out_specs=(vmem, vmem, vmem),
        scratch_shapes=[pltpu.VMEM(value.shape, value.dtype) for value in operands]
        + [
            dma((12,)),
            pltpu.VMEM((2, 64, length_y), F32),
            pltpu.VMEM((2, 2, 64, length_y), F32),
            pltpu.VMEM((3, 3, rows, length_y), F32),
            pltpu.VMEM((ROUNDS, faces, length_y), F32),
            pltpu.VMEM((ROUNDS, faces, length_y), F32),
            pltpu.VMEM((56, length_y), F32),
            pltpu.VMEM((2, 128), F32),
            pltpu.VMEM((first - 1, 128), F32),
            pltpu.VMEM((n_span - 1, 128), F32),
            pltpu.VMEM((8, 128), F32),
            pltpu.VMEM((25, 8, 128), F32),
            dma,
            dma,
            dma,
            dma,
            dma((ROUNDS,)),
            dma((ROUNDS,)),
            dma,
            dma,
            dma,
            dma,
        ],
        compiler_params=pltpu.CompilerParams(
            collective_id=0, has_side_effects=True, vmem_limit_bytes=VMEM_LIMIT
        ),
    )(*[pltpu.with_memory_space_constraint(value, pltpu.HBM) for value in operands])
    return pl.pallas_call(
        combine,
        out_shape=(
            jax.ShapeDtypeStruct(velocity_old.shape, F32),
            jax.ShapeDtypeStruct((2, points), F32),
        ),
        in_specs=[vmem] * 3,
        out_specs=(hbm, hbm),
        scratch_shapes=[pltpu.VMEM(velocity_old.shape, F32), dma((4,))],
        compiler_params=pltpu.CompilerParams(vmem_limit_bytes=VMEM_LIMIT),
    )(field, factors, neumann)


def solution(mesh):
    placed = (
        P(None, "wall", "span", None),
        P(),
        P(("wall", "span"), None),
        P(("wall", "span"), None),
        P(None, ("wall", "span")),
        P(("wall", "span")),
    )
    return jax.shard_map(
        functools.partial(body, mesh.shape["wall"], mesh.shape["span"]),
        mesh=mesh,
        in_specs=placed,
        out_specs=(P(None, "wall", "span", None), P(None, ("wall", "span"))),
        check_vma=False,
    )
```

```python
import functools

import jax
import jax.numpy as jnp
import numpy as np
from jax import lax
from jax.experimental import pallas as pl
from jax.experimental.pallas import tpu as pltpu
from jax.sharding import PartitionSpec as P

GLL_NODES = (
    -1.0,
    -0.8717401485096066,
    -0.5917001814331423,
    -0.2092992179024789,
    0.2092992179024789,
    0.5917001814331423,
    0.8717401485096066,
    1.0,
)
GLL_WEIGHTS = (
    0.03571428571428571,
    0.2107042271435061,
    0.3411226924835044,
    0.4124587946587038,
    0.4124587946587038,
    0.3411226924835044,
    0.2107042271435061,
    0.03571428571428571,
)
viscosity = 0.02
inverse_step = 20.0
karman = 0.41
sample_height = 0.1
speed_floor = 0.01
element_dx = 0.05
element_dz = 0.13
NEAR = 2
ROUNDS = 2
REACH = 2
TERMS = (
    (0, 0, 0),
    (1, 1, 2),
    (1, 2, 1),
    (2, 2, 2),
    (3, 3, 6),
    (3, 4, 5),
    (3, 5, 4),
    (3, 6, 3),
    (4, 4, 6),
    (4, 6, 4),
    (5, 5, 6),
    (5, 6, 5),
    (6, 6, 6),
)
SINGLE_STAGE = 64
VMEM_LIMIT = 32 * 2**20
MESH = pl.DeviceIdType.MESH
F32 = jnp.float32
BF16 = jnp.bfloat16


def stiffness_table():
    points = np.array(GLL_NODES)
    weights = np.array(GLL_WEIGHTS)
    previous = np.ones(8)
    current = points.copy()
    for degree in range(1, 7):
        previous, current = (
            current,
            ((2 * degree + 1) * points * current - degree * previous) / (degree + 1),
        )
    derivative = np.zeros((8, 8))
    for target in range(8):
        for source in range(8):
            if target != source:
                derivative[target, source] = (
                    current[target] / current[source] / (points[target] - points[source])
                )
    derivative[0, 0] = -14.0
    derivative[7, 7] = 14.0
    return derivative.T @ (weights[:, None] * derivative)


def join_matrix(length):
    joined = np.eye(length)
    for left in range(7, length - 1, 8):
        joined[left, left + 1] = 1.0
        joined[left + 1, left] = 1.0
    return joined


def face_weights(length, open_ends):
    values = np.ones(length)
    position = np.arange(length) % 8
    values[(position == 0) | (position == 7)] = 0.5
    if open_ends:
        values[0] = 1.0
        values[-1] = 1.0
    return values


def split_np(matrix):
    single = jnp.asarray(matrix, F32)
    high = single.astype(BF16)
    low = (jnp.asarray(matrix, F32) - high.astype(F32)).astype(BF16)
    return high, low


def tables(length_x, length_z, length_y):
    weights = np.array(GLL_WEIGHTS)
    stiffness = stiffness_table()
    count_x, count_z, count_y = length_x // 8, length_z // 8, length_y // 8
    mass_x = np.tile(0.5 * element_dx * weights, count_x)
    mass_z = np.tile(0.5 * element_dz * weights, count_z)
    stiff_x = np.kron(np.eye(count_x), stiffness * (2.0 / element_dx))
    stiff_z = np.kron(np.eye(count_z), stiffness * (2.0 / element_dz))
    mass_xz = np.kron(mass_x, mass_z)
    join_xz = np.kron(join_matrix(length_x), join_matrix(length_z))
    join_y = join_matrix(length_y)
    plane = viscosity * (
        np.kron(stiff_x, np.diag(mass_z)) + np.kron(np.diag(mass_x), stiff_z)
    ) + inverse_step * np.diag(mass_xz)
    plane = join_xz @ plane
    mass_plane = join_xz @ mass_xz
    lines_mass = np.tile(0.5 * weights, count_y)[:, None] * join_y
    lines_stiff = viscosity * 2.0 * (np.kron(np.eye(count_y), stiffness) @ join_y)
    lines = np.stack([lines_mass, lines_stiff])
    ring_x = join_matrix(length_x) @ mass_x
    ring_z = join_matrix(length_z) @ mass_z
    ring_x[0] *= 2.0
    ring_x[-1] *= 2.0
    ring_z[0] *= 2.0
    ring_z[-1] *= 2.0
    assembled = inverse_step * np.kron(ring_x, ring_z)
    inner_x = face_weights(length_x, True)
    inner_z = face_weights(length_z, True)
    outer_x = face_weights(length_x, False)
    outer_z = face_weights(length_z, False)
    columns = np.stack(
        [assembled, mass_plane, np.kron(outer_x, outer_z), np.kron(inner_x, inner_z)]
    )
    columns = columns[:, :, None] * np.ones(length_y)[None, None]
    reach = 2 * REACH + 1

    def words(length, mass, stiff, extra):
        size = reach * length
        join = join_matrix(size)
        light = join @ np.diag(np.tile(mass, reach))
        heavy = viscosity * join @ np.kron(np.eye(size // 8), stiff) + extra * light
        chains = [
            light,
            heavy @ light,
            light @ light,
            heavy @ heavy @ light,
            heavy @ light @ light,
            light @ heavy @ light,
            light @ light @ light,
        ]
        middle = REACH * length
        chains = [chain[middle : middle + length] for chain in chains]
        return np.concatenate(chains + [np.zeros((128 - 7 * length, size))], axis=0)

    words_x = words(length_x, mass_x, stiffness * (2.0 / element_dx), 0.0)
    words_z = words(length_z, mass_z, stiffness * (2.0 / element_dz), inverse_step)
    pad = np.zeros((128, 128 - reach * length_z))
    words_z = np.concatenate([words_z, pad], axis=1)
    pad = np.zeros((128, 128 - reach * length_x))
    words_x = np.concatenate([words_x, pad], axis=1)
    return plane, lines, columns, words_x, words_z


def split(value):
    high = value.astype(BF16)
    low = (value - high.astype(F32)).astype(BF16)
    return high, low


def dot3(left, right, dims):
    def one(a, b):
        return lax.dot_general(a, b, (dims, ((), ())), preferred_element_type=F32)

    return one(left[0], right[0]) + (one(left[0], right[1]) + one(left[1], right[0]))


NN = ((1,), (0,))
NT = ((1,), (1,))
TN = ((0,), (0,))
DIRS = ((1, 1), (1, -1), (-1, 1), (-1, -1))


def lagrange_rows(coord):
    points = np.array(GLL_NODES)
    scale = 1.0 / np.prod(points[:, None] - points[None, :] + np.eye(8), axis=1)
    shape = (8, coord.shape[1])
    node = lax.broadcasted_iota(jnp.int32, shape, 0)
    total = jnp.zeros(shape, F32)
    for a in range(8):
        total = jnp.where(node == a, F32(scale[a]), total)
    for b in range(8):
        total = total * jnp.where(node == b, F32(1.0), coord - F32(points[b]))
    return total


def kernel(
    n_wall,
    n_span,
    sizes,
    vel_in,
    heights_in,
    owner_in,
    element_in,
    coords_in,
    roughness_in,
    plane_in,
    lines_in,
    columns_in,
    words_in,
    field,
    factors,
    neumann,
    vel,
    heights,
    owner,
    element,
    coords,
    roughness,
    sheet,
    lines,
    columns,
    words,
    load_sem,
    near,
    near_got,
    local,
    face_send,
    face_got,
    parts,
    sum_send,
    wall_got,
    span_got,
    pull_send,
    pull_got,
    pull_ss,
    pull_rs,
    near_ss,
    near_rs,
    face_ss,
    face_rs,
    wall_ss,
    wall_rs,
    span_ss,
    span_rs,
):
    length_x, length_z, length_y = sizes
    rows = length_x * length_z
    count_z, count_y = length_z // 8, length_y // 8
    w = lax.axis_index("wall")
    s = lax.axis_index("span")

    def at(dx, dz):
        return (lax.rem(w + (dx + n_wall), n_wall), lax.rem(s + (dz + n_span), n_span))

    loads = {
        name: pltpu.make_async_copy(source, target, load_sem.at[index])
        for index, (name, source, target) in enumerate(
            (
                ("vel", vel_in, vel),
                ("heights", heights_in, heights),
                ("lines", lines_in, lines),
                ("scale", columns_in.at[pl.ds(0, 2)], columns.at[pl.ds(0, 2)]),
                ("plane", plane_in, sheet),
                ("coords", coords_in, coords),
                ("owner", owner_in, owner),
                ("element", element_in, element),
                ("roughness", roughness_in, roughness),
                ("words", words_in, words),
                ("weights", columns_in.at[pl.ds(2, 2)], columns.at[pl.ds(2, 2)]),
            )
        )
    }
    for load in loads.values():
        load.start()

    def loaded(*names):
        for name in names:
            loads[name].wait()

    single = n_wall * n_span <= SINGLE_STAGE
    if single:
        greeted = [divmod(k, n_span) for k in range(1, n_wall * n_span)]
    else:
        greeted = [(k, 0) for k in range(1, n_wall)] + [(0, k) for k in range(1, n_span)]
        greeted += sorted(
            {
                ((dx + n_wall) % n_wall, (dz + n_span) % n_span)
                for dx in range(-REACH, REACH + 1)
                for dz in range(-REACH, REACH + 1)
            }
            - {(0, 0)}
            - set(greeted)
        )
    barrier = pltpu.get_barrier_semaphore()
    for dx, dz in greeted:
        pl.semaphore_signal(barrier, inc=1, device_id=at(dx, dz), device_id_type=MESH)

    loaded("vel")
    lane = lax.broadcasted_iota(jnp.int32, (64, length_y), 1)
    groups = (length_x // 8) * count_z
    for index, comp in enumerate((0, 2)):
        packed = jnp.zeros((64, length_y), F32)
        for group in range(groups):
            ex, ez = group // count_z, group % count_z
            block = vel[comp, pl.ds(ex * 8, 8), pl.ds(ez * 8, 8), :].reshape(64, length_y)
            moved = pltpu.roll(block, (group * 32 + 16) % length_y, 1)
            packed = jnp.where(lane // 32 == group, moved, packed)
        near[index] = packed
    loaded("heights", "lines", "scale", "plane")

    layer_of = lax.broadcasted_iota(jnp.int32, (length_y, count_y), 0) // 8
    layer = lax.broadcasted_iota(jnp.int32, (length_y, count_y), 1)
    height_row = heights[...]
    height = jnp.sum(jnp.where(layer_of == layer, height_row, 0.0), axis=1, keepdims=True)
    lines_mass = height * lines[0]
    lines_stiff = lines[1] / height
    stiff_hi, stiff_lo = split(lines_stiff)
    lines_packed = jnp.concatenate(
        [
            jnp.concatenate([stiff_hi, stiff_lo], axis=1),
            jnp.concatenate([stiff_hi, jnp.zeros_like(stiff_lo)], axis=1),
        ],
        axis=0,
    )
    bound = jnp.max(0.1535 * height_row + 0.000182 / height_row, axis=1, keepdims=True)
    shifts = (0.15 * bound, 0.85 * bound)

    mass_row = jnp.sum(lines_mass, axis=0, keepdims=True)
    scale = columns[0] * mass_row
    for c in range(3):
        field[0, c] = vel[c].reshape(rows, length_y) * scale

    def remote(src, dst, ss, rs, where):
        return pltpu.make_async_remote_copy(
            src_ref=src,
            dst_ref=dst,
            send_sem=ss,
            recv_sem=rs,
            device_id=where,
            device_id_type=MESH,
        )

    face_rows = []
    for slot, (dx, dz) in enumerate(((1, 0), (-1, 0), (0, 1), (0, -1)) + DIRS):
        size = 3 * (1 if dx and dz else length_z if dx else length_x)
        face_rows.append((sum(entry[1] for entry in face_rows), size, dx, dz))
    face_total = sum(entry[1] for entry in face_rows)

    def corner(dx, dz):
        return (rows - length_z if dx == 1 else 0) + (length_z - 1 if dz == 1 else 0)

    def face_part(slot, c, dx, dz):
        first, size = face_rows[slot][0] + c * (face_rows[slot][1] // 3), face_rows[slot][1] // 3
        if dx and dz:
            rows_of = pl.ds(corner(dx, dz), 1)
        elif dx:
            rows_of = pl.ds(rows - length_z if dx == 1 else 0, length_z)
        else:
            rows_of = pl.ds(length_z - 1 if dz == 1 else 0, length_x, stride=length_z)
        return pl.ds(first, size), rows_of

    def send_faces(turn):
        for c in range(3):
            for slot, (_, _, dx, dz) in enumerate(face_rows):
                packed_rows, rows_of = face_part(slot, c, dx, dz)
                face_send[turn, packed_rows, :] = local[turn, c, rows_of, :]
        if turn == 0:
            pl.semaphore_wait(barrier, len(greeted))
            for copy in near_copies:
                copy.start()
        for first, size, dx, dz in face_rows:
            part = (turn, pl.ds(first, size), slice(None))
            remote(
                face_send.at[part], face_got.at[part], face_ss.at[turn], face_rs.at[turn], at(dx, dz)
            ).start()

    def settle(ss, rs, ref):
        for semaphore in (rs, ss):
            pltpu.make_async_copy(ref, ref, semaphore).wait()

    def add_faces(turn):
        settle(face_ss.at[turn], face_rs.at[turn], face_got.at[turn, pl.ds(0, face_total), :])
        for c in range(3):
            for slot, (_, _, dx, dz) in enumerate(face_rows):
                packed_rows, rows_of = face_part(slot, c, -dx, -dz)
                field[turn + 1, c, rows_of, :] = (
                    field[turn + 1, c, rows_of, :] + face_got[turn, packed_rows, :]
                )

    def inner(quantity, c, product):
        parts[quantity * 8 + c : quantity * 8 + c + 1, :] = jnp.sum(
            product, axis=0, keepdims=True
        )

    def operate(source, target):
        highs, lows = zip(*[split(field[source, c]) for c in range(3)])
        along_y = jnp.dot(
            jnp.concatenate(
                [jnp.concatenate([high, low], axis=1) for high, low in zip(highs, lows)], axis=0
            ),
            lines_packed,
            preferred_element_type=F32,
        )
        across = jnp.dot(
            sheet[0], jnp.concatenate(highs + lows, axis=1), preferred_element_type=F32
        )
        across_low = jnp.dot(sheet[1], jnp.concatenate(highs, axis=1), preferred_element_type=F32)
        for c in range(3):
            here = slice(c * length_y, (c + 1) * length_y)
            also = slice((3 + c) * length_y, (4 + c) * length_y)
            flat = across[:, here] + (across[:, also] + across_low[:, here])
            tall = along_y[c * rows : (c + 1) * rows]
            tall = tall[:, :length_y] + tall[:, length_y:]
            local[target, c] = flat * mass_row + tall * columns[1]

    slots = {(0, 0): 0, (0, 1): 1, (1, 1): 2, (0, 2): 3, (1, 2): 4, (2, 2): 5}

    def inner_products(newest):
        for c in range(3):
            weighted = field[newest, c] * columns[2]
            for other in range(newest + 1):
                inner(slots[(other, newest)], c, weighted * field[other, c])

    near_copies = []
    for slot, dx in enumerate((1, -1)):
        copy = remote(near, near_got.at[slot], near_ss, near_rs, at(dx, 0))
        near_copies.append(copy)

    operate(0, 0)
    send_faces(0)
    for c in range(3):
        field[1, c] = local[0, c]
    parts[...] = jnp.zeros_like(parts)

    loaded("coords", "owner", "element", "roughness")
    points = owner.shape[1]
    row_x = lagrange_rows(coords[0:1, :])
    row_z = lagrange_rows(coords[1:2, :])
    row_y = lagrange_rows(coords[2:3, :])
    cross = jnp.concatenate([row_x[a : a + 1] * row_z for a in range(8)], axis=0)
    distance = lax.rem(owner[...] - w + n_wall, n_wall)
    from_next = distance == 1
    from_prev = distance == n_wall - 1
    own = jnp.logical_not(jnp.logical_or(from_next, from_prev))
    spread = jnp.concatenate(
        [jnp.where(mask, cross, 0.0) for mask in (own, from_prev, from_next)], axis=0
    )
    n_row = lax.broadcasted_iota(jnp.int32, (length_y, points), 0)
    within = (n_row % 32) // 8
    layer_y = jnp.where(within < NEAR, within + (count_y - NEAR), within - NEAR)
    wanted = (n_row // 32) * count_y + layer_y == element[...]
    along = jnp.where(wanted, jnp.concatenate([row_y] * (length_y // 8), axis=0), 0.0)
    spread = split(spread)

    settle(near_ss, near_rs, near_got)

    sampled = []
    for index in range(2):
        sources = jnp.concatenate(
            [near[index], near_got[0, index], near_got[1, index]], axis=0
        )
        values = dot3(split(sources), spread, TN)
        sampled.append(jnp.sum(values * along, axis=0, keepdims=True))
    stream, spanwise = sampled
    speed = jnp.sqrt(stream * stream + spanwise * spanwise + speed_floor)
    drag = karman / jnp.log(sample_height / roughness[...])
    factor = -(drag * drag * speed / viscosity)
    gradient = (factor * stream, factor * spanwise)
    neumann[0:1, :] = gradient[0]
    neumann[1:2, :] = gradient[1]

    planes = []
    for index in range(2):
        pull = viscosity * gradient[index]
        planes += [pull[:, :rows], pull[:, rows:]]
    node = lax.broadcasted_iota(jnp.int32, (length_x, rows), 1) // length_z
    node_row = lax.broadcasted_iota(jnp.int32, (length_x, rows), 0)
    masked = jnp.concatenate([jnp.where(node == node_row, plane, 0.0) for plane in planes], axis=0)
    pick_row = lax.broadcasted_iota(jnp.int32, (rows, 128), 0)
    pick_lane = lax.broadcasted_iota(jnp.int32, (rows, 128), 1)
    pick = jnp.where(lax.rem(pick_row, length_z) == pick_lane, 1.0, 0.0).astype(BF16)
    masked_hi, masked_lo = split(masked)
    flat = jnp.dot(masked_hi, pick, preferred_element_type=F32) + jnp.dot(
        masked_lo, pick, preferred_element_type=F32
    )
    bundle = flat[0:8]
    tiles = 4 * length_x // 8
    for tile in range(1, tiles):
        bundle = bundle + pltpu.roll(flat[tile * 8 : tile * 8 + 8], tile * length_z, 1)
    pull_send[...] = bundle
    reach = 2 * REACH + 1
    folded = n_span == 2 * REACH
    offsets = [
        (dx, dz)
        for dx in range(-REACH, REACH + 1)
        for dz in range(-REACH, REACH + 1)
        if (dx, dz) != (0, 0) and not (folded and dz == REACH)
    ]
    for dx, dz in sorted(offsets, key=lambda pair: -abs(pair[0]) - abs(pair[1])):
        slot = (REACH - dx) * reach + (REACH - dz)
        remote(pull_send, pull_got.at[slot], pull_ss, pull_rs, at(dx, dz)).start()

    add_faces(0)
    operate(1, 1)
    send_faces(1)
    for c in range(3):
        field[2, c] = local[1, c]
    loaded("words", "weights")
    lines_rows = jnp.concatenate([lines_mass, lines_stiff], axis=1)
    ends = [lines_rows[0:1], lines_rows[length_y - 1 : length_y]]
    once = [(end[:, :length_y], end[:, length_y:]) for end in ends]
    twice = dot3(
        split(jnp.concatenate([once[0][0], once[0][1], once[1][0], once[1][1]] * 2, axis=0)),
        split(lines_rows),
        NN,
    )
    one_lane = lax.broadcasted_iota(jnp.int32, (1, length_y), 1)
    zero = jnp.zeros((1, length_y), F32)
    images = []
    for side in range(2):
        tip = jnp.where(one_lane == side * (length_y - 1), 1.0, 0.0)
        by_mass, by_stiff = twice[2 * side : 2 * side + 1], twice[2 * side + 1 : 2 * side + 2]
        rows_of = [
            (tip, zero, zero),
            (zero, once[side][0], zero),
            (zero, once[side][1], zero),
            (zero, zero, by_mass[:, :length_y]),
            (zero, zero, by_stiff[:, :length_y]),
            (zero, zero, by_mass[:, length_y:]),
            (zero, zero, by_stiff[:, length_y:]),
        ]
        for entry in rows_of:
            image = jnp.concatenate(entry, axis=1)
            images.append(jnp.broadcast_to(image, (length_z, 3 * length_y)))
        images.append(jnp.zeros((128 - 7 * length_z, 3 * length_y), F32))
    images = split(jnp.concatenate(images, axis=0))
    words_x_parts = (words[0, :, : reach * length_x], words[1, :, : reach * length_x])
    words_z_parts = (words[2], words[3])

    settle(pull_ss, pull_rs, pull_got.at[pl.ds(0, len(offsets))])
    small_lane = lax.broadcasted_iota(jnp.int32, (8, 128), 1) // length_z
    spans = []
    for ix in range(reach):
        pieces = [
            bundle
            if (ix, iz) == (REACH, REACH)
            else pull_got[ix * reach + (reach - 1 if folded and iz == 0 else iz)]
            for iz in range(reach)
        ]
        for tile in range(tiles):
            line = jnp.zeros((8, 128), F32)
            for iz in range(reach):
                shift = ((iz - tile) * length_z) % 128
                moved = pltpu.roll(pieces[iz], shift, 1) if shift else pieces[iz]
                line = jnp.where(small_lane == iz, moved, line)
            spans.append(line)
    along_z = dot3(split(jnp.concatenate(spans, axis=0)), words_z_parts, NT)
    by_plane = []
    for plane in range(4):
        by_plane.append(
            jnp.concatenate(
                [
                    along_z[(ix * 4 + plane) * length_x : (ix * 4 + plane + 1) * length_x]
                    for ix in range(reach)
                ],
                axis=0,
            )
        )
    both_ways = dot3(words_x_parts, split(jnp.concatenate(by_plane, axis=1)), NN)
    block_lane = lax.broadcasted_iota(jnp.int32, (length_x, 128), 1) // length_z
    keep_row = lax.rem(lax.broadcasted_iota(jnp.int32, (rows, 256), 0), length_z)
    keep_lane = lax.rem(lax.broadcasted_iota(jnp.int32, (rows, 256), 1), length_z)
    tractions = []
    for index in range(2):
        blocks = []
        for side in range(2):
            plane = index * 2 + side
            total = jnp.zeros((length_x, 128), F32)
            for block, word_x, word_z in TERMS:
                piece = both_ways[
                    word_x * length_x : (word_x + 1) * length_x, plane * 128 : plane * 128 + 128
                ]
                shift = ((block - word_z) * length_z) % 128
                moved = pltpu.roll(piece, shift, 1) if shift else piece
                total = total + jnp.where(block_lane == block, moved, 0.0)
            blocks.append(total)
        wide = jnp.concatenate(blocks, axis=1)
        tall = jnp.concatenate(
            [jnp.broadcast_to(wide[x : x + 1], (length_z, 256)) for x in range(length_x)], axis=0
        )
        tall = jnp.where(keep_row == keep_lane, tall, 0.0)
        tractions.append(dot3(split(tall), images, NN))
    add_faces(1)
    t1, t2 = shifts
    for c in range(3):
        chain = [field[level, c] for level in range(3)]
        if c != 1:
            taus = tractions[c // 2]
            chain = [
                chain[level] + taus[:, level * length_y : (level + 1) * length_y]
                for level in range(3)
            ]
        v1 = chain[1] - t1 * chain[0]
        field[0, c] = chain[0]
        field[1, c] = v1
        field[2, c] = chain[2] - t1 * chain[1] - t2 * v1
    operate(2, 2)
    for newest in range(3):
        inner_products(newest)
    for c in range(3):
        inner(6, c, field[2, c] * columns[3] * local[2, c])

    total_rows = parts.shape[0]
    r_iota = lax.broadcasted_iota(jnp.int32, (total_rows, 128), 0)
    l_iota = lax.broadcasted_iota(jnp.int32, (total_rows, 128), 1)
    diagonal = r_iota == l_iota
    end_lane = lax.broadcasted_iota(jnp.int32, (total_rows, 128), 1)
    shared = jnp.logical_or(end_lane % 8 == 0, end_lane % 8 == 7)
    tips = jnp.logical_or(end_lane == 0, end_lane == length_y - 1)
    weight_y = jnp.where(jnp.logical_and(shared, jnp.logical_not(tips)), 0.5, 1.0)
    summed = jnp.sum(parts[...] * weight_y, axis=1, keepdims=True)
    row = jnp.sum(jnp.where(diagonal, summed, 0.0), axis=0, keepdims=True)

    def gather_sum(stage, row, count, got, ss, rs, place):
        sum_send[stage : stage + 1, :] = row
        for k in range(1, count):
            remote(
                sum_send.at[pl.ds(stage, 1), :], got.at[pl.ds(k - 1, 1), :], ss, rs, place(k)
            ).start()
        settle(ss, rs, got)
        return row + jnp.sum(got[...], axis=0, keepdims=True)

    if single:
        every = n_wall * n_span
        row = gather_sum(
            0, row, every, wall_got, wall_ss, wall_rs, lambda k: at(k // n_span, k % n_span)
        )
    else:
        row = gather_sum(0, row, n_wall, wall_got, wall_ss, wall_rs, lambda k: at(k, 0))
        row = gather_sum(1, row, n_span, span_got, span_ss, span_rs, lambda k: at(0, k))
    totals = jnp.sum(jnp.where(diagonal, row, 0.0), axis=1, keepdims=True)
    m00, m01, m11, m02, m12, m22, e22 = [totals[q * 8 : q * 8 + 8, :] for q in range(7)]
    t1, t2 = shifts
    a00 = m01 + t1 * m00
    a01 = m11 + t1 * m01
    a02 = m12 + t1 * m02
    a11 = m12 + t2 * m11
    a12 = m22 + t2 * m12
    l10 = a01 / a00
    l20 = a02 / a00
    d1 = a11 - l10 * a01
    u12 = a12 - l10 * a02
    l21 = u12 / d1
    d2 = e22 - l20 * a02 - l21 * u12
    y1 = m01 - l10 * m00
    y2 = m02 - l20 * m00 - l21 * y1
    x2 = y2 / d2
    x1 = y1 / d1 - l21 * x2
    x0 = m00 / a00 - l10 * x1 - l20 * x2
    for index, value in enumerate((x0, x1, x2)):
        factors[index] = jnp.broadcast_to(value, (8, 128))


def combine(field, factors, neumann_in, out, neumann, stage, sems):
    small = pltpu.make_async_copy(neumann_in, neumann, sems.at[3])
    small.start()
    copies = []
    for c in range(3):
        result = factors[0, c : c + 1] * field[0, c]
        for level in range(1, 3):
            result += factors[level, c : c + 1] * field[level, c]
        stage[c] = result.reshape(stage.shape[1:])
        copy = pltpu.make_async_copy(stage.at[c], out.at[c], sems.at[c])
        copy.start()
        copies.append(copy)
    for copy in copies:
        copy.wait()
    small.wait()


def body(n_wall, n_span, velocity_old, heights, owner_device, owner_element, ref_coords, roughness):
    sizes = velocity_old.shape[1:]
    length_x, length_z, length_y = sizes
    rows = length_x * length_z
    points = owner_device.shape[0]
    plane, lines, columns, words_x, words_z = tables(*sizes)
    every = n_wall * n_span
    first = every if every <= SINGLE_STAGE else n_wall
    faces = -(-(6 * (length_x + length_z) + 12) // 8) * 8
    vmem = pl.BlockSpec(memory_space=pltpu.VMEM)
    hbm = pl.BlockSpec(memory_space=pltpu.HBM)
    operands = (
        velocity_old,
        heights.reshape(1, -1),
        owner_device.reshape(1, -1),
        owner_element.reshape(1, -1),
        ref_coords,
        roughness.reshape(1, -1),
        jnp.stack(split_np(plane)),
        jnp.asarray(lines, F32),
        jnp.asarray(columns, F32),
        jnp.stack(split_np(words_x) + split_np(words_z)),
    )
    dma = pltpu.SemaphoreType.DMA
    field, factors, neumann = pl.pallas_call(
        functools.partial(kernel, n_wall, n_span, sizes),
        out_shape=(
            pltpu.VMEM((3, 3, rows, length_y), F32),
            pltpu.VMEM((3, 8, 128), F32),
            pltpu.VMEM((2, points), F32),
        ),
        in_specs=[hbm] * 10,
        out_specs=(vmem, vmem, vmem),
        scratch_shapes=[pltpu.VMEM(value.shape, value.dtype) for value in operands]
        + [
            dma((11,)),
            pltpu.VMEM((2, 64, length_y), F32),
            pltpu.VMEM((2, 2, 64, length_y), F32),
            pltpu.VMEM((3, 3, rows, length_y), F32),
            pltpu.VMEM((ROUNDS, faces, length_y), F32),
            pltpu.VMEM((ROUNDS, faces, length_y), F32),
            pltpu.VMEM((56, length_y), F32),
            pltpu.VMEM((2, 128), F32),
            pltpu.VMEM((first - 1, 128), F32),
            pltpu.VMEM((n_span - 1, 128), F32),
            pltpu.VMEM((8, 128), F32),
            pltpu.VMEM((25, 8, 128), F32),
            dma,
            dma,
            dma,
            dma,
            dma((ROUNDS,)),
            dma((ROUNDS,)),
            dma,
            dma,
            dma,
            dma,
        ],
        compiler_params=pltpu.CompilerParams(
            collective_id=0, has_side_effects=True, vmem_limit_bytes=VMEM_LIMIT
        ),
    )(*[pltpu.with_memory_space_constraint(value, pltpu.HBM) for value in operands])
    return pl.pallas_call(
        combine,
        out_shape=(
            jax.ShapeDtypeStruct(velocity_old.shape, F32),
            jax.ShapeDtypeStruct((2, points), F32),
        ),
        in_specs=[vmem] * 3,
        out_specs=(hbm, hbm),
        scratch_shapes=[pltpu.VMEM(velocity_old.shape, F32), dma((4,))],
        compiler_params=pltpu.CompilerParams(vmem_limit_bytes=VMEM_LIMIT),
    )(field, factors, neumann)


def solution(mesh):
    placed = (
        P(None, "wall", "span", None),
        P(),
        P(("wall", "span"), None),
        P(("wall", "span"), None),
        P(None, ("wall", "span")),
        P(("wall", "span")),
    )
    return jax.shard_map(
        functools.partial(body, mesh.shape["wall"], mesh.shape["span"]),
        mesh=mesh,
        in_specs=placed,
        out_specs=(P(None, "wall", "span", None), P(None, ("wall", "span"))),
        check_vma=False,
    )
```

```python
import functools

import jax
import jax.numpy as jnp
import numpy as np
from jax import lax
from jax.experimental import pallas as pl
from jax.experimental.pallas import tpu as pltpu
from jax.sharding import PartitionSpec as P

GLL_NODES = (
    -1.0,
    -0.8717401485096066,
    -0.5917001814331423,
    -0.2092992179024789,
    0.2092992179024789,
    0.5917001814331423,
    0.8717401485096066,
    1.0,
)
GLL_WEIGHTS = (
    0.03571428571428571,
    0.2107042271435061,
    0.3411226924835044,
    0.4124587946587038,
    0.4124587946587038,
    0.3411226924835044,
    0.2107042271435061,
    0.03571428571428571,
)
viscosity = 0.02
inverse_step = 20.0
karman = 0.41
sample_height = 0.1
speed_floor = 0.01
element_dx = 0.05
element_dz = 0.13
NEAR = 2
ROUNDS = 2
REACH = 2
TERMS = (
    (0, 0, 0),
    (1, 1, 2),
    (1, 2, 1),
    (2, 2, 2),
    (3, 3, 6),
    (3, 4, 5),
    (3, 5, 4),
    (3, 6, 3),
    (4, 4, 6),
    (4, 6, 4),
    (5, 5, 6),
    (5, 6, 5),
    (6, 6, 6),
)
SINGLE_STAGE = 64
VMEM_LIMIT = 32 * 2**20
MESH = pl.DeviceIdType.MESH
F32 = jnp.float32
BF16 = jnp.bfloat16


def stiffness_table():
    points = np.array(GLL_NODES)
    weights = np.array(GLL_WEIGHTS)
    previous = np.ones(8)
    current = points.copy()
    for degree in range(1, 7):
        previous, current = (
            current,
            ((2 * degree + 1) * points * current - degree * previous) / (degree + 1),
        )
    derivative = np.zeros((8, 8))
    for target in range(8):
        for source in range(8):
            if target != source:
                derivative[target, source] = (
                    current[target] / current[source] / (points[target] - points[source])
                )
    derivative[0, 0] = -14.0
    derivative[7, 7] = 14.0
    return derivative.T @ (weights[:, None] * derivative)


def join_matrix(length):
    joined = np.eye(length)
    for left in range(7, length - 1, 8):
        joined[left, left + 1] = 1.0
        joined[left + 1, left] = 1.0
    return joined


def face_weights(length, open_ends):
    values = np.ones(length)
    position = np.arange(length) % 8
    values[(position == 0) | (position == 7)] = 0.5
    if open_ends:
        values[0] = 1.0
        values[-1] = 1.0
    return values


def split_np(matrix):
    single = jnp.asarray(matrix, F32)
    high = single.astype(BF16)
    low = (jnp.asarray(matrix, F32) - high.astype(F32)).astype(BF16)
    return high, low


def tables(length_x, length_z, length_y):
    weights = np.array(GLL_WEIGHTS)
    stiffness = stiffness_table()
    count_x, count_z, count_y = length_x // 8, length_z // 8, length_y // 8
    mass_x = np.tile(0.5 * element_dx * weights, count_x)
    mass_z = np.tile(0.5 * element_dz * weights, count_z)
    stiff_x = np.kron(np.eye(count_x), stiffness * (2.0 / element_dx))
    stiff_z = np.kron(np.eye(count_z), stiffness * (2.0 / element_dz))
    mass_xz = np.kron(mass_x, mass_z)
    join_xz = np.kron(join_matrix(length_x), join_matrix(length_z))
    join_y = join_matrix(length_y)
    plane = viscosity * (
        np.kron(stiff_x, np.diag(mass_z)) + np.kron(np.diag(mass_x), stiff_z)
    ) + inverse_step * np.diag(mass_xz)
    plane = join_xz @ plane
    mass_plane = join_xz @ mass_xz
    lines_mass = np.tile(0.5 * weights, count_y)[:, None] * join_y
    lines_stiff = viscosity * 2.0 * (np.kron(np.eye(count_y), stiffness) @ join_y)
    lines = np.stack([lines_mass, lines_stiff])
    ring_x = join_matrix(length_x) @ mass_x
    ring_z = join_matrix(length_z) @ mass_z
    ring_x[0] *= 2.0
    ring_x[-1] *= 2.0
    ring_z[0] *= 2.0
    ring_z[-1] *= 2.0
    assembled = inverse_step * np.kron(ring_x, ring_z)
    inner_x = face_weights(length_x, True)
    inner_z = face_weights(length_z, True)
    outer_x = face_weights(length_x, False)
    outer_z = face_weights(length_z, False)
    columns = np.stack(
        [assembled, mass_plane, np.kron(outer_x, outer_z), np.kron(inner_x, inner_z)]
    )
    columns = columns[:, :, None] * np.ones(length_y)[None, None]
    reach = 2 * REACH + 1

    def words(length, mass, stiff, extra):
        size = reach * length
        join = join_matrix(size)
        light = join @ np.diag(np.tile(mass, reach))
        heavy = viscosity * join @ np.kron(np.eye(size // 8), stiff) + extra * light
        chains = [
            light,
            heavy @ light,
            light @ light,
            heavy @ heavy @ light,
            heavy @ light @ light,
            light @ heavy @ light,
            light @ light @ light,
        ]
        middle = REACH * length
        chains = [chain[middle : middle + length] for chain in chains]
        return np.concatenate(chains + [np.zeros((128 - 7 * length, size))], axis=0)

    words_x = words(length_x, mass_x, stiffness * (2.0 / element_dx), 0.0)
    words_z = words(length_z, mass_z, stiffness * (2.0 / element_dz), inverse_step)
    pad = np.zeros((128, 128 - reach * length_z))
    words_z = np.concatenate([words_z, pad], axis=1)
    pad = np.zeros((128, 128 - reach * length_x))
    words_x = np.concatenate([words_x, pad], axis=1)
    return plane, lines, columns, words_x, words_z


def split(value):
    high = value.astype(BF16)
    low = (value - high.astype(F32)).astype(BF16)
    return high, low


def dot3(left, right, dims):
    def one(a, b):
        return lax.dot_general(a, b, (dims, ((), ())), preferred_element_type=F32)

    return one(left[0], right[0]) + (one(left[0], right[1]) + one(left[1], right[0]))


NN = ((1,), (0,))
NT = ((1,), (1,))
TN = ((0,), (0,))
DIRS = ((1, 1), (1, -1), (-1, 1), (-1, -1))


def lagrange_rows(coord):
    points = np.array(GLL_NODES)
    scale = 1.0 / np.prod(points[:, None] - points[None, :] + np.eye(8), axis=1)
    shape = (8, coord.shape[1])
    node = lax.broadcasted_iota(jnp.int32, shape, 0)
    total = jnp.zeros(shape, F32)
    for a in range(8):
        total = jnp.where(node == a, F32(scale[a]), total)
    for b in range(8):
        total = total * jnp.where(node == b, F32(1.0), coord - F32(points[b]))
    return total


def kernel(
    n_wall,
    n_span,
    sizes,
    vel_in,
    heights_in,
    owner_in,
    element_in,
    coords_in,
    roughness_in,
    plane_in,
    lines_in,
    columns_in,
    words_in,
    field,
    factors,
    neumann,
    vel,
    heights,
    owner,
    element,
    coords,
    roughness,
    sheet,
    lines,
    columns,
    words,
    load_sem,
    near,
    near_got,
    local,
    face_send,
    face_got,
    parts,
    sum_send,
    wall_got,
    span_got,
    pull_send,
    pull_got,
    pull_ss,
    pull_rs,
    near_ss,
    near_rs,
    face_ss,
    face_rs,
    wall_ss,
    wall_rs,
    span_ss,
    span_rs,
    step_one,
    step_two,
):
    length_x, length_z, length_y = sizes
    rows = length_x * length_z
    count_z, count_y = length_z // 8, length_y // 8
    w = lax.axis_index("wall")
    s = lax.axis_index("span")

    def at(dx, dz):
        return (lax.rem(w + (dx + n_wall), n_wall), lax.rem(s + (dz + n_span), n_span))

    loads = {
        name: pltpu.make_async_copy(source, target, load_sem.at[index])
        for index, (name, source, target) in enumerate(
            (
                ("vel", vel_in, vel),
                ("heights", heights_in, heights),
                ("lines", lines_in, lines),
                ("scale", columns_in.at[pl.ds(0, 2)], columns.at[pl.ds(0, 2)]),
                ("plane", plane_in, sheet),
                ("coords", coords_in, coords),
                ("owner", owner_in, owner),
                ("element", element_in, element),
                ("roughness", roughness_in, roughness),
                ("words", words_in, words),
                ("weights", columns_in.at[pl.ds(2, 2)], columns.at[pl.ds(2, 2)]),
            )
        )
    }
    for load in loads.values():
        load.start()

    def loaded(*names):
        for name in names:
            loads[name].wait()

    single = n_wall * n_span <= SINGLE_STAGE
    stepwise = single and 3 <= n_wall <= 4 * REACH and 3 <= n_span <= 4 * REACH
    sides = ((1, 0), (-1, 0), (0, 1), (0, -1))
    if stepwise:
        greeted = sides
    elif single:
        greeted = [divmod(k, n_span) for k in range(1, n_wall * n_span)]
    else:
        greeted = [(k, 0) for k in range(1, n_wall)] + [(0, k) for k in range(1, n_span)]
        greeted += sorted(
            {
                ((dx + n_wall) % n_wall, (dz + n_span) % n_span)
                for dx in range(-REACH, REACH + 1)
                for dz in range(-REACH, REACH + 1)
            }
            - {(0, 0)}
            - set(greeted)
        )
    barrier = pltpu.get_barrier_semaphore()

    def greet(semaphore, places):
        for dx, dz in places:
            pl.semaphore_signal(semaphore, inc=1, device_id=at(dx, dz), device_id_type=MESH)

    greet(barrier, greeted)

    loaded("vel")
    lane = lax.broadcasted_iota(jnp.int32, (64, length_y), 1)
    groups = (length_x // 8) * count_z
    for index, comp in enumerate((0, 2)):
        packed = jnp.zeros((64, length_y), F32)
        for group in range(groups):
            ex, ez = group // count_z, group % count_z
            block = vel[comp, pl.ds(ex * 8, 8), pl.ds(ez * 8, 8), :].reshape(64, length_y)
            moved = pltpu.roll(block, (group * 32 + 16) % length_y, 1)
            packed = jnp.where(lane // 32 == group, moved, packed)
        near[index] = packed
    def remote(src, dst, ss, rs, where):
        return pltpu.make_async_remote_copy(
            src_ref=src,
            dst_ref=dst,
            send_sem=ss,
            recv_sem=rs,
            device_id=where,
            device_id_type=MESH,
        )

    near_copies = []
    for slot, dx in enumerate((1, -1)):
        copy = remote(near, near_got.at[slot], near_ss, near_rs, at(dx, 0))
        near_copies.append(copy)

    def enter():
        pl.semaphore_wait(barrier, len(greeted))
        for copy in near_copies:
            copy.start()
        if stepwise:
            greet(step_one, sides)

    if stepwise:
        enter()
    loaded("heights", "lines", "scale", "plane")

    layer_of = lax.broadcasted_iota(jnp.int32, (length_y, count_y), 0) // 8
    layer = lax.broadcasted_iota(jnp.int32, (length_y, count_y), 1)
    height_row = heights[...]
    height = jnp.sum(jnp.where(layer_of == layer, height_row, 0.0), axis=1, keepdims=True)
    lines_mass = height * lines[0]
    lines_stiff = lines[1] / height
    stiff_hi, stiff_lo = split(lines_stiff)
    lines_packed = jnp.concatenate(
        [
            jnp.concatenate([stiff_hi, stiff_lo], axis=1),
            jnp.concatenate([stiff_hi, jnp.zeros_like(stiff_lo)], axis=1),
        ],
        axis=0,
    )
    bound = jnp.max(0.1535 * height_row + 0.000182 / height_row, axis=1, keepdims=True)
    shifts = (0.15 * bound, 0.85 * bound)

    mass_row = jnp.sum(lines_mass, axis=0, keepdims=True)
    scale = columns[0] * mass_row
    for c in range(3):
        field[0, c] = vel[c].reshape(rows, length_y) * scale

    face_rows = []
    for slot, (dx, dz) in enumerate(DIRS + ((0, 1), (0, -1), (1, 0), (-1, 0))):
        size = 3 * (1 if dx and dz else length_z if dx else length_x)
        face_rows.append((sum(entry[1] for entry in face_rows), size, dx, dz))
    face_total = sum(entry[1] for entry in face_rows)

    def corner(dx, dz):
        return (rows - length_z if dx == 1 else 0) + (length_z - 1 if dz == 1 else 0)

    def face_part(slot, c, dx, dz):
        first, size = face_rows[slot][0] + c * (face_rows[slot][1] // 3), face_rows[slot][1] // 3
        if dx and dz:
            rows_of = pl.ds(corner(dx, dz), 1)
        elif dx:
            rows_of = pl.ds(rows - length_z if dx == 1 else 0, length_z)
        else:
            rows_of = pl.ds(length_z - 1 if dz == 1 else 0, length_x, stride=length_z)
        return pl.ds(first, size), rows_of

    def send_faces(turn):
        for c in range(3):
            for slot, (_, _, dx, dz) in enumerate(face_rows):
                packed_rows, rows_of = face_part(slot, c, dx, dz)
                face_send[turn, packed_rows, :] = local[turn, c, rows_of, :]
        if turn == 0 and stepwise:
            pl.semaphore_wait(step_one, len(sides))
            greet(step_two, sides + DIRS)
        elif turn == 0:
            enter()
        for first, size, dx, dz in face_rows:
            part = (turn, pl.ds(first, size), slice(None))
            remote(
                face_send.at[part], face_got.at[part], face_ss.at[turn], face_rs.at[turn], at(dx, dz)
            ).start()

    def settle(ss, rs, ref):
        for semaphore in (rs, ss):
            pltpu.make_async_copy(ref, ref, semaphore).wait()

    def add_faces(turn):
        settle(face_ss.at[turn], face_rs.at[turn], face_got.at[turn, pl.ds(0, face_total), :])
        for c in range(3):
            for slot, (_, _, dx, dz) in enumerate(face_rows):
                packed_rows, rows_of = face_part(slot, c, -dx, -dz)
                field[turn + 1, c, rows_of, :] = (
                    field[turn + 1, c, rows_of, :] + face_got[turn, packed_rows, :]
                )

    def inner(quantity, c, product):
        parts[quantity * 8 + c : quantity * 8 + c + 1, :] = jnp.sum(
            product, axis=0, keepdims=True
        )

    def operate(source, target):
        highs, lows = zip(*[split(field[source, c]) for c in range(3)])
        along_y = jnp.dot(
            jnp.concatenate(
                [jnp.concatenate([high, low], axis=1) for high, low in zip(highs, lows)], axis=0
            ),
            lines_packed,
            preferred_element_type=F32,
        )
        across = jnp.dot(
            sheet[0], jnp.concatenate(highs + lows, axis=1), preferred_element_type=F32
        )
        across_low = jnp.dot(sheet[1], jnp.concatenate(highs, axis=1), preferred_element_type=F32)
        for c in range(3):
            here = slice(c * length_y, (c + 1) * length_y)
            also = slice((3 + c) * length_y, (4 + c) * length_y)
            flat = across[:, here] + (across[:, also] + across_low[:, here])
            tall = along_y[c * rows : (c + 1) * rows]
            tall = tall[:, :length_y] + tall[:, length_y:]
            local[target, c] = flat * mass_row + tall * columns[1]

    slots = {(0, 0): 0, (0, 1): 1, (1, 1): 2, (0, 2): 3, (1, 2): 4, (2, 2): 5}

    def inner_products(newest):
        for c in range(3):
            weighted = field[newest, c] * columns[2]
            for other in range(newest + 1):
                inner(slots[(other, newest)], c, weighted * field[other, c])

    operate(0, 0)
    send_faces(0)
    for c in range(3):
        field[1, c] = local[0, c]
    parts[...] = jnp.zeros_like(parts)

    loaded("coords", "owner", "element", "roughness")
    points = owner.shape[1]
    row_x = lagrange_rows(coords[0:1, :])
    row_z = lagrange_rows(coords[1:2, :])
    row_y = lagrange_rows(coords[2:3, :])
    cross = jnp.concatenate([row_x[a : a + 1] * row_z for a in range(8)], axis=0)
    distance = lax.rem(owner[...] - w + n_wall, n_wall)
    from_next = distance == 1
    from_prev = distance == n_wall - 1
    own = jnp.logical_not(jnp.logical_or(from_next, from_prev))
    spread = jnp.concatenate(
        [jnp.where(mask, cross, 0.0) for mask in (own, from_prev, from_next)], axis=0
    )
    n_row = lax.broadcasted_iota(jnp.int32, (length_y, points), 0)
    within = (n_row % 32) // 8
    layer_y = jnp.where(within < NEAR, within + (count_y - NEAR), within - NEAR)
    wanted = (n_row // 32) * count_y + layer_y == element[...]
    along = jnp.where(wanted, jnp.concatenate([row_y] * (length_y // 8), axis=0), 0.0)
    spread = split(spread)

    settle(near_ss, near_rs, near_got)

    sampled = []
    for index in range(2):
        sources = jnp.concatenate(
            [near[index], near_got[0, index], near_got[1, index]], axis=0
        )
        values = dot3(split(sources), spread, TN)
        sampled.append(jnp.sum(values * along, axis=0, keepdims=True))
    stream, spanwise = sampled
    speed = jnp.sqrt(stream * stream + spanwise * spanwise + speed_floor)
    drag = karman / jnp.log(sample_height / roughness[...])
    factor = -(drag * drag * speed / viscosity)
    gradient = (factor * stream, factor * spanwise)
    neumann[0:1, :] = gradient[0]
    neumann[1:2, :] = gradient[1]

    planes = []
    for index in range(2):
        pull = viscosity * gradient[index]
        planes += [pull[:, :rows], pull[:, rows:]]
    node = lax.broadcasted_iota(jnp.int32, (length_x, rows), 1) // length_z
    node_row = lax.broadcasted_iota(jnp.int32, (length_x, rows), 0)
    masked = jnp.concatenate([jnp.where(node == node_row, plane, 0.0) for plane in planes], axis=0)
    pick_row = lax.broadcasted_iota(jnp.int32, (rows, 128), 0)
    pick_lane = lax.broadcasted_iota(jnp.int32, (rows, 128), 1)
    pick = jnp.where(lax.rem(pick_row, length_z) == pick_lane, 1.0, 0.0).astype(BF16)
    masked_hi, masked_lo = split(masked)
    flat = jnp.dot(masked_hi, pick, preferred_element_type=F32) + jnp.dot(
        masked_lo, pick, preferred_element_type=F32
    )
    bundle = flat[0:8]
    tiles = 4 * length_x // 8
    for tile in range(1, tiles):
        bundle = bundle + pltpu.roll(flat[tile * 8 : tile * 8 + 8], tile * length_z, 1)
    pull_send[...] = bundle
    if stepwise:
        pl.semaphore_wait(step_two, len(sides + DIRS))
    reach = 2 * REACH + 1
    folded = n_span == 2 * REACH
    offsets = [
        (dx, dz)
        for dx in range(-REACH, REACH + 1)
        for dz in range(-REACH, REACH + 1)
        if (dx, dz) != (0, 0) and not (folded and dz == REACH)
    ]
    for dx, dz in sorted(offsets, key=lambda pair: -abs(pair[0]) - abs(pair[1])):
        slot = (REACH - dx) * reach + (REACH - dz)
        remote(pull_send, pull_got.at[slot], pull_ss, pull_rs, at(dx, dz)).start()

    add_faces(0)
    operate(1, 1)
    send_faces(1)
    for c in range(3):
        field[2, c] = local[1, c]
    loaded("words", "weights")
    lines_rows = jnp.concatenate([lines_mass, lines_stiff], axis=1)
    ends = [lines_rows[0:1], lines_rows[length_y - 1 : length_y]]
    once = [(end[:, :length_y], end[:, length_y:]) for end in ends]
    twice = dot3(
        split(jnp.concatenate([once[0][0], once[0][1], once[1][0], once[1][1]] * 2, axis=0)),
        split(lines_rows),
        NN,
    )
    one_lane = lax.broadcasted_iota(jnp.int32, (1, length_y), 1)
    zero = jnp.zeros((1, length_y), F32)
    images = []
    for side in range(2):
        tip = jnp.where(one_lane == side * (length_y - 1), 1.0, 0.0)
        by_mass, by_stiff = twice[2 * side : 2 * side + 1], twice[2 * side + 1 : 2 * side + 2]
        rows_of = [
            (tip, zero, zero),
            (zero, once[side][0], zero),
            (zero, once[side][1], zero),
            (zero, zero, by_mass[:, :length_y]),
            (zero, zero, by_stiff[:, :length_y]),
            (zero, zero, by_mass[:, length_y:]),
            (zero, zero, by_stiff[:, length_y:]),
        ]
        for entry in rows_of:
            image = jnp.concatenate(entry, axis=1)
            images.append(jnp.broadcast_to(image, (length_z, 3 * length_y)))
        images.append(jnp.zeros((128 - 7 * length_z, 3 * length_y), F32))
    images = split(jnp.concatenate(images, axis=0))
    words_x_parts = (words[0, :, : reach * length_x], words[1, :, : reach * length_x])
    words_z_parts = (words[2], words[3])

    settle(pull_ss, pull_rs, pull_got.at[pl.ds(0, len(offsets))])
    small_lane = lax.broadcasted_iota(jnp.int32, (8, 128), 1) // length_z
    spans = []
    for ix in range(reach):
        pieces = [
            bundle
            if (ix, iz) == (REACH, REACH)
            else pull_got[ix * reach + (reach - 1 if folded and iz == 0 else iz)]
            for iz in range(reach)
        ]
        for tile in range(tiles):
            line = jnp.zeros((8, 128), F32)
            for iz in range(reach):
                shift = ((iz - tile) * length_z) % 128
                moved = pltpu.roll(pieces[iz], shift, 1) if shift else pieces[iz]
                line = jnp.where(small_lane == iz, moved, line)
            spans.append(line)
    along_z = dot3(split(jnp.concatenate(spans, axis=0)), words_z_parts, NT)
    by_plane = []
    for plane in range(4):
        by_plane.append(
            jnp.concatenate(
                [
                    along_z[(ix * 4 + plane) * length_x : (ix * 4 + plane + 1) * length_x]
                    for ix in range(reach)
                ],
                axis=0,
            )
        )
    both_ways = dot3(words_x_parts, split(jnp.concatenate(by_plane, axis=1)), NN)
    block_lane = lax.broadcasted_iota(jnp.int32, (length_x, 128), 1) // length_z
    keep_row = lax.rem(lax.broadcasted_iota(jnp.int32, (rows, 256), 0), length_z)
    keep_lane = lax.rem(lax.broadcasted_iota(jnp.int32, (rows, 256), 1), length_z)
    tractions = []
    for index in range(2):
        blocks = []
        for side in range(2):
            plane = index * 2 + side
            total = jnp.zeros((length_x, 128), F32)
            for block, word_x, word_z in TERMS:
                piece = both_ways[
                    word_x * length_x : (word_x + 1) * length_x, plane * 128 : plane * 128 + 128
                ]
                shift = ((block - word_z) * length_z) % 128
                moved = pltpu.roll(piece, shift, 1) if shift else piece
                total = total + jnp.where(block_lane == block, moved, 0.0)
            blocks.append(total)
        wide = jnp.concatenate(blocks, axis=1)
        tall = jnp.concatenate(
            [jnp.broadcast_to(wide[x : x + 1], (length_z, 256)) for x in range(length_x)], axis=0
        )
        tall = jnp.where(keep_row == keep_lane, tall, 0.0)
        tractions.append(dot3(split(tall), images, NN))
    add_faces(1)
    t1, t2 = shifts
    for c in range(3):
        chain = [field[level, c] for level in range(3)]
        if c != 1:
            taus = tractions[c // 2]
            chain = [
                chain[level] + taus[:, level * length_y : (level + 1) * length_y]
                for level in range(3)
            ]
        v1 = chain[1] - t1 * chain[0]
        field[0, c] = chain[0]
        field[1, c] = v1
        field[2, c] = chain[2] - t1 * chain[1] - t2 * v1
    operate(2, 2)
    for newest in range(3):
        inner_products(newest)
    for c in range(3):
        inner(6, c, field[2, c] * columns[3] * local[2, c])

    total_rows = parts.shape[0]
    r_iota = lax.broadcasted_iota(jnp.int32, (total_rows, 128), 0)
    l_iota = lax.broadcasted_iota(jnp.int32, (total_rows, 128), 1)
    diagonal = r_iota == l_iota
    end_lane = lax.broadcasted_iota(jnp.int32, (total_rows, 128), 1)
    shared = jnp.logical_or(end_lane % 8 == 0, end_lane % 8 == 7)
    tips = jnp.logical_or(end_lane == 0, end_lane == length_y - 1)
    weight_y = jnp.where(jnp.logical_and(shared, jnp.logical_not(tips)), 0.5, 1.0)
    summed = jnp.sum(parts[...] * weight_y, axis=1, keepdims=True)
    row = jnp.sum(jnp.where(diagonal, summed, 0.0), axis=0, keepdims=True)

    def gather_sum(stage, row, count, got, ss, rs, place):
        sum_send[stage : stage + 1, :] = row
        for k in range(1, count):
            remote(
                sum_send.at[pl.ds(stage, 1), :], got.at[pl.ds(k - 1, 1), :], ss, rs, place(k)
            ).start()
        settle(ss, rs, got)
        return row + jnp.sum(got[...], axis=0, keepdims=True)

    if single:
        every = n_wall * n_span
        row = gather_sum(
            0, row, every, wall_got, wall_ss, wall_rs, lambda k: at(k // n_span, k % n_span)
        )
    else:
        row = gather_sum(0, row, n_wall, wall_got, wall_ss, wall_rs, lambda k: at(k, 0))
        row = gather_sum(1, row, n_span, span_got, span_ss, span_rs, lambda k: at(0, k))
    totals = jnp.sum(jnp.where(diagonal, row, 0.0), axis=1, keepdims=True)
    m00, m01, m11, m02, m12, m22, e22 = [totals[q * 8 : q * 8 + 8, :] for q in range(7)]
    t1, t2 = shifts
    a00 = m01 + t1 * m00
    a01 = m11 + t1 * m01
    a02 = m12 + t1 * m02
    a11 = m12 + t2 * m11
    a12 = m22 + t2 * m12
    l10 = a01 / a00
    l20 = a02 / a00
    d1 = a11 - l10 * a01
    u12 = a12 - l10 * a02
    l21 = u12 / d1
    d2 = e22 - l20 * a02 - l21 * u12
    y1 = m01 - l10 * m00
    y2 = m02 - l20 * m00 - l21 * y1
    x2 = y2 / d2
    x1 = y1 / d1 - l21 * x2
    x0 = m00 / a00 - l10 * x1 - l20 * x2
    for index, value in enumerate((x0, x1, x2)):
        factors[index] = jnp.broadcast_to(value, (8, 128))


def combine(field, factors, neumann_in, out, neumann, stage, sems):
    small = pltpu.make_async_copy(neumann_in, neumann, sems.at[3])
    small.start()
    copies = []
    for c in range(3):
        result = factors[0, c : c + 1] * field[0, c]
        for level in range(1, 3):
            result += factors[level, c : c + 1] * field[level, c]
        stage[c] = result.reshape(stage.shape[1:])
        copy = pltpu.make_async_copy(stage.at[c], out.at[c], sems.at[c])
        copy.start()
        copies.append(copy)
    for copy in copies:
        copy.wait()
    small.wait()


def body(n_wall, n_span, velocity_old, heights, owner_device, owner_element, ref_coords, roughness):
    sizes = velocity_old.shape[1:]
    length_x, length_z, length_y = sizes
    rows = length_x * length_z
    points = owner_device.shape[0]
    plane, lines, columns, words_x, words_z = tables(*sizes)
    every = n_wall * n_span
    first = every if every <= SINGLE_STAGE else n_wall
    faces = -(-(6 * (length_x + length_z) + 12) // 8) * 8
    vmem = pl.BlockSpec(memory_space=pltpu.VMEM)
    hbm = pl.BlockSpec(memory_space=pltpu.HBM)
    operands = (
        velocity_old,
        heights.reshape(1, -1),
        owner_device.reshape(1, -1),
        owner_element.reshape(1, -1),
        ref_coords,
        roughness.reshape(1, -1),
        jnp.stack(split_np(plane)),
        jnp.asarray(lines, F32),
        jnp.asarray(columns, F32),
        jnp.stack(split_np(words_x) + split_np(words_z)),
    )
    dma = pltpu.SemaphoreType.DMA
    field, factors, neumann = pl.pallas_call(
        functools.partial(kernel, n_wall, n_span, sizes),
        out_shape=(
            pltpu.VMEM((3, 3, rows, length_y), F32),
            pltpu.VMEM((3, 8, 128), F32),
            pltpu.VMEM((2, points), F32),
        ),
        in_specs=[hbm] * 10,
        out_specs=(vmem, vmem, vmem),
        scratch_shapes=[pltpu.VMEM(value.shape, value.dtype) for value in operands]
        + [
            dma((11,)),
            pltpu.VMEM((2, 64, length_y), F32),
            pltpu.VMEM((2, 2, 64, length_y), F32),
            pltpu.VMEM((3, 3, rows, length_y), F32),
            pltpu.VMEM((ROUNDS, faces, length_y), F32),
            pltpu.VMEM((ROUNDS, faces, length_y), F32),
            pltpu.VMEM((56, length_y), F32),
            pltpu.VMEM((2, 128), F32),
            pltpu.VMEM((first - 1, 128), F32),
            pltpu.VMEM((n_span - 1, 128), F32),
            pltpu.VMEM((8, 128), F32),
            pltpu.VMEM((25, 8, 128), F32),
            dma,
            dma,
            dma,
            dma,
            dma((ROUNDS,)),
            dma((ROUNDS,)),
            dma,
            dma,
            dma,
            dma,
            pltpu.SemaphoreType.REGULAR,
            pltpu.SemaphoreType.REGULAR,
        ],
        compiler_params=pltpu.CompilerParams(
            collective_id=0, has_side_effects=True, vmem_limit_bytes=VMEM_LIMIT
        ),
    )(*[pltpu.with_memory_space_constraint(value, pltpu.HBM) for value in operands])
    return pl.pallas_call(
        combine,
        out_shape=(
            jax.ShapeDtypeStruct(velocity_old.shape, F32),
            jax.ShapeDtypeStruct((2, points), F32),
        ),
        in_specs=[vmem] * 3,
        out_specs=(hbm, hbm),
        scratch_shapes=[pltpu.VMEM(velocity_old.shape, F32), dma((4,))],
        compiler_params=pltpu.CompilerParams(vmem_limit_bytes=VMEM_LIMIT),
    )(field, factors, neumann)


def solution(mesh):
    placed = (
        P(None, "wall", "span", None),
        P(),
        P(("wall", "span"), None),
        P(("wall", "span"), None),
        P(None, ("wall", "span")),
        P(("wall", "span")),
    )
    return jax.shard_map(
        functools.partial(body, mesh.shape["wall"], mesh.shape["span"]),
        mesh=mesh,
        in_specs=placed,
        out_specs=(P(None, "wall", "span", None), P(None, ("wall", "span"))),
        check_vma=False,
    )
```

```python
import functools

import jax
import jax.numpy as jnp
import numpy as np
from jax import lax
from jax.experimental import pallas as pl
from jax.experimental.pallas import tpu as pltpu
from jax.sharding import PartitionSpec as P

GLL_NODES = (
    -1.0,
    -0.8717401485096066,
    -0.5917001814331423,
    -0.2092992179024789,
    0.2092992179024789,
    0.5917001814331423,
    0.8717401485096066,
    1.0,
)
GLL_WEIGHTS = (
    0.03571428571428571,
    0.2107042271435061,
    0.3411226924835044,
    0.4124587946587038,
    0.4124587946587038,
    0.3411226924835044,
    0.2107042271435061,
    0.03571428571428571,
)
viscosity = 0.02
inverse_step = 20.0
karman = 0.41
sample_height = 0.1
speed_floor = 0.01
element_dx = 0.05
element_dz = 0.13
NEAR = 2
ROUNDS = 2
REACH = 2
TERMS = (
    (0, 0, 0),
    (1, 1, 2),
    (1, 2, 1),
    (2, 2, 2),
    (3, 3, 6),
    (3, 4, 5),
    (3, 5, 4),
    (3, 6, 3),
    (4, 4, 6),
    (4, 6, 4),
    (5, 5, 6),
    (5, 6, 5),
    (6, 6, 6),
)
SINGLE_STAGE = 64
VMEM_LIMIT = 32 * 2**20
MESH = pl.DeviceIdType.MESH
F32 = jnp.float32
BF16 = jnp.bfloat16


def stiffness_table():
    points = np.array(GLL_NODES)
    weights = np.array(GLL_WEIGHTS)
    previous = np.ones(8)
    current = points.copy()
    for degree in range(1, 7):
        previous, current = (
            current,
            ((2 * degree + 1) * points * current - degree * previous) / (degree + 1),
        )
    derivative = np.zeros((8, 8))
    for target in range(8):
        for source in range(8):
            if target != source:
                derivative[target, source] = (
                    current[target] / current[source] / (points[target] - points[source])
                )
    derivative[0, 0] = -14.0
    derivative[7, 7] = 14.0
    return derivative.T @ (weights[:, None] * derivative)


def join_matrix(length):
    joined = np.eye(length)
    for left in range(7, length - 1, 8):
        joined[left, left + 1] = 1.0
        joined[left + 1, left] = 1.0
    return joined


def face_weights(length, open_ends):
    values = np.ones(length)
    position = np.arange(length) % 8
    values[(position == 0) | (position == 7)] = 0.5
    if open_ends:
        values[0] = 1.0
        values[-1] = 1.0
    return values


def split_np(matrix):
    single = jnp.asarray(matrix, F32)
    high = single.astype(BF16)
    low = (jnp.asarray(matrix, F32) - high.astype(F32)).astype(BF16)
    return high, low


def tables(length_x, length_z, length_y):
    weights = np.array(GLL_WEIGHTS)
    stiffness = stiffness_table()
    count_x, count_z, count_y = length_x // 8, length_z // 8, length_y // 8
    mass_x = np.tile(0.5 * element_dx * weights, count_x)
    mass_z = np.tile(0.5 * element_dz * weights, count_z)
    stiff_x = np.kron(np.eye(count_x), stiffness * (2.0 / element_dx))
    stiff_z = np.kron(np.eye(count_z), stiffness * (2.0 / element_dz))
    mass_xz = np.kron(mass_x, mass_z)
    join_xz = np.kron(join_matrix(length_x), join_matrix(length_z))
    join_y = join_matrix(length_y)
    plane = viscosity * (
        np.kron(stiff_x, np.diag(mass_z)) + np.kron(np.diag(mass_x), stiff_z)
    ) + inverse_step * np.diag(mass_xz)
    plane = join_xz @ plane
    mass_plane = join_xz @ mass_xz
    lines_mass = np.tile(0.5 * weights, count_y)[:, None] * join_y
    lines_stiff = viscosity * 2.0 * (np.kron(np.eye(count_y), stiffness) @ join_y)
    lines = np.stack([lines_mass, lines_stiff])
    ring_x = join_matrix(length_x) @ mass_x
    ring_z = join_matrix(length_z) @ mass_z
    ring_x[0] *= 2.0
    ring_x[-1] *= 2.0
    ring_z[0] *= 2.0
    ring_z[-1] *= 2.0
    assembled = inverse_step * np.kron(ring_x, ring_z)
    inner_x = face_weights(length_x, True)
    inner_z = face_weights(length_z, True)
    outer_x = face_weights(length_x, False)
    outer_z = face_weights(length_z, False)
    columns = np.stack(
        [assembled, mass_plane, np.kron(outer_x, outer_z), np.kron(inner_x, inner_z)]
    )
    columns = columns[:, :, None] * np.ones(length_y)[None, None]
    reach = 2 * REACH + 1

    def words(length, mass, stiff, extra):
        size = reach * length
        join = join_matrix(size)
        light = join @ np.diag(np.tile(mass, reach))
        heavy = viscosity * join @ np.kron(np.eye(size // 8), stiff) + extra * light
        chains = [
            light,
            heavy @ light,
            light @ light,
            heavy @ heavy @ light,
            heavy @ light @ light,
            light @ heavy @ light,
            light @ light @ light,
        ]
        middle = REACH * length
        chains = [chain[middle : middle + length] for chain in chains]
        return np.concatenate(chains + [np.zeros((128 - 7 * length, size))], axis=0)

    words_x = words(length_x, mass_x, stiffness * (2.0 / element_dx), 0.0)
    words_z = words(length_z, mass_z, stiffness * (2.0 / element_dz), inverse_step)
    full = range(REACH - 1, REACH + 2)
    half = 4 * length_x
    turned = words_z.T
    along_z = np.concatenate(
        [np.tile(turned[iz * length_z : (iz + 1) * length_z], (8, 1)) for iz in full]
        + [np.tile(turned[row : row + 1], (half, 1)) for row in (2 * REACH * length_z, length_z - 1)],
        axis=0,
    )
    ends = [2 * REACH * length_x] * 4 + [length_x - 1] * 4
    along_x = np.concatenate(
        [words_x[:, (REACH - 1) * length_x : (REACH + 2) * length_x], words_x[:, ends]]
        + [np.zeros((128, 8))],
        axis=1,
    )
    return plane, lines, columns, along_x, along_z


def split(value):
    high = value.astype(BF16)
    low = (value - high.astype(F32)).astype(BF16)
    return high, low


def dot3(left, right, dims):
    def one(a, b):
        return lax.dot_general(a, b, (dims, ((), ())), preferred_element_type=F32)

    return one(left[0], right[0]) + (one(left[0], right[1]) + one(left[1], right[0]))


NN = ((1,), (0,))
NT = ((1,), (1,))
TN = ((0,), (0,))
DIRS = ((1, 1), (1, -1), (-1, 1), (-1, -1))


def lagrange_rows(coord):
    points = np.array(GLL_NODES)
    scale = 1.0 / np.prod(points[:, None] - points[None, :] + np.eye(8), axis=1)
    shape = (8, coord.shape[1])
    node = lax.broadcasted_iota(jnp.int32, shape, 0)
    total = jnp.zeros(shape, F32)
    for a in range(8):
        total = jnp.where(node == a, F32(scale[a]), total)
    for b in range(8):
        total = total * jnp.where(node == b, F32(1.0), coord - F32(points[b]))
    return total


def kernel(
    n_wall,
    n_span,
    sizes,
    vel_in,
    heights_in,
    owner_in,
    element_in,
    coords_in,
    roughness_in,
    plane_in,
    lines_in,
    columns_in,
    along_x_in,
    along_z_in,
    field,
    factors,
    neumann,
    vel,
    heights,
    owner,
    element,
    coords,
    roughness,
    sheet,
    lines,
    columns,
    along_x,
    along_z,
    load_sem,
    near,
    near_got,
    local,
    face_send,
    face_got,
    parts,
    sum_send,
    wall_got,
    span_got,
    pull_send,
    edge_send,
    pull_got,
    pull_ss,
    pull_rs,
    near_ss,
    near_rs,
    face_ss,
    face_rs,
    wall_ss,
    wall_rs,
    span_ss,
    span_rs,
    step_one,
    step_two,
):
    length_x, length_z, length_y = sizes
    rows = length_x * length_z
    count_z, count_y = length_z // 8, length_y // 8
    w = lax.axis_index("wall")
    s = lax.axis_index("span")

    def at(dx, dz):
        return (lax.rem(w + (dx + n_wall), n_wall), lax.rem(s + (dz + n_span), n_span))

    loads = {
        name: pltpu.make_async_copy(source, target, load_sem.at[index])
        for index, (name, source, target) in enumerate(
            (
                ("vel", vel_in, vel),
                ("heights", heights_in, heights),
                ("lines", lines_in, lines),
                ("scale", columns_in.at[pl.ds(0, 2)], columns.at[pl.ds(0, 2)]),
                ("plane", plane_in, sheet),
                ("coords", coords_in, coords),
                ("owner", owner_in, owner),
                ("element", element_in, element),
                ("roughness", roughness_in, roughness),
                ("along_x", along_x_in, along_x),
                ("along_z", along_z_in, along_z),
                ("weights", columns_in.at[pl.ds(2, 2)], columns.at[pl.ds(2, 2)]),
            )
        )
    }
    for load in loads.values():
        load.start()

    def loaded(*names):
        for name in names:
            loads[name].wait()

    single = n_wall * n_span <= SINGLE_STAGE
    stepwise = single and 3 <= n_wall <= 4 * REACH and 3 <= n_span <= 4 * REACH
    across_wall = ((1, 0), (-1, 0))
    if stepwise:
        greeted = across_wall + tuple((0, k) for k in range(1, n_span))
    elif single:
        greeted = [divmod(k, n_span) for k in range(1, n_wall * n_span)]
    else:
        greeted = [(k, 0) for k in range(1, n_wall)] + [(0, k) for k in range(1, n_span)]
        greeted += sorted(
            {
                ((dx + n_wall) % n_wall, (dz + n_span) % n_span)
                for dx in range(-REACH, REACH + 1)
                for dz in range(-REACH, REACH + 1)
            }
            - {(0, 0)}
            - set(greeted)
        )
    barrier = pltpu.get_barrier_semaphore()

    def greet(semaphore, places):
        for dx, dz in places:
            pl.semaphore_signal(semaphore, inc=1, device_id=at(dx, dz), device_id_type=MESH)

    greet(barrier, greeted)

    loaded("vel")
    lane = lax.broadcasted_iota(jnp.int32, (64, length_y), 1)
    groups = (length_x // 8) * count_z
    for index, comp in enumerate((0, 2)):
        packed = jnp.zeros((64, length_y), F32)
        for group in range(groups):
            ex, ez = group // count_z, group % count_z
            block = vel[comp, pl.ds(ex * 8, 8), pl.ds(ez * 8, 8), :].reshape(64, length_y)
            moved = pltpu.roll(block, (group * 32 + 16) % length_y, 1)
            packed = jnp.where(lane // 32 == group, moved, packed)
        near[index] = packed
    def remote(src, dst, ss, rs, where):
        return pltpu.make_async_remote_copy(
            src_ref=src,
            dst_ref=dst,
            send_sem=ss,
            recv_sem=rs,
            device_id=where,
            device_id_type=MESH,
        )

    near_copies = []
    for slot, dx in enumerate((1, -1)):
        copy = remote(near, near_got.at[slot], near_ss, near_rs, at(dx, 0))
        near_copies.append(copy)

    def enter():
        pl.semaphore_wait(barrier, len(greeted))
        for copy in near_copies:
            copy.start()
        if stepwise:
            greet(step_one, across_wall)

    if stepwise:
        enter()
    loaded("heights", "lines", "scale", "plane")

    layer_of = lax.broadcasted_iota(jnp.int32, (length_y, count_y), 0) // 8
    layer = lax.broadcasted_iota(jnp.int32, (length_y, count_y), 1)
    height_row = heights[...]
    height = jnp.sum(jnp.where(layer_of == layer, height_row, 0.0), axis=1, keepdims=True)
    lines_mass = height * lines[0]
    lines_stiff = lines[1] / height
    stiff_hi, stiff_lo = split(lines_stiff)
    lines_packed = jnp.concatenate(
        [
            jnp.concatenate([stiff_hi, stiff_lo], axis=1),
            jnp.concatenate([stiff_hi, jnp.zeros_like(stiff_lo)], axis=1),
        ],
        axis=0,
    )
    bound = jnp.max(0.1535 * height_row + 0.000182 / height_row, axis=1, keepdims=True)
    shifts = (0.15 * bound, 0.85 * bound)

    mass_row = jnp.sum(lines_mass, axis=0, keepdims=True)
    scale = columns[0] * mass_row
    for c in range(3):
        field[0, c] = vel[c].reshape(rows, length_y) * scale

    face_rows = []
    for slot, (dx, dz) in enumerate(DIRS + ((0, 1), (0, -1), (1, 0), (-1, 0))):
        size = 3 * (1 if dx and dz else length_z if dx else length_x)
        face_rows.append((sum(entry[1] for entry in face_rows), size, dx, dz))
    face_total = sum(entry[1] for entry in face_rows)

    def corner(dx, dz):
        return (rows - length_z if dx == 1 else 0) + (length_z - 1 if dz == 1 else 0)

    def face_part(slot, c, dx, dz):
        first, size = face_rows[slot][0] + c * (face_rows[slot][1] // 3), face_rows[slot][1] // 3
        if dx and dz:
            rows_of = pl.ds(corner(dx, dz), 1)
        elif dx:
            rows_of = pl.ds(rows - length_z if dx == 1 else 0, length_z)
        else:
            rows_of = pl.ds(length_z - 1 if dz == 1 else 0, length_x, stride=length_z)
        return pl.ds(first, size), rows_of

    def send_faces(turn):
        for c in range(3):
            for slot, (_, _, dx, dz) in enumerate(face_rows):
                packed_rows, rows_of = face_part(slot, c, dx, dz)
                face_send[turn, packed_rows, :] = local[turn, c, rows_of, :]
        first_turn = turn == 0 and stepwise
        if turn == 0 and not stepwise:
            enter()
        for corners in (False, True) if first_turn else (True, False):
            if corners and first_turn:
                pl.semaphore_wait(step_one, len(across_wall))
                greet(step_two, across_wall)
            for first, size, dx, dz in face_rows:
                if bool(dx and dz) == corners:
                    part = (turn, pl.ds(first, size), slice(None))
                    remote(
                        face_send.at[part],
                        face_got.at[part],
                        face_ss.at[turn],
                        face_rs.at[turn],
                        at(dx, dz),
                    ).start()

    def settle(ss, rs, ref):
        for semaphore in (rs, ss):
            pltpu.make_async_copy(ref, ref, semaphore).wait()

    def add_faces(turn):
        settle(face_ss.at[turn], face_rs.at[turn], face_got.at[turn, pl.ds(0, face_total), :])
        for c in range(3):
            for slot, (_, _, dx, dz) in enumerate(face_rows):
                packed_rows, rows_of = face_part(slot, c, -dx, -dz)
                field[turn + 1, c, rows_of, :] = (
                    field[turn + 1, c, rows_of, :] + face_got[turn, packed_rows, :]
                )

    def inner(quantity, c, product):
        parts[quantity * 8 + c : quantity * 8 + c + 1, :] = jnp.sum(
            product, axis=0, keepdims=True
        )

    def operate(source, target):
        highs, lows = zip(*[split(field[source, c]) for c in range(3)])
        along_y = jnp.dot(
            jnp.concatenate(
                [jnp.concatenate([high, low], axis=1) for high, low in zip(highs, lows)], axis=0
            ),
            lines_packed,
            preferred_element_type=F32,
        )
        across = jnp.dot(
            sheet[0], jnp.concatenate(highs + lows, axis=1), preferred_element_type=F32
        )
        across_low = jnp.dot(sheet[1], jnp.concatenate(highs, axis=1), preferred_element_type=F32)
        for c in range(3):
            here = slice(c * length_y, (c + 1) * length_y)
            also = slice((3 + c) * length_y, (4 + c) * length_y)
            flat = across[:, here] + (across[:, also] + across_low[:, here])
            tall = along_y[c * rows : (c + 1) * rows]
            tall = tall[:, :length_y] + tall[:, length_y:]
            local[target, c] = flat * mass_row + tall * columns[1]

    slots = {(0, 0): 0, (0, 1): 1, (1, 1): 2, (0, 2): 3, (1, 2): 4, (2, 2): 5}

    def inner_products(newest):
        for c in range(3):
            weighted = field[newest, c] * columns[2]
            for other in range(newest + 1):
                inner(slots[(other, newest)], c, weighted * field[other, c])

    operate(0, 0)
    send_faces(0)
    for c in range(3):
        field[1, c] = local[0, c]
    parts[...] = jnp.zeros_like(parts)

    loaded("coords", "owner", "element", "roughness")
    points = owner.shape[1]
    row_x = lagrange_rows(coords[0:1, :])
    row_z = lagrange_rows(coords[1:2, :])
    row_y = lagrange_rows(coords[2:3, :])
    cross = jnp.concatenate([row_x[a : a + 1] * row_z for a in range(8)], axis=0)
    distance = lax.rem(owner[...] - w + n_wall, n_wall)
    from_next = distance == 1
    from_prev = distance == n_wall - 1
    own = jnp.logical_not(jnp.logical_or(from_next, from_prev))
    spread = jnp.concatenate(
        [jnp.where(mask, cross, 0.0) for mask in (own, from_prev, from_next)], axis=0
    )
    n_row = lax.broadcasted_iota(jnp.int32, (length_y, points), 0)
    within = (n_row % 32) // 8
    layer_y = jnp.where(within < NEAR, within + (count_y - NEAR), within - NEAR)
    wanted = (n_row // 32) * count_y + layer_y == element[...]
    along = jnp.where(wanted, jnp.concatenate([row_y] * (length_y // 8), axis=0), 0.0)
    spread = split(spread)

    settle(near_ss, near_rs, near_got)

    sampled = []
    for index in range(2):
        sources = jnp.concatenate(
            [near[index], near_got[0, index], near_got[1, index]], axis=0
        )
        values = dot3(split(sources), spread, TN)
        sampled.append(jnp.sum(values * along, axis=0, keepdims=True))
    stream, spanwise = sampled
    speed = jnp.sqrt(stream * stream + spanwise * spanwise + speed_floor)
    drag = karman / jnp.log(sample_height / roughness[...])
    factor = -(drag * drag * speed / viscosity)
    gradient = (factor * stream, factor * spanwise)
    neumann[0:1, :] = gradient[0]
    neumann[1:2, :] = gradient[1]

    planes = []
    for index in range(2):
        pull = viscosity * gradient[index]
        planes += [pull[:, :rows], pull[:, rows:]]
    node = lax.broadcasted_iota(jnp.int32, (length_x, rows), 1) // length_z
    node_row = lax.broadcasted_iota(jnp.int32, (length_x, rows), 0)
    masked = jnp.concatenate([jnp.where(node == node_row, plane, 0.0) for plane in planes], axis=0)
    pick_row = lax.rem(lax.broadcasted_iota(jnp.int32, (rows, 256), 0), length_z)
    pick_lane = lax.broadcasted_iota(jnp.int32, (rows, 256), 1)
    wanted_z = jnp.where(
        pick_lane < 128, lax.rem(pick_lane, length_z), (length_z - 1) * ((pick_lane - 128) // 64)
    )
    pick = jnp.where(pick_row == wanted_z, 1.0, 0.0).astype(BF16)
    masked_hi, masked_lo = split(masked)
    flat = jnp.dot(masked_hi, pick, preferred_element_type=F32) + jnp.dot(
        masked_lo, pick, preferred_element_type=F32
    )
    tiles = 4 * length_x // 8
    tile_lane = lax.broadcasted_iota(jnp.int32, (8, 128), 1)
    tile_row = lax.broadcasted_iota(jnp.int32, (8, 128), 0)
    block_of = tile_lane // length_z
    bundle = jnp.zeros((8, 128), F32)
    for tile in range(tiles):
        bundle = jnp.where(block_of == tile, flat[tile * 8 : tile * 8 + 8, :128], bundle)
    pull_send[...] = bundle
    flat_row = lax.broadcasted_iota(jnp.int32, (64, 128), 0)
    flat_lane = lax.broadcasted_iota(jnp.int32, (64, 128), 1)
    ends_x = lax.rem(flat_lane, 64) // length_z * length_x + (length_x - 1) * (flat_lane // 64)
    edge_send[0:1, :] = jnp.sum(
        jnp.where(lax.rem(flat_lane, 64) == flat_row, flat[:, 128:], 0.0), axis=0, keepdims=True
    )
    edge_send[1:2, :] = jnp.sum(
        jnp.where(flat_row == ends_x, flat[:, :128], 0.0), axis=0, keepdims=True
    )
    if stepwise:
        pl.semaphore_wait(step_two, len(across_wall))
    reach = 2 * REACH + 1
    offsets = [
        (dx, dz)
        for dx in range(-REACH, REACH + 1)
        for dz in range(-REACH, REACH + 1)
        if (dx, dz) != (0, 0)
    ]
    nearby = [place for place in offsets if max(abs(place[0]), abs(place[1])) < REACH]
    remaining = [place for place in offsets if place not in nearby]
    pull_rows = {place: pl.ds(8 * index, 8) for index, place in enumerate(nearby)}
    for index, place in enumerate(remaining):
        pull_rows[place] = pl.ds(8 * len(nearby) + index, 1)
    for dx, dz in sorted(offsets, key=lambda pair: -abs(pair[0]) - abs(pair[1])):
        if (dx, dz) in nearby:
            source = pull_send
        else:
            source = edge_send.at[pl.ds(0 if abs(dz) == REACH else 1, 1), :]
        remote(
            source, pull_got.at[pull_rows[(-dx, -dz)], :], pull_ss, pull_rs, at(dx, dz)
        ).start()

    add_faces(0)
    operate(1, 1)
    send_faces(1)
    for c in range(3):
        field[2, c] = local[1, c]
    loaded("along_x", "along_z", "weights")
    lines_rows = jnp.concatenate([lines_mass, lines_stiff], axis=1)
    ends = [lines_rows[0:1], lines_rows[length_y - 1 : length_y]]
    once = [(end[:, :length_y], end[:, length_y:]) for end in ends]
    twice = dot3(
        split(jnp.concatenate([once[0][0], once[0][1], once[1][0], once[1][1]] * 2, axis=0)),
        split(lines_rows),
        NN,
    )
    one_lane = lax.broadcasted_iota(jnp.int32, (1, length_y), 1)
    zero = jnp.zeros((1, length_y), F32)
    images = []
    for side in range(2):
        by_mass, by_stiff = twice[2 * side : 2 * side + 1], twice[2 * side + 1 : 2 * side + 2]
        moved_tip = jnp.where(one_lane == length_y // 2 - side, 1.0, 0.0)
        rows_of = [
            (zero, moved_tip),
            (zero, once[side][0]),
            (zero, once[side][1]),
            (by_mass[:, :length_y], zero),
            (by_stiff[:, :length_y], zero),
            (by_mass[:, length_y:], zero),
            (by_stiff[:, length_y:], zero),
        ]
        for entry in rows_of:
            image = jnp.concatenate(entry, axis=1)
            images.append(jnp.broadcast_to(image, (length_z, 2 * length_y)))
        images.append(jnp.zeros((128 - 7 * length_z, 2 * length_y), F32))
    images = split(jnp.concatenate(images, axis=0))
    settle(pull_ss, pull_rs, pull_got)
    low_half = tile_lane < 64
    low_rows = tile_row < 4

    def edge(dx, dz):
        return jnp.broadcast_to(pull_got[pull_rows[(dx, dz)], :], (8, 128))

    def both_ends(dx):
        return jnp.where(low_half, edge(dx, REACH), edge(dx, -REACH))

    middle = range(-REACH + 1, REACH)
    spans = []
    for dx in middle:
        ends = both_ends(dx)
        parts_z = [bundle if (dx, dz) == (0, 0) else pull_got[pull_rows[(dx, dz)], :] for dz in middle]
        for tile in range(tiles):
            pieces = [jnp.where(block_of == tile, part, 0.0) for part in parts_z]
            pieces.append(jnp.where(lax.rem(tile_lane, 64) == tile_row + 8 * tile, ends, 0.0))
            spans.append(jnp.concatenate(pieces, axis=1))
    pieces = [
        jnp.where(block_of == tile_row, jnp.where(low_rows, edge(REACH, dz), edge(-REACH, dz)), 0.0)
        for dz in middle
    ]
    corner_lane = lax.rem(tile_row, 4) * length_x + (length_x - 1) * (tile_row // 4)
    ends = jnp.where(low_rows, both_ends(REACH), both_ends(-REACH))
    pieces.append(jnp.where(lax.rem(tile_lane, 64) == corner_lane, ends, 0.0))
    spans.append(jnp.concatenate(pieces, axis=1))
    spans.append(jnp.zeros((8, 512), F32))
    spans_hi, spans_lo = split(jnp.concatenate(spans, axis=0))
    reached = jnp.dot(spans_hi, along_z[...], preferred_element_type=F32)
    reached = (reached[:, :128] + reached[:, 128:]) + jnp.dot(
        spans_lo, along_z[:, :128], preferred_element_type=F32
    )
    by_plane = []
    for plane in range(4):
        kept = [
            reached[ix * 64 + plane * length_x : ix * 64 + (plane + 1) * length_x]
            for ix in range(len(middle))
        ]
        last = reached[64 * len(middle) : 64 * len(middle) + 8]
        kept.append(jnp.where(lax.rem(tile_row, 4) == plane, last, 0.0))
        kept.append(jnp.zeros((8, 128), F32))
        by_plane.append(jnp.concatenate(kept, axis=0))
    stacked_hi, stacked_lo = split(jnp.concatenate(by_plane, axis=1))
    both_ways = jnp.dot(
        along_x[...],
        jnp.concatenate([stacked_hi, stacked_lo, stacked_hi], axis=0),
        preferred_element_type=F32,
    )
    block_lane = lax.broadcasted_iota(jnp.int32, (length_x, 128), 1) // length_z
    keep_row = lax.rem(lax.broadcasted_iota(jnp.int32, (rows, 256), 0), length_z)
    keep_lane = lax.rem(lax.broadcasted_iota(jnp.int32, (rows, 256), 1), length_z)
    wall_lane = lax.broadcasted_iota(jnp.int32, (rows, length_y), 1)
    tractions = []
    for index in range(2):
        blocks = []
        for side in range(2):
            plane = index * 2 + side
            total = jnp.zeros((length_x, 128), F32)
            for block, word_x, word_z in TERMS:
                piece = both_ways[
                    word_x * length_x : (word_x + 1) * length_x, plane * 128 : plane * 128 + 128
                ]
                shift = ((block - word_z) * length_z) % 128
                moved = pltpu.roll(piece, shift, 1) if shift else piece
                total = total + jnp.where(block_lane == block, moved, 0.0)
            blocks.append(total)
        wide = jnp.concatenate(blocks, axis=1)
        tall = jnp.concatenate(
            [jnp.broadcast_to(wide[x : x + 1], (length_z, 256)) for x in range(length_x)], axis=0
        )
        tall = jnp.where(keep_row == keep_lane, tall, 0.0)
        deep = dot3(split(tall), images, NN)
        level_two, shallow = deep[:, :length_y], deep[:, length_y:]
        tip = jnp.logical_or(wall_lane == 0, wall_lane == length_y - 1)
        level_zero = jnp.where(tip, pltpu.roll(shallow, length_y // 2, 1), 0.0)
        outside = jnp.logical_or(wall_lane < length_y // 4, wall_lane >= 3 * length_y // 4)
        level_one = jnp.where(outside, shallow, 0.0)
        tractions.append((level_zero, level_one, level_two))
    add_faces(1)
    t1, t2 = shifts
    for c in range(3):
        chain = [field[level, c] for level in range(3)]
        if c != 1:
            taus = tractions[c // 2]
            chain = [chain[level] + taus[level] for level in range(3)]
        v1 = chain[1] - t1 * chain[0]
        field[0, c] = chain[0]
        field[1, c] = v1
        field[2, c] = chain[2] - t1 * chain[1] - t2 * v1
    operate(2, 2)
    for newest in range(3):
        inner_products(newest)
    for c in range(3):
        inner(6, c, field[2, c] * columns[3] * local[2, c])

    total_rows = parts.shape[0]
    r_iota = lax.broadcasted_iota(jnp.int32, (total_rows, 128), 0)
    l_iota = lax.broadcasted_iota(jnp.int32, (total_rows, 128), 1)
    diagonal = r_iota == l_iota
    end_lane = lax.broadcasted_iota(jnp.int32, (total_rows, 128), 1)
    shared = jnp.logical_or(end_lane % 8 == 0, end_lane % 8 == 7)
    tips = jnp.logical_or(end_lane == 0, end_lane == length_y - 1)
    weight_y = jnp.where(jnp.logical_and(shared, jnp.logical_not(tips)), 0.5, 1.0)
    summed = jnp.sum(parts[...] * weight_y, axis=1, keepdims=True)
    row = jnp.sum(jnp.where(diagonal, summed, 0.0), axis=0, keepdims=True)

    def gather_sum(stage, row, count, got, ss, rs, place):
        sum_send[stage : stage + 1, :] = row
        for k in range(1, count):
            remote(
                sum_send.at[pl.ds(stage, 1), :], got.at[pl.ds(k - 1, 1), :], ss, rs, place(k)
            ).start()
        settle(ss, rs, got)
        return row + jnp.sum(got[...], axis=0, keepdims=True)

    if single:
        every = n_wall * n_span
        row = gather_sum(
            0, row, every, wall_got, wall_ss, wall_rs, lambda k: at(k // n_span, k % n_span)
        )
    else:
        row = gather_sum(0, row, n_wall, wall_got, wall_ss, wall_rs, lambda k: at(k, 0))
        row = gather_sum(1, row, n_span, span_got, span_ss, span_rs, lambda k: at(0, k))
    totals = jnp.sum(jnp.where(diagonal, row, 0.0), axis=1, keepdims=True)
    m00, m01, m11, m02, m12, m22, e22 = [totals[q * 8 : q * 8 + 8, :] for q in range(7)]
    t1, t2 = shifts
    a00 = m01 + t1 * m00
    a01 = m11 + t1 * m01
    a02 = m12 + t1 * m02
    a11 = m12 + t2 * m11
    a12 = m22 + t2 * m12
    l10 = a01 / a00
    l20 = a02 / a00
    d1 = a11 - l10 * a01
    u12 = a12 - l10 * a02
    l21 = u12 / d1
    d2 = e22 - l20 * a02 - l21 * u12
    y1 = m01 - l10 * m00
    y2 = m02 - l20 * m00 - l21 * y1
    x2 = y2 / d2
    x1 = y1 / d1 - l21 * x2
    x0 = m00 / a00 - l10 * x1 - l20 * x2
    for index, value in enumerate((x0, x1, x2)):
        factors[index] = jnp.broadcast_to(value, (8, 128))


def combine(field, factors, neumann_in, out, neumann, stage, sems):
    small = pltpu.make_async_copy(neumann_in, neumann, sems.at[3])
    small.start()
    copies = []
    for c in range(3):
        result = factors[0, c : c + 1] * field[0, c]
        for level in range(1, 3):
            result += factors[level, c : c + 1] * field[level, c]
        stage[c] = result.reshape(stage.shape[1:])
        copy = pltpu.make_async_copy(stage.at[c], out.at[c], sems.at[c])
        copy.start()
        copies.append(copy)
    for copy in copies:
        copy.wait()
    small.wait()


def body(n_wall, n_span, velocity_old, heights, owner_device, owner_element, ref_coords, roughness):
    sizes = velocity_old.shape[1:]
    length_x, length_z, length_y = sizes
    rows = length_x * length_z
    points = owner_device.shape[0]
    plane, lines, columns, along_x, along_z = tables(*sizes)
    along_x_hi, along_x_lo = split_np(along_x)
    every = n_wall * n_span
    first = every if every <= SINGLE_STAGE else n_wall
    faces = -(-(6 * (length_x + length_z) + 12) // 8) * 8
    vmem = pl.BlockSpec(memory_space=pltpu.VMEM)
    hbm = pl.BlockSpec(memory_space=pltpu.HBM)
    operands = (
        velocity_old,
        heights.reshape(1, -1),
        owner_device.reshape(1, -1),
        owner_element.reshape(1, -1),
        ref_coords,
        roughness.reshape(1, -1),
        jnp.stack(split_np(plane)),
        jnp.asarray(lines, F32),
        jnp.asarray(columns, F32),
        jnp.concatenate([along_x_hi, along_x_hi, along_x_lo], axis=1),
        jnp.concatenate(split_np(along_z), axis=1),
    )
    dma = pltpu.SemaphoreType.DMA
    field, factors, neumann = pl.pallas_call(
        functools.partial(kernel, n_wall, n_span, sizes),
        out_shape=(
            pltpu.VMEM((3, 3, rows, length_y), F32),
            pltpu.VMEM((3, 8, 128), F32),
            pltpu.VMEM((2, points), F32),
        ),
        in_specs=[hbm] * 11,
        out_specs=(vmem, vmem, vmem),
        scratch_shapes=[pltpu.VMEM(value.shape, value.dtype) for value in operands]
        + [
            dma((12,)),
            pltpu.VMEM((2, 64, length_y), F32),
            pltpu.VMEM((2, 2, 64, length_y), F32),
            pltpu.VMEM((3, 3, rows, length_y), F32),
            pltpu.VMEM((ROUNDS, faces, length_y), F32),
            pltpu.VMEM((ROUNDS, faces, length_y), F32),
            pltpu.VMEM((56, length_y), F32),
            pltpu.VMEM((2, 128), F32),
            pltpu.VMEM((first - 1, 128), F32),
            pltpu.VMEM((n_span - 1, 128), F32),
            pltpu.VMEM((8, 128), F32),
            pltpu.VMEM((8, 128), F32),
            pltpu.VMEM((80, 128), F32),
            dma,
            dma,
            dma,
            dma,
            dma((ROUNDS,)),
            dma((ROUNDS,)),
            dma,
            dma,
            dma,
            dma,
            pltpu.SemaphoreType.REGULAR,
            pltpu.SemaphoreType.REGULAR,
        ],
        compiler_params=pltpu.CompilerParams(
            collective_id=0, has_side_effects=True, vmem_limit_bytes=VMEM_LIMIT
        ),
    )(*[pltpu.with_memory_space_constraint(value, pltpu.HBM) for value in operands])
    return pl.pallas_call(
        combine,
        out_shape=(
            jax.ShapeDtypeStruct(velocity_old.shape, F32),
            jax.ShapeDtypeStruct((2, points), F32),
        ),
        in_specs=[vmem] * 3,
        out_specs=(hbm, hbm),
        scratch_shapes=[pltpu.VMEM(velocity_old.shape, F32), dma((4,))],
        compiler_params=pltpu.CompilerParams(vmem_limit_bytes=VMEM_LIMIT),
    )(field, factors, neumann)


def solution(mesh):
    placed = (
        P(None, "wall", "span", None),
        P(),
        P(("wall", "span"), None),
        P(("wall", "span"), None),
        P(None, ("wall", "span")),
        P(("wall", "span")),
    )
    return jax.shard_map(
        functools.partial(body, mesh.shape["wall"], mesh.shape["span"]),
        mesh=mesh,
        in_specs=placed,
        out_specs=(P(None, "wall", "span", None), P(None, ("wall", "span"))),
        check_vma=False,
    )
```

```python
import functools

import jax
import jax.numpy as jnp
import numpy as np
from jax import lax
from jax.experimental import pallas as pl
from jax.experimental.pallas import tpu as pltpu
from jax.sharding import PartitionSpec as P

GLL_NODES = (
    -1.0,
    -0.8717401485096066,
    -0.5917001814331423,
    -0.2092992179024789,
    0.2092992179024789,
    0.5917001814331423,
    0.8717401485096066,
    1.0,
)
GLL_WEIGHTS = (
    0.03571428571428571,
    0.2107042271435061,
    0.3411226924835044,
    0.4124587946587038,
    0.4124587946587038,
    0.3411226924835044,
    0.2107042271435061,
    0.03571428571428571,
)
viscosity = 0.02
inverse_step = 20.0
karman = 0.41
sample_height = 0.1
speed_floor = 0.01
element_dx = 0.05
element_dz = 0.13
NEAR = 2
ROUNDS = 2
REACH = 2
TERMS = (
    (0, 0, 0),
    (1, 1, 2),
    (1, 2, 1),
    (2, 2, 2),
    (3, 3, 6),
    (3, 4, 5),
    (3, 5, 4),
    (3, 6, 3),
    (4, 4, 6),
    (4, 6, 4),
    (5, 5, 6),
    (5, 6, 5),
    (6, 6, 6),
)
SINGLE_STAGE = 64
VMEM_LIMIT = 32 * 2**20
MESH = pl.DeviceIdType.MESH
F32 = jnp.float32
BF16 = jnp.bfloat16


def stiffness_table():
    points = np.array(GLL_NODES)
    weights = np.array(GLL_WEIGHTS)
    previous = np.ones(8)
    current = points.copy()
    for degree in range(1, 7):
        previous, current = (
            current,
            ((2 * degree + 1) * points * current - degree * previous) / (degree + 1),
        )
    derivative = np.zeros((8, 8))
    for target in range(8):
        for source in range(8):
            if target != source:
                derivative[target, source] = (
                    current[target] / current[source] / (points[target] - points[source])
                )
    derivative[0, 0] = -14.0
    derivative[7, 7] = 14.0
    return derivative.T @ (weights[:, None] * derivative)


def join_matrix(length):
    joined = np.eye(length)
    for left in range(7, length - 1, 8):
        joined[left, left + 1] = 1.0
        joined[left + 1, left] = 1.0
    return joined


def face_weights(length, open_ends):
    values = np.ones(length)
    position = np.arange(length) % 8
    values[(position == 0) | (position == 7)] = 0.5
    if open_ends:
        values[0] = 1.0
        values[-1] = 1.0
    return values


def split_np(matrix):
    single = jnp.asarray(matrix, F32)
    high = single.astype(BF16)
    low = (jnp.asarray(matrix, F32) - high.astype(F32)).astype(BF16)
    return high, low


def tables(length_x, length_z, length_y):
    weights = np.array(GLL_WEIGHTS)
    stiffness = stiffness_table()
    count_x, count_z, count_y = length_x // 8, length_z // 8, length_y // 8
    mass_x = np.tile(0.5 * element_dx * weights, count_x)
    mass_z = np.tile(0.5 * element_dz * weights, count_z)
    stiff_x = np.kron(np.eye(count_x), stiffness * (2.0 / element_dx))
    stiff_z = np.kron(np.eye(count_z), stiffness * (2.0 / element_dz))
    mass_xz = np.kron(mass_x, mass_z)
    join_xz = np.kron(join_matrix(length_x), join_matrix(length_z))
    join_y = join_matrix(length_y)
    plane = viscosity * (
        np.kron(stiff_x, np.diag(mass_z)) + np.kron(np.diag(mass_x), stiff_z)
    ) + inverse_step * np.diag(mass_xz)
    plane = join_xz @ plane
    mass_plane = join_xz @ mass_xz
    lines_mass = np.tile(0.5 * weights, count_y)[:, None] * join_y
    lines_stiff = viscosity * 2.0 * (np.kron(np.eye(count_y), stiffness) @ join_y)
    lines = np.stack([lines_mass, lines_stiff])
    ring_x = join_matrix(length_x) @ mass_x
    ring_z = join_matrix(length_z) @ mass_z
    ring_x[0] *= 2.0
    ring_x[-1] *= 2.0
    ring_z[0] *= 2.0
    ring_z[-1] *= 2.0
    assembled = inverse_step * np.kron(ring_x, ring_z)
    inner_x = face_weights(length_x, True)
    inner_z = face_weights(length_z, True)
    outer_x = face_weights(length_x, False)
    outer_z = face_weights(length_z, False)
    columns = np.stack(
        [assembled, mass_plane, np.kron(outer_x, outer_z), np.kron(inner_x, inner_z)]
    )
    columns = columns[:, :, None] * np.ones(length_y)[None, None]
    reach = 2 * REACH + 1

    def words(length, mass, stiff, extra):
        size = reach * length
        join = join_matrix(size)
        light = join @ np.diag(np.tile(mass, reach))
        heavy = viscosity * join @ np.kron(np.eye(size // 8), stiff) + extra * light
        chains = [
            light,
            heavy @ light,
            light @ light,
            heavy @ heavy @ light,
            heavy @ light @ light,
            light @ heavy @ light,
            light @ light @ light,
        ]
        middle = REACH * length
        chains = [chain[middle : middle + length] for chain in chains]
        return np.concatenate(chains + [np.zeros((128 - 7 * length, size))], axis=0)

    words_x = words(length_x, mass_x, stiffness * (2.0 / element_dx), 0.0)
    words_z = words(length_z, mass_z, stiffness * (2.0 / element_dz), inverse_step)
    full = range(REACH - 1, REACH + 2)
    half = 4 * length_x
    turned = words_z.T
    along_z = np.concatenate(
        [np.tile(turned[iz * length_z : (iz + 1) * length_z], (8, 1)) for iz in full]
        + [np.tile(turned[row : row + 1], (half, 1)) for row in (2 * REACH * length_z, length_z - 1)],
        axis=0,
    )
    ends = [2 * REACH * length_x] * 4 + [length_x - 1] * 4
    along_x = np.concatenate(
        [words_x[:, (REACH - 1) * length_x : (REACH + 2) * length_x], words_x[:, ends]]
        + [np.zeros((128, 8))],
        axis=1,
    )
    return plane, lines, columns, along_x, along_z


def split(value):
    high = value.astype(BF16)
    low = (value - high.astype(F32)).astype(BF16)
    return high, low


def dot3(left, right, dims):
    def one(a, b):
        return lax.dot_general(a, b, (dims, ((), ())), preferred_element_type=F32)

    return one(left[0], right[0]) + (one(left[0], right[1]) + one(left[1], right[0]))


NN = ((1,), (0,))
NT = ((1,), (1,))
TN = ((0,), (0,))
DIRS = ((1, 1), (1, -1), (-1, 1), (-1, -1))


def lagrange_rows(coord):
    points = np.array(GLL_NODES)
    scale = 1.0 / np.prod(points[:, None] - points[None, :] + np.eye(8), axis=1)
    shape = (8, coord.shape[1])
    node = lax.broadcasted_iota(jnp.int32, shape, 0)
    total = jnp.zeros(shape, F32)
    for a in range(8):
        total = jnp.where(node == a, F32(scale[a]), total)
    for b in range(8):
        total = total * jnp.where(node == b, F32(1.0), coord - F32(points[b]))
    return total


def kernel(
    n_wall,
    n_span,
    sizes,
    vel_in,
    heights_in,
    owner_in,
    element_in,
    coords_in,
    roughness_in,
    plane_in,
    lines_in,
    columns_in,
    along_x_in,
    along_z_in,
    field,
    factors,
    neumann,
    vel,
    heights,
    owner,
    element,
    coords,
    roughness,
    sheet,
    lines,
    columns,
    along_x,
    along_z,
    load_sem,
    near,
    near_got,
    local,
    face_send,
    face_got,
    parts,
    sum_send,
    wall_got,
    span_got,
    pull_send,
    edge_send,
    pull_got,
    pull_ss,
    pull_rs,
    near_ss,
    near_rs,
    face_ss,
    face_rs,
    wall_ss,
    wall_rs,
    span_ss,
    span_rs,
    step_one,
    step_two,
):
    length_x, length_z, length_y = sizes
    rows = length_x * length_z
    count_z, count_y = length_z // 8, length_y // 8
    w = lax.axis_index("wall")
    s = lax.axis_index("span")

    def at(dx, dz):
        return (lax.rem(w + (dx + n_wall), n_wall), lax.rem(s + (dz + n_span), n_span))

    loads = {
        name: pltpu.make_async_copy(source, target, load_sem.at[index])
        for index, (name, source, target) in enumerate(
            (
                ("vel", vel_in, vel),
                ("heights", heights_in, heights),
                ("lines", lines_in, lines),
                ("scale", columns_in.at[pl.ds(0, 2)], columns.at[pl.ds(0, 2)]),
                ("plane", plane_in, sheet),
                ("coords", coords_in, coords),
                ("owner", owner_in, owner),
                ("element", element_in, element),
                ("roughness", roughness_in, roughness),
                ("along_x", along_x_in, along_x),
                ("along_z", along_z_in, along_z),
                ("weights", columns_in.at[pl.ds(2, 2)], columns.at[pl.ds(2, 2)]),
            )
        )
    }
    for load in loads.values():
        load.start()

    def loaded(*names):
        for name in names:
            loads[name].wait()

    single = n_wall * n_span <= SINGLE_STAGE
    stepwise = single and 3 <= n_wall <= 4 * REACH and 3 <= n_span <= 4 * REACH
    across_wall = ((1, 0), (-1, 0))
    if stepwise:
        greeted = across_wall + tuple((0, k) for k in range(1, n_span))
    elif single:
        greeted = [divmod(k, n_span) for k in range(1, n_wall * n_span)]
    else:
        greeted = [(k, 0) for k in range(1, n_wall)] + [(0, k) for k in range(1, n_span)]
        greeted += sorted(
            {
                ((dx + n_wall) % n_wall, (dz + n_span) % n_span)
                for dx in range(-REACH, REACH + 1)
                for dz in range(-REACH, REACH + 1)
            }
            - {(0, 0)}
            - set(greeted)
        )
    barrier = pltpu.get_barrier_semaphore()

    def greet(semaphore, places):
        for dx, dz in places:
            pl.semaphore_signal(semaphore, inc=1, device_id=at(dx, dz), device_id_type=MESH)

    greet(barrier, greeted)

    loaded("vel")
    lane = lax.broadcasted_iota(jnp.int32, (64, length_y), 1)
    groups = (length_x // 8) * count_z
    for index, comp in enumerate((0, 2)):
        packed = jnp.zeros((64, length_y), F32)
        for group in range(groups):
            ex, ez = group // count_z, group % count_z
            block = vel[comp, pl.ds(ex * 8, 8), pl.ds(ez * 8, 8), :].reshape(64, length_y)
            moved = pltpu.roll(block, (group * 32 + 16) % length_y, 1)
            packed = jnp.where(lane // 32 == group, moved, packed)
        near[index] = packed
    def remote(src, dst, ss, rs, where):
        return pltpu.make_async_remote_copy(
            src_ref=src,
            dst_ref=dst,
            send_sem=ss,
            recv_sem=rs,
            device_id=where,
            device_id_type=MESH,
        )

    near_copies = []
    for slot, dx in enumerate((1, -1)):
        copy = remote(near, near_got.at[slot], near_ss, near_rs, at(dx, 0))
        near_copies.append(copy)

    def enter():
        pl.semaphore_wait(barrier, len(greeted))
        for copy in near_copies:
            copy.start()
        if stepwise:
            greet(step_one, across_wall)

    if stepwise:
        enter()
    loaded("heights", "lines", "scale", "plane")

    layer_of = lax.broadcasted_iota(jnp.int32, (length_y, count_y), 0) // 8
    layer = lax.broadcasted_iota(jnp.int32, (length_y, count_y), 1)
    height_row = heights[...]
    height = jnp.sum(jnp.where(layer_of == layer, height_row, 0.0), axis=1, keepdims=True)
    lines_mass = height * lines[0]
    lines_stiff = lines[1] / height
    stiff_hi, stiff_lo = split(lines_stiff)
    lines_packed = jnp.concatenate(
        [
            jnp.concatenate([stiff_hi, stiff_lo], axis=1),
            jnp.concatenate([stiff_hi, jnp.zeros_like(stiff_lo)], axis=1),
        ],
        axis=0,
    )
    bound = jnp.max(0.1535 * height_row + 0.000182 / height_row, axis=1, keepdims=True)
    shifts = (0.15 * bound, 0.85 * bound)

    mass_row = jnp.sum(lines_mass, axis=0, keepdims=True)
    scale = columns[0] * mass_row
    for c in range(3):
        field[0, c] = vel[c].reshape(rows, length_y) * scale

    face_rows = []
    for slot, (dx, dz) in enumerate(DIRS + ((0, 1), (0, -1), (1, 0), (-1, 0))):
        size = 3 * (1 if dx and dz else length_z if dx else length_x)
        face_rows.append((sum(entry[1] for entry in face_rows), size, dx, dz))
    face_total = sum(entry[1] for entry in face_rows)

    def corner(dx, dz):
        return (rows - length_z if dx == 1 else 0) + (length_z - 1 if dz == 1 else 0)

    def face_part(slot, c, dx, dz):
        first, size = face_rows[slot][0] + c * (face_rows[slot][1] // 3), face_rows[slot][1] // 3
        if dx and dz:
            rows_of = pl.ds(corner(dx, dz), 1)
        elif dx:
            rows_of = pl.ds(rows - length_z if dx == 1 else 0, length_z)
        else:
            rows_of = pl.ds(length_z - 1 if dz == 1 else 0, length_x, stride=length_z)
        return pl.ds(first, size), rows_of

    def send_faces(turn):
        for c in range(3):
            for slot, (_, _, dx, dz) in enumerate(face_rows):
                packed_rows, rows_of = face_part(slot, c, dx, dz)
                face_send[turn, packed_rows, :] = local[turn, c, rows_of, :]
        first_turn = turn == 0 and stepwise
        if turn == 0 and not stepwise:
            enter()
        for corners in (False, True) if first_turn else (True, False):
            if corners and first_turn:
                pl.semaphore_wait(step_one, len(across_wall))
                greet(step_two, across_wall)
            for first, size, dx, dz in face_rows:
                if bool(dx and dz) == corners:
                    part = (turn, pl.ds(first, size), slice(None))
                    remote(
                        face_send.at[part],
                        face_got.at[part],
                        face_ss.at[turn],
                        face_rs.at[turn],
                        at(dx, dz),
                    ).start()

    def settle(ss, rs, ref):
        for semaphore in (rs, ss):
            pltpu.make_async_copy(ref, ref, semaphore).wait()

    def add_faces(turn):
        settle(face_ss.at[turn], face_rs.at[turn], face_got.at[turn, pl.ds(0, face_total), :])
        for c in range(3):
            for slot, (_, _, dx, dz) in enumerate(face_rows):
                packed_rows, rows_of = face_part(slot, c, -dx, -dz)
                field[turn + 1, c, rows_of, :] = (
                    field[turn + 1, c, rows_of, :] + face_got[turn, packed_rows, :]
                )

    def inner(quantity, c, product):
        parts[quantity * 8 + c : quantity * 8 + c + 1, :] = jnp.sum(
            product, axis=0, keepdims=True
        )

    def operate(source, target):
        highs, lows = zip(*[split(field[source, c]) for c in range(3)])
        along_y = jnp.dot(
            jnp.concatenate(
                [jnp.concatenate([high, low], axis=1) for high, low in zip(highs, lows)], axis=0
            ),
            lines_packed,
            preferred_element_type=F32,
        )
        across = jnp.dot(
            sheet[0], jnp.concatenate(highs + lows, axis=1), preferred_element_type=F32
        )
        across_low = jnp.dot(sheet[1], jnp.concatenate(highs, axis=1), preferred_element_type=F32)
        for c in range(3):
            here = slice(c * length_y, (c + 1) * length_y)
            also = slice((3 + c) * length_y, (4 + c) * length_y)
            flat = across[:, here] + (across[:, also] + across_low[:, here])
            tall = along_y[c * rows : (c + 1) * rows]
            tall = tall[:, :length_y] + tall[:, length_y:]
            local[target, c] = flat * mass_row + tall * columns[1]

    slots = {(0, 0): 0, (0, 1): 1, (1, 1): 2, (0, 2): 3, (1, 2): 4, (2, 2): 5}

    def inner_products(newest):
        for c in range(3):
            weighted = field[newest, c] * columns[2]
            for other in range(newest + 1):
                inner(slots[(other, newest)], c, weighted * field[other, c])

    operate(0, 0)
    send_faces(0)
    for c in range(3):
        field[1, c] = local[0, c]
    parts[...] = jnp.zeros_like(parts)

    loaded("coords", "owner", "element", "roughness")
    points = owner.shape[1]
    row_x = lagrange_rows(coords[0:1, :])
    row_z = lagrange_rows(coords[1:2, :])
    row_y = lagrange_rows(coords[2:3, :])
    cross = jnp.concatenate([row_x[a : a + 1] * row_z for a in range(8)], axis=0)
    distance = lax.rem(owner[...] - w + n_wall, n_wall)
    from_next = distance == 1
    from_prev = distance == n_wall - 1
    own = jnp.logical_not(jnp.logical_or(from_next, from_prev))
    spread = jnp.concatenate(
        [jnp.where(mask, cross, 0.0) for mask in (own, from_prev, from_next)], axis=0
    )
    n_row = lax.broadcasted_iota(jnp.int32, (length_y, points), 0)
    within = (n_row % 32) // 8
    layer_y = jnp.where(within < NEAR, within + (count_y - NEAR), within - NEAR)
    wanted = (n_row // 32) * count_y + layer_y == element[...]
    along = jnp.where(wanted, jnp.concatenate([row_y] * (length_y // 8), axis=0), 0.0)
    spread = split(spread)

    drag = karman / jnp.log(sample_height / roughness[...])
    drag = drag * drag * (-1.0 / viscosity)

    settle(near_ss, near_rs, near_got)

    sampled = []
    for index in range(2):
        sources = jnp.concatenate(
            [near[index], near_got[0, index], near_got[1, index]], axis=0
        )
        values = dot3(split(sources), spread, TN)
        sampled.append(jnp.sum(values * along, axis=0, keepdims=True))
    stream, spanwise = sampled
    speed = jnp.sqrt(stream * stream + spanwise * spanwise + speed_floor)
    factor = drag * speed
    gradient = (factor * stream, factor * spanwise)
    neumann[0:1, :] = gradient[0]
    neumann[1:2, :] = gradient[1]

    planes = []
    for index in range(2):
        pull = viscosity * gradient[index]
        planes += [pull[:, :rows], pull[:, rows:]]
    node = lax.broadcasted_iota(jnp.int32, (length_x, rows), 1) // length_z
    node_row = lax.broadcasted_iota(jnp.int32, (length_x, rows), 0)
    masked = jnp.concatenate([jnp.where(node == node_row, plane, 0.0) for plane in planes], axis=0)
    pick_row = lax.rem(lax.broadcasted_iota(jnp.int32, (rows, 256), 0), length_z)
    pick_lane = lax.broadcasted_iota(jnp.int32, (rows, 256), 1)
    wanted_z = jnp.where(
        pick_lane < 128, lax.rem(pick_lane, length_z), (length_z - 1) * ((pick_lane - 128) // 64)
    )
    pick = jnp.where(pick_row == wanted_z, 1.0, 0.0).astype(BF16)
    masked_hi, masked_lo = split(masked)
    flat = jnp.dot(masked_hi, pick, preferred_element_type=F32) + jnp.dot(
        masked_lo, pick, preferred_element_type=F32
    )
    tiles = 4 * length_x // 8
    tile_lane = lax.broadcasted_iota(jnp.int32, (8, 128), 1)
    tile_row = lax.broadcasted_iota(jnp.int32, (8, 128), 0)
    block_of = tile_lane // length_z
    bundle = jnp.zeros((8, 128), F32)
    for tile in range(tiles):
        bundle = jnp.where(block_of == tile, flat[tile * 8 : tile * 8 + 8, :128], bundle)
    pull_send[...] = bundle
    flat_row = lax.broadcasted_iota(jnp.int32, (64, 128), 0)
    flat_lane = lax.broadcasted_iota(jnp.int32, (64, 128), 1)
    ends_x = lax.rem(flat_lane, 64) // length_z * length_x + (length_x - 1) * (flat_lane // 64)
    edge_send[0:1, :] = jnp.sum(
        jnp.where(lax.rem(flat_lane, 64) == flat_row, flat[:, 128:], 0.0), axis=0, keepdims=True
    )
    edge_send[1:2, :] = jnp.sum(
        jnp.where(flat_row == ends_x, flat[:, :128], 0.0), axis=0, keepdims=True
    )
    if stepwise:
        pl.semaphore_wait(step_two, len(across_wall))
    reach = 2 * REACH + 1
    offsets = [
        (dx, dz)
        for dx in range(-REACH, REACH + 1)
        for dz in range(-REACH, REACH + 1)
        if (dx, dz) != (0, 0)
    ]
    nearby = [place for place in offsets if max(abs(place[0]), abs(place[1])) < REACH]
    remaining = [place for place in offsets if place not in nearby]
    pull_rows = {place: pl.ds(8 * index, 8) for index, place in enumerate(nearby)}
    for index, place in enumerate(remaining):
        pull_rows[place] = pl.ds(8 * len(nearby) + index, 1)
    for dx, dz in sorted(offsets, key=lambda pair: -abs(pair[0]) - abs(pair[1])):
        if (dx, dz) in nearby:
            source = pull_send
        else:
            source = edge_send.at[pl.ds(0 if abs(dz) == REACH else 1, 1), :]
        remote(
            source, pull_got.at[pull_rows[(-dx, -dz)], :], pull_ss, pull_rs, at(dx, dz)
        ).start()

    add_faces(0)
    operate(1, 1)
    send_faces(1)
    for c in range(3):
        field[2, c] = local[1, c]
    loaded("along_x", "along_z", "weights")
    lines_rows = jnp.concatenate([lines_mass, lines_stiff], axis=1)
    ends = [lines_rows[0:1], lines_rows[length_y - 1 : length_y]]
    once = [(end[:, :length_y], end[:, length_y:]) for end in ends]
    twice = dot3(
        split(jnp.concatenate([once[0][0], once[0][1], once[1][0], once[1][1]] * 2, axis=0)),
        split(lines_rows),
        NN,
    )
    one_lane = lax.broadcasted_iota(jnp.int32, (1, length_y), 1)
    zero = jnp.zeros((1, length_y), F32)
    images = []
    for side in range(2):
        by_mass, by_stiff = twice[2 * side : 2 * side + 1], twice[2 * side + 1 : 2 * side + 2]
        moved_tip = jnp.where(one_lane == length_y // 2 - side, 1.0, 0.0)
        rows_of = [
            (zero, moved_tip),
            (zero, once[side][0]),
            (zero, once[side][1]),
            (by_mass[:, :length_y], zero),
            (by_stiff[:, :length_y], zero),
            (by_mass[:, length_y:], zero),
            (by_stiff[:, length_y:], zero),
        ]
        for entry in rows_of:
            image = jnp.concatenate(entry, axis=1)
            images.append(jnp.broadcast_to(image, (length_z, 2 * length_y)))
        images.append(jnp.zeros((128 - 7 * length_z, 2 * length_y), F32))
    images = split(jnp.concatenate(images, axis=0))
    settle(pull_ss, pull_rs, pull_got)
    low_half = tile_lane < 64
    low_rows = tile_row < 4

    def edge(dx, dz):
        return jnp.broadcast_to(pull_got[pull_rows[(dx, dz)], :], (8, 128))

    def both_ends(dx):
        return jnp.where(low_half, edge(dx, REACH), edge(dx, -REACH))

    middle = range(-REACH + 1, REACH)
    spans = []
    for dx in middle:
        ends = both_ends(dx)
        parts_z = [bundle if (dx, dz) == (0, 0) else pull_got[pull_rows[(dx, dz)], :] for dz in middle]
        for tile in range(tiles):
            pieces = [jnp.where(block_of == tile, part, 0.0) for part in parts_z]
            pieces.append(jnp.where(lax.rem(tile_lane, 64) == tile_row + 8 * tile, ends, 0.0))
            spans.append(jnp.concatenate(pieces, axis=1))
    pieces = [
        jnp.where(block_of == tile_row, jnp.where(low_rows, edge(REACH, dz), edge(-REACH, dz)), 0.0)
        for dz in middle
    ]
    corner_lane = lax.rem(tile_row, 4) * length_x + (length_x - 1) * (tile_row // 4)
    ends = jnp.where(low_rows, both_ends(REACH), both_ends(-REACH))
    pieces.append(jnp.where(lax.rem(tile_lane, 64) == corner_lane, ends, 0.0))
    spans.append(jnp.concatenate(pieces, axis=1))
    spans.append(jnp.zeros((8, 512), F32))
    spans_hi, spans_lo = split(jnp.concatenate(spans, axis=0))
    reached = jnp.dot(spans_hi, along_z[...], preferred_element_type=F32)
    reached = (reached[:, :128] + reached[:, 128:]) + jnp.dot(
        spans_lo, along_z[:, :128], preferred_element_type=F32
    )
    by_plane = []
    for plane in range(4):
        kept = [
            reached[ix * 64 + plane * length_x : ix * 64 + (plane + 1) * length_x]
            for ix in range(len(middle))
        ]
        last = reached[64 * len(middle) : 64 * len(middle) + 8]
        kept.append(jnp.where(lax.rem(tile_row, 4) == plane, last, 0.0))
        kept.append(jnp.zeros((8, 128), F32))
        by_plane.append(jnp.concatenate(kept, axis=0))
    stacked_hi, stacked_lo = split(jnp.concatenate(by_plane, axis=1))
    both_ways = jnp.dot(
        along_x[...],
        jnp.concatenate([stacked_hi, stacked_lo, stacked_hi], axis=0),
        preferred_element_type=F32,
    )
    block_lane = lax.broadcasted_iota(jnp.int32, (length_x, 128), 1) // length_z
    keep_row = lax.rem(lax.broadcasted_iota(jnp.int32, (rows, 256), 0), length_z)
    keep_lane = lax.rem(lax.broadcasted_iota(jnp.int32, (rows, 256), 1), length_z)
    wall_lane = lax.broadcasted_iota(jnp.int32, (rows, length_y), 1)
    tractions = []
    for index in range(2):
        blocks = []
        for side in range(2):
            plane = index * 2 + side
            total = jnp.zeros((length_x, 128), F32)
            for block, word_x, word_z in TERMS:
                piece = both_ways[
                    word_x * length_x : (word_x + 1) * length_x, plane * 128 : plane * 128 + 128
                ]
                shift = ((block - word_z) * length_z) % 128
                moved = pltpu.roll(piece, shift, 1) if shift else piece
                total = total + jnp.where(block_lane == block, moved, 0.0)
            blocks.append(total)
        wide = jnp.concatenate(blocks, axis=1)
        tall = jnp.concatenate(
            [jnp.broadcast_to(wide[x : x + 1], (length_z, 256)) for x in range(length_x)], axis=0
        )
        tall = jnp.where(keep_row == keep_lane, tall, 0.0)
        deep = dot3(split(tall), images, NN)
        level_two, shallow = deep[:, :length_y], deep[:, length_y:]
        tip = jnp.logical_or(wall_lane == 0, wall_lane == length_y - 1)
        level_zero = jnp.where(tip, pltpu.roll(shallow, length_y // 2, 1), 0.0)
        outside = jnp.logical_or(wall_lane < length_y // 4, wall_lane >= 3 * length_y // 4)
        level_one = jnp.where(outside, shallow, 0.0)
        tractions.append((level_zero, level_one, level_two))
    t1, t2 = shifts
    for c in range(3):
        chain = [field[level, c] for level in range(3)]
        if c != 1:
            taus = tractions[c // 2]
            chain = [chain[level] + taus[level] for level in range(3)]
        v1 = chain[1] - t1 * chain[0]
        field[0, c] = chain[0]
        field[1, c] = v1
        field[2, c] = chain[2] - t1 * chain[1] - t2 * v1
    for newest in range(2):
        inner_products(newest)
    add_faces(1)
    highs = [field[2, c].astype(BF16) for c in range(3)]
    along_y = jnp.dot(
        jnp.concatenate(highs, axis=0), lines_packed[:length_y], preferred_element_type=F32
    )
    wide = jnp.concatenate(highs, axis=1)
    across = jnp.dot(sheet[0], wide, preferred_element_type=F32)
    across_low = jnp.dot(sheet[1], wide, preferred_element_type=F32)
    inner_products(2)
    for c in range(3):
        here = slice(c * length_y, (c + 1) * length_y)
        tall = along_y[c * rows : (c + 1) * rows]
        tall = tall[:, :length_y] + tall[:, length_y:]
        image = (across[:, here] + across_low[:, here]) * mass_row + tall * columns[1]
        value = field[2, c]
        partner = value + (value - highs[c].astype(F32))
        inner(6, c, partner * columns[3] * image)

    total_rows = parts.shape[0]
    r_iota = lax.broadcasted_iota(jnp.int32, (total_rows, 128), 0)
    l_iota = lax.broadcasted_iota(jnp.int32, (total_rows, 128), 1)
    diagonal = r_iota == l_iota
    end_lane = lax.broadcasted_iota(jnp.int32, (total_rows, 128), 1)
    shared = jnp.logical_or(end_lane % 8 == 0, end_lane % 8 == 7)
    tips = jnp.logical_or(end_lane == 0, end_lane == length_y - 1)
    weight_y = jnp.where(jnp.logical_and(shared, jnp.logical_not(tips)), 0.5, 1.0)
    summed = jnp.sum(parts[...] * weight_y, axis=1, keepdims=True)
    row = jnp.sum(jnp.where(diagonal, summed, 0.0), axis=0, keepdims=True)

    def gather_sum(stage, row, count, got, ss, rs, place):
        sum_send[stage : stage + 1, :] = row
        for k in range(1, count):
            remote(
                sum_send.at[pl.ds(stage, 1), :], got.at[pl.ds(k - 1, 1), :], ss, rs, place(k)
            ).start()
        settle(ss, rs, got)
        return row + jnp.sum(got[...], axis=0, keepdims=True)

    if single:
        every = n_wall * n_span
        row = gather_sum(
            0, row, every, wall_got, wall_ss, wall_rs, lambda k: at(k // n_span, k % n_span)
        )
    else:
        row = gather_sum(0, row, n_wall, wall_got, wall_ss, wall_rs, lambda k: at(k, 0))
        row = gather_sum(1, row, n_span, span_got, span_ss, span_rs, lambda k: at(0, k))
    totals = jnp.sum(jnp.where(diagonal, row, 0.0), axis=1, keepdims=True)
    m00, m01, m11, m02, m12, m22, e22 = [totals[q * 8 : q * 8 + 8, :] for q in range(7)]
    t1, t2 = shifts
    a00 = m01 + t1 * m00
    a01 = m11 + t1 * m01
    a02 = m12 + t1 * m02
    a11 = m12 + t2 * m11
    a12 = m22 + t2 * m12
    l10 = a01 / a00
    l20 = a02 / a00
    d1 = a11 - l10 * a01
    u12 = a12 - l10 * a02
    l21 = u12 / d1
    d2 = e22 - l20 * a02 - l21 * u12
    y1 = m01 - l10 * m00
    y2 = m02 - l20 * m00 - l21 * y1
    x2 = y2 / d2
    x1 = y1 / d1 - l21 * x2
    x0 = m00 / a00 - l10 * x1 - l20 * x2
    for index, value in enumerate((x0, x1, x2)):
        factors[index] = jnp.broadcast_to(value, (8, 128))


def combine(field, factors, neumann_in, out, neumann, stage, sems):
    small = pltpu.make_async_copy(neumann_in, neumann, sems.at[3])
    small.start()
    copies = []
    for c in range(3):
        result = factors[0, c : c + 1] * field[0, c]
        for level in range(1, 3):
            result += factors[level, c : c + 1] * field[level, c]
        stage[c] = result.reshape(stage.shape[1:])
        copy = pltpu.make_async_copy(stage.at[c], out.at[c], sems.at[c])
        copy.start()
        copies.append(copy)
    for copy in copies:
        copy.wait()
    small.wait()


def body(n_wall, n_span, velocity_old, heights, owner_device, owner_element, ref_coords, roughness):
    sizes = velocity_old.shape[1:]
    length_x, length_z, length_y = sizes
    rows = length_x * length_z
    points = owner_device.shape[0]
    plane, lines, columns, along_x, along_z = tables(*sizes)
    along_x_hi, along_x_lo = split_np(along_x)
    every = n_wall * n_span
    first = every if every <= SINGLE_STAGE else n_wall
    faces = -(-(6 * (length_x + length_z) + 12) // 8) * 8
    vmem = pl.BlockSpec(memory_space=pltpu.VMEM)
    hbm = pl.BlockSpec(memory_space=pltpu.HBM)
    operands = (
        velocity_old,
        heights.reshape(1, -1),
        owner_device.reshape(1, -1),
        owner_element.reshape(1, -1),
        ref_coords,
        roughness.reshape(1, -1),
        jnp.stack(split_np(plane)),
        jnp.asarray(lines, F32),
        jnp.asarray(columns, F32),
        jnp.concatenate([along_x_hi, along_x_hi, along_x_lo], axis=1),
        jnp.concatenate(split_np(along_z), axis=1),
    )
    dma = pltpu.SemaphoreType.DMA
    field, factors, neumann = pl.pallas_call(
        functools.partial(kernel, n_wall, n_span, sizes),
        out_shape=(
            pltpu.VMEM((3, 3, rows, length_y), F32),
            pltpu.VMEM((3, 8, 128), F32),
            pltpu.VMEM((2, points), F32),
        ),
        in_specs=[hbm] * 11,
        out_specs=(vmem, vmem, vmem),
        scratch_shapes=[pltpu.VMEM(value.shape, value.dtype) for value in operands]
        + [
            dma((12,)),
            pltpu.VMEM((2, 64, length_y), F32),
            pltpu.VMEM((2, 2, 64, length_y), F32),
            pltpu.VMEM((ROUNDS, 3, rows, length_y), F32),
            pltpu.VMEM((ROUNDS, faces, length_y), F32),
            pltpu.VMEM((ROUNDS, faces, length_y), F32),
            pltpu.VMEM((56, length_y), F32),
            pltpu.VMEM((2, 128), F32),
            pltpu.VMEM((first - 1, 128), F32),
            pltpu.VMEM((n_span - 1, 128), F32),
            pltpu.VMEM((8, 128), F32),
            pltpu.VMEM((8, 128), F32),
            pltpu.VMEM((80, 128), F32),
            dma,
            dma,
            dma,
            dma,
            dma((ROUNDS,)),
            dma((ROUNDS,)),
            dma,
            dma,
            dma,
            dma,
            pltpu.SemaphoreType.REGULAR,
            pltpu.SemaphoreType.REGULAR,
        ],
        compiler_params=pltpu.CompilerParams(
            collective_id=0, has_side_effects=True, vmem_limit_bytes=VMEM_LIMIT
        ),
    )(*[pltpu.with_memory_space_constraint(value, pltpu.HBM) for value in operands])
    return pl.pallas_call(
        combine,
        out_shape=(
            jax.ShapeDtypeStruct(velocity_old.shape, F32),
            jax.ShapeDtypeStruct((2, points), F32),
        ),
        in_specs=[vmem] * 3,
        out_specs=(hbm, hbm),
        scratch_shapes=[pltpu.VMEM(velocity_old.shape, F32), dma((4,))],
        compiler_params=pltpu.CompilerParams(vmem_limit_bytes=VMEM_LIMIT),
    )(field, factors, neumann)


def solution(mesh):
    placed = (
        P(None, "wall", "span", None),
        P(),
        P(("wall", "span"), None),
        P(("wall", "span"), None),
        P(None, ("wall", "span")),
        P(("wall", "span")),
    )
    return jax.shard_map(
        functools.partial(body, mesh.shape["wall"], mesh.shape["span"]),
        mesh=mesh,
        in_specs=placed,
        out_specs=(P(None, "wall", "span", None), P(None, ("wall", "span"))),
        check_vma=False,
    )
```

```python
import functools

import jax
import jax.numpy as jnp
import numpy as np
from jax import lax
from jax.experimental import pallas as pl
from jax.experimental.pallas import tpu as pltpu
from jax.sharding import PartitionSpec as P

GLL_NODES = (
    -1.0,
    -0.8717401485096066,
    -0.5917001814331423,
    -0.2092992179024789,
    0.2092992179024789,
    0.5917001814331423,
    0.8717401485096066,
    1.0,
)
GLL_WEIGHTS = (
    0.03571428571428571,
    0.2107042271435061,
    0.3411226924835044,
    0.4124587946587038,
    0.4124587946587038,
    0.3411226924835044,
    0.2107042271435061,
    0.03571428571428571,
)
viscosity = 0.02
inverse_step = 20.0
karman = 0.41
sample_height = 0.1
speed_floor = 0.01
element_dx = 0.05
element_dz = 0.13
NEAR = 2
ROUNDS = 2
REACH = 2
TERMS = (
    (0, 0, 0),
    (1, 1, 2),
    (1, 2, 1),
    (2, 2, 2),
    (3, 3, 6),
    (3, 4, 5),
    (3, 5, 4),
    (3, 6, 3),
    (4, 4, 6),
    (4, 6, 4),
    (5, 5, 6),
    (5, 6, 5),
    (6, 6, 6),
)
SINGLE_STAGE = 64
VMEM_LIMIT = 32 * 2**20
MESH = pl.DeviceIdType.MESH
F32 = jnp.float32
BF16 = jnp.bfloat16


def stiffness_table():
    points = np.array(GLL_NODES)
    weights = np.array(GLL_WEIGHTS)
    previous = np.ones(8)
    current = points.copy()
    for degree in range(1, 7):
        previous, current = (
            current,
            ((2 * degree + 1) * points * current - degree * previous) / (degree + 1),
        )
    derivative = np.zeros((8, 8))
    for target in range(8):
        for source in range(8):
            if target != source:
                derivative[target, source] = (
                    current[target] / current[source] / (points[target] - points[source])
                )
    derivative[0, 0] = -14.0
    derivative[7, 7] = 14.0
    return derivative.T @ (weights[:, None] * derivative)


def join_matrix(length):
    joined = np.eye(length)
    for left in range(7, length - 1, 8):
        joined[left, left + 1] = 1.0
        joined[left + 1, left] = 1.0
    return joined


def face_weights(length, open_ends):
    values = np.ones(length)
    position = np.arange(length) % 8
    values[(position == 0) | (position == 7)] = 0.5
    if open_ends:
        values[0] = 1.0
        values[-1] = 1.0
    return values


def split_np(matrix):
    single = jnp.asarray(matrix, F32)
    high = single.astype(BF16)
    low = (jnp.asarray(matrix, F32) - high.astype(F32)).astype(BF16)
    return high, low


def tables(length_x, length_z, length_y):
    weights = np.array(GLL_WEIGHTS)
    stiffness = stiffness_table()
    count_x, count_z, count_y = length_x // 8, length_z // 8, length_y // 8
    mass_x = np.tile(0.5 * element_dx * weights, count_x)
    mass_z = np.tile(0.5 * element_dz * weights, count_z)
    stiff_x = np.kron(np.eye(count_x), stiffness * (2.0 / element_dx))
    stiff_z = np.kron(np.eye(count_z), stiffness * (2.0 / element_dz))
    mass_xz = np.kron(mass_x, mass_z)
    join_xz = np.kron(join_matrix(length_x), join_matrix(length_z))
    join_y = join_matrix(length_y)
    plane = viscosity * (
        np.kron(stiff_x, np.diag(mass_z)) + np.kron(np.diag(mass_x), stiff_z)
    ) + inverse_step * np.diag(mass_xz)
    plane = join_xz @ plane
    mass_plane = join_xz @ mass_xz
    lines_mass = np.tile(0.5 * weights, count_y)[:, None] * join_y
    lines_stiff = viscosity * 2.0 * (np.kron(np.eye(count_y), stiffness) @ join_y)
    lines = np.stack([lines_mass, lines_stiff])
    ring_x = join_matrix(length_x) @ mass_x
    ring_z = join_matrix(length_z) @ mass_z
    ring_x[0] *= 2.0
    ring_x[-1] *= 2.0
    ring_z[0] *= 2.0
    ring_z[-1] *= 2.0
    assembled = inverse_step * np.kron(ring_x, ring_z)
    inner_x = face_weights(length_x, True)
    inner_z = face_weights(length_z, True)
    outer_x = face_weights(length_x, False)
    outer_z = face_weights(length_z, False)
    columns = np.stack(
        [assembled, mass_plane, np.kron(outer_x, outer_z), np.kron(inner_x, inner_z)]
    )
    columns = columns[:, :, None] * np.ones(length_y)[None, None]
    reach = 2 * REACH + 1

    def words(length, mass, stiff, extra):
        size = reach * length
        join = join_matrix(size)
        light = join @ np.diag(np.tile(mass, reach))
        heavy = viscosity * join @ np.kron(np.eye(size // 8), stiff) + extra * light
        chains = [
            light,
            heavy @ light,
            light @ light,
            heavy @ heavy @ light,
            heavy @ light @ light,
            light @ heavy @ light,
            light @ light @ light,
        ]
        middle = REACH * length
        chains = [chain[middle : middle + length] for chain in chains]
        return np.concatenate(chains + [np.zeros((128 - 7 * length, size))], axis=0)

    words_x = words(length_x, mass_x, stiffness * (2.0 / element_dx), 0.0)
    words_z = words(length_z, mass_z, stiffness * (2.0 / element_dz), inverse_step)
    full = range(REACH - 1, REACH + 2)
    turned = words_z.T
    ends_z = [2 * REACH * length_z] * 8 + [length_z - 1] * 8
    along_z = np.concatenate(
        [np.tile(turned[iz * length_z : (iz + 1) * length_z], (8, 1)) for iz in full]
        + [np.tile(turned[ends_z], (8, 1))],
        axis=0,
    )
    ends = [2 * REACH * length_x, length_x - 1] * 4
    inner = [ix * length_x + half + (-r) % 8 for ix in full for half in (0, 8) for r in range(8)]
    along_x = np.concatenate(
        [words_x[:, inner], words_x[:, ends]]
        + [np.zeros((128, 8))],
        axis=1,
    )
    return plane, lines, columns, along_x, along_z


def split(value):
    high = value.astype(BF16)
    low = (value - high.astype(F32)).astype(BF16)
    return high, low


def dot3(left, right, dims):
    def one(a, b):
        return lax.dot_general(a, b, (dims, ((), ())), preferred_element_type=F32)

    return one(left[0], right[0]) + (one(left[0], right[1]) + one(left[1], right[0]))


NN = ((1,), (0,))
NT = ((1,), (1,))
TN = ((0,), (0,))
DIRS = ((1, 1), (1, -1), (-1, 1), (-1, -1))


def lagrange_rows(coord):
    points = np.array(GLL_NODES)
    scale = 1.0 / np.prod(points[:, None] - points[None, :] + np.eye(8), axis=1)
    shape = (8, coord.shape[1])
    node = lax.broadcasted_iota(jnp.int32, shape, 0)
    total = jnp.zeros(shape, F32)
    for a in range(8):
        total = jnp.where(node == a, F32(scale[a]), total)
    for b in range(8):
        total = total * jnp.where(node == b, F32(1.0), coord - F32(points[b]))
    return total


def kernel(
    n_wall,
    n_span,
    sizes,
    vel_in,
    heights_in,
    owner_in,
    element_in,
    coords_in,
    roughness_in,
    plane_in,
    lines_in,
    columns_in,
    along_x_in,
    along_z_in,
    field,
    factors,
    neumann,
    vel,
    heights,
    owner,
    element,
    coords,
    roughness,
    sheet,
    lines,
    columns,
    along_x,
    along_z,
    load_sem,
    near,
    near_got,
    local,
    face_send,
    face_got,
    parts,
    sum_send,
    wall_got,
    span_got,
    pull_send,
    edge_send,
    pull_got,
    everything,
    sent,
    near_rs,
    pull_rs,
    face_rs,
    wall_rs,
    step_one,
    step_two,
    *span_rs,
):
    length_x, length_z, length_y = sizes
    rows = length_x * length_z
    count_z, count_y = length_z // 8, length_y // 8
    w = lax.axis_index("wall")
    s = lax.axis_index("span")

    def at(dx, dz):
        return (lax.rem(w + (dx + n_wall), n_wall), lax.rem(s + (dz + n_span), n_span))

    loads = {
        name: pltpu.make_async_copy(source, target, load_sem.at[index])
        for index, (name, source, target) in enumerate(
            (
                ("vel", vel_in, vel),
                ("heights", heights_in, heights),
                ("lines", lines_in, lines),
                ("scale", columns_in.at[pl.ds(0, 2)], columns.at[pl.ds(0, 2)]),
                ("plane", plane_in, sheet),
                ("coords", coords_in, coords),
                ("owner", owner_in, owner),
                ("element", element_in, element),
                ("roughness", roughness_in, roughness),
                ("along_x", along_x_in, along_x),
                ("along_z", along_z_in, along_z),
                ("weights", columns_in.at[pl.ds(2, 2)], columns.at[pl.ds(2, 2)]),
            )
        )
    }
    for load in loads.values():
        load.start()

    def loaded(*names):
        for name in names:
            loads[name].wait()

    single = n_wall * n_span <= SINGLE_STAGE
    stepwise = single and 3 <= n_wall <= 4 * REACH and 3 <= n_span <= 4 * REACH
    across_wall = ((1, 0), (-1, 0))
    if stepwise:
        greeted = across_wall + tuple((0, k) for k in range(1, n_span))
    elif single:
        greeted = [divmod(k, n_span) for k in range(1, n_wall * n_span)]
    else:
        greeted = [(k, 0) for k in range(1, n_wall)] + [(0, k) for k in range(1, n_span)]
        greeted += sorted(
            {
                ((dx + n_wall) % n_wall, (dz + n_span) % n_span)
                for dx in range(-REACH, REACH + 1)
                for dz in range(-REACH, REACH + 1)
            }
            - {(0, 0)}
            - set(greeted)
        )
    barrier = pltpu.get_barrier_semaphore()

    def greet(semaphore, places):
        for dx, dz in places:
            pl.semaphore_signal(semaphore, inc=1, device_id=at(dx, dz), device_id_type=MESH)

    greet(barrier, greeted)

    loaded("vel")
    lane = lax.broadcasted_iota(jnp.int32, (64, length_y), 1)
    groups = (length_x // 8) * count_z
    for index, comp in enumerate((0, 2)):
        packed = jnp.zeros((64, length_y), F32)
        for group in range(groups):
            ex, ez = group // count_z, group % count_z
            block = vel[comp, pl.ds(ex * 8, 8), pl.ds(ez * 8, 8), :].reshape(64, length_y)
            moved = pltpu.roll(block, (group * 32 + 16) % length_y, 1)
            packed = jnp.where(lane // 32 == group, moved, packed)
        near[index] = packed
    def remote(src, dst, ss, rs, where):
        return pltpu.make_async_remote_copy(
            src_ref=src,
            dst_ref=dst,
            send_sem=ss,
            recv_sem=rs,
            device_id=where,
            device_id_type=MESH,
        )

    near_copies = []
    for slot, dx in enumerate((1, -1)):
        copy = remote(near, near_got.at[slot], sent, near_rs, at(dx, 0))
        near_copies.append(copy)

    def enter():
        pl.semaphore_wait(barrier, len(greeted))
        for copy in near_copies:
            copy.start()
        if stepwise:
            greet(step_one, across_wall)

    if stepwise:
        enter()
    loaded("heights", "lines", "scale", "plane")

    layer_of = lax.broadcasted_iota(jnp.int32, (length_y, count_y), 0) // 8
    layer = lax.broadcasted_iota(jnp.int32, (length_y, count_y), 1)
    height_row = heights[...]
    height = jnp.sum(jnp.where(layer_of == layer, height_row, 0.0), axis=1, keepdims=True)
    lines_mass = height * lines[0]
    lines_stiff = lines[1] / height
    stiff_hi, stiff_lo = split(lines_stiff)
    lines_packed = jnp.concatenate(
        [
            jnp.concatenate([stiff_hi, stiff_lo], axis=1),
            jnp.concatenate([stiff_hi, jnp.zeros_like(stiff_lo)], axis=1),
        ],
        axis=0,
    )
    bound = jnp.max(0.1535 * height_row + 0.000182 / height_row, axis=1, keepdims=True)
    shifts = (0.15 * bound, 0.85 * bound)

    mass_row = jnp.sum(lines_mass, axis=0, keepdims=True)
    scale = columns[0] * mass_row
    for c in range(3):
        field[0, c] = vel[c].reshape(rows, length_y) * scale

    face_rows = []
    for slot, (dx, dz) in enumerate(DIRS + ((0, 1), (0, -1), (1, 0), (-1, 0))):
        size = 3 * (1 if dx and dz else length_z if dx else length_x)
        face_rows.append((sum(entry[1] for entry in face_rows), size, dx, dz))
    face_total = sum(entry[1] for entry in face_rows)

    def corner(dx, dz):
        return (rows - length_z if dx == 1 else 0) + (length_z - 1 if dz == 1 else 0)

    def face_part(slot, c, dx, dz):
        first, size = face_rows[slot][0] + c * (face_rows[slot][1] // 3), face_rows[slot][1] // 3
        if dx and dz:
            rows_of = pl.ds(corner(dx, dz), 1)
        elif dx:
            rows_of = pl.ds(rows - length_z if dx == 1 else 0, length_z)
        else:
            rows_of = pl.ds(length_z - 1 if dz == 1 else 0, length_x, stride=length_z)
        return pl.ds(first, size), rows_of

    def send_faces(turn):
        for c in range(3):
            for slot, (_, _, dx, dz) in enumerate(face_rows):
                packed_rows, rows_of = face_part(slot, c, dx, dz)
                face_send[turn, packed_rows, :] = local[turn, c, rows_of, :]
        first_turn = turn == 0 and stepwise
        if turn == 0 and not stepwise:
            enter()
        for stage in ((0,), (2, 1)) if first_turn else ((2, 0, 1),):
            if stage[0] == 2 and first_turn:
                pl.semaphore_wait(step_one, len(across_wall))
                greet(step_two, across_wall)
            for kind in stage:
                for first, size, dx, dz in face_rows:
                    if (2 if dx and dz else abs(dx)) != kind:
                        continue
                    part = (turn, pl.ds(first, size), slice(None))
                    remote(
                        face_send.at[part],
                        face_got.at[part],
                        sent,
                        face_rs.at[turn],
                        at(dx, dz),
                    ).start()

    def settle(semaphore, ref):
        pltpu.make_async_copy(ref, ref, semaphore).wait()

    def add_faces(turn):
        settle(face_rs.at[turn], face_got.at[turn, pl.ds(0, face_total), :])
        for c in range(3):
            for slot, (_, _, dx, dz) in enumerate(face_rows):
                packed_rows, rows_of = face_part(slot, c, -dx, -dz)
                field[turn + 1, c, rows_of, :] = (
                    field[turn + 1, c, rows_of, :] + face_got[turn, packed_rows, :]
                )

    def inner(quantity, c, product):
        parts[quantity * 8 + c : quantity * 8 + c + 1, :] = jnp.sum(
            product, axis=0, keepdims=True
        )

    def operate(source, target):
        highs, lows = zip(*[split(field[source, c]) for c in range(3)])
        along_y = jnp.dot(
            jnp.concatenate(
                [jnp.concatenate([high, low], axis=1) for high, low in zip(highs, lows)], axis=0
            ),
            lines_packed,
            preferred_element_type=F32,
        )
        across = jnp.dot(
            sheet[0], jnp.concatenate(highs + lows, axis=1), preferred_element_type=F32
        )
        across_low = jnp.dot(sheet[1], jnp.concatenate(highs, axis=1), preferred_element_type=F32)
        for c in range(3):
            here = slice(c * length_y, (c + 1) * length_y)
            also = slice((3 + c) * length_y, (4 + c) * length_y)
            flat = across[:, here] + (across[:, also] + across_low[:, here])
            tall = along_y[c * rows : (c + 1) * rows]
            tall = tall[:, :length_y] + tall[:, length_y:]
            local[target, c] = flat * mass_row + tall * columns[1]

    slots = {(0, 0): 0, (0, 1): 1, (1, 1): 2, (0, 2): 3, (1, 2): 4, (2, 2): 5}

    def inner_products(newest):
        for c in range(3):
            weighted = field[newest, c] * columns[2]
            for other in range(newest + 1):
                inner(slots[(other, newest)], c, weighted * field[other, c])

    operate(0, 0)
    send_faces(0)
    for c in range(3):
        field[1, c] = local[0, c]
    parts[...] = jnp.zeros_like(parts)

    loaded("coords", "owner", "element", "roughness")
    points = owner.shape[1]
    row_x = lagrange_rows(coords[0:1, :])
    row_z = lagrange_rows(coords[1:2, :])
    row_y = lagrange_rows(coords[2:3, :])
    cross = jnp.concatenate([row_x[a : a + 1] * row_z for a in range(8)], axis=0)
    distance = lax.rem(owner[...] - w + n_wall, n_wall)
    from_next = distance == 1
    from_prev = distance == n_wall - 1
    own = jnp.logical_not(jnp.logical_or(from_next, from_prev))
    spread = jnp.concatenate(
        [jnp.where(mask, cross, 0.0) for mask in (own, from_prev, from_next)], axis=0
    )
    n_row = lax.broadcasted_iota(jnp.int32, (length_y, points), 0)
    within = (n_row % 32) // 8
    layer_y = jnp.where(within < NEAR, within + (count_y - NEAR), within - NEAR)
    wanted = (n_row // 32) * count_y + layer_y == element[...]
    along = jnp.where(wanted, jnp.concatenate([row_y] * (length_y // 8), axis=0), 0.0)
    spread = split(spread)

    drag = karman / jnp.log(sample_height / roughness[...])
    drag = drag * drag * (-1.0 / viscosity)

    settle(near_rs, near_got)

    sampled = []
    for index in range(2):
        sources = jnp.concatenate(
            [near[index], near_got[0, index], near_got[1, index]], axis=0
        )
        values = dot3(split(sources), spread, TN)
        sampled.append(jnp.sum(values * along, axis=0, keepdims=True))
    stream, spanwise = sampled
    speed = jnp.sqrt(stream * stream + spanwise * spanwise + speed_floor)
    factor = drag * speed
    gradient = (factor * stream, factor * spanwise)
    neumann[0:1, :] = gradient[0]
    neumann[1:2, :] = gradient[1]

    planes = []
    for index in range(2):
        pull = viscosity * gradient[index]
        planes += [pull[:, :rows], pull[:, rows:]]
    tiles = 4 * length_x // 8
    tile_lane = lax.broadcasted_iota(jnp.int32, (8, 128), 1)
    tile_row = lax.broadcasted_iota(jnp.int32, (8, 128), 0)
    block_of = tile_lane // length_z
    bundle = jnp.zeros((8, 128), F32)
    fringe = jnp.zeros((8, 128), F32)
    for tile in range(tiles):
        part = planes[tile // 2][:, 128 * (tile % 2) : 128 * (tile % 2) + 128]
        part = jnp.broadcast_to(part, (8, 128))
        spread_rows = pltpu.roll(part, 0, 1, stride=length_z, stride_axis=0)
        spread_rows = pltpu.roll(spread_rows, (8 - tile) % 8, 0)
        bundle = jnp.where(block_of == tile, spread_rows, bundle)
        for end in range(2):
            turned = pltpu.roll(part, 7 * (1 - end), 1, stride=length_z - 1, stride_axis=0)
            wanted_lane = tile * length_z + 8 * end + 7 - tile_row
            fringe = jnp.where(tile_lane == wanted_lane, turned, fringe)
    pull_send[...] = bundle
    edge_send[0:1, :] = jnp.sum(fringe, axis=0, keepdims=True)
    edge_send[1:2, :] = jnp.where(block_of[0:1] % 2 == 0, bundle[0:1], bundle[1:2])
    if stepwise:
        pl.semaphore_wait(step_two, len(across_wall))
    reach = 2 * REACH + 1
    offsets = [
        (dx, dz)
        for dx in range(-REACH, REACH + 1)
        for dz in range(-REACH, REACH + 1)
        if (dx, dz) != (0, 0)
    ]
    nearby = [place for place in offsets if max(abs(place[0]), abs(place[1])) < REACH]
    remaining = [place for place in offsets if place not in nearby]
    pull_rows = {place: pl.ds(8 * index, 8) for index, place in enumerate(nearby)}
    for index, place in enumerate(remaining):
        pull_rows[place] = pl.ds(8 * len(nearby) + index, 1)
    for dx, dz in sorted(offsets, key=lambda pair: -abs(pair[0]) - abs(pair[1])):
        if (dx, dz) in nearby:
            source = pull_send
        else:
            source = edge_send.at[pl.ds(0 if abs(dz) == REACH else 1, 1), :]
        remote(
            source, pull_got.at[pull_rows[(-dx, -dz)], :], sent, pull_rs, at(dx, dz)
        ).start()

    add_faces(0)
    operate(1, 1)
    send_faces(1)
    for c in range(3):
        field[2, c] = local[1, c]
    loaded("along_x", "along_z", "weights")
    lines_rows = jnp.concatenate([lines_mass, lines_stiff], axis=1)
    ends = [lines_rows[0:1], lines_rows[length_y - 1 : length_y]]
    once = [(end[:, :length_y], end[:, length_y:]) for end in ends]
    twice = dot3(
        split(jnp.concatenate([once[0][0], once[0][1], once[1][0], once[1][1]] * 2, axis=0)),
        split(lines_rows),
        NN,
    )
    one_lane = lax.broadcasted_iota(jnp.int32, (1, length_y), 1)
    zero = jnp.zeros((1, length_y), F32)
    images = []
    for side in range(2):
        by_mass, by_stiff = twice[2 * side : 2 * side + 1], twice[2 * side + 1 : 2 * side + 2]
        moved_tip = jnp.where(one_lane == length_y // 2 - side, 1.0, 0.0)
        rows_of = [
            (zero, moved_tip),
            (zero, once[side][0]),
            (zero, once[side][1]),
            (by_mass[:, :length_y], zero),
            (by_stiff[:, :length_y], zero),
            (by_mass[:, length_y:], zero),
            (by_stiff[:, length_y:], zero),
        ]
        for entry in rows_of:
            image = jnp.concatenate(entry, axis=1)
            images.append(jnp.broadcast_to(image, (length_z, 2 * length_y)))
        images.append(jnp.zeros((128 - 7 * length_z, 2 * length_y), F32))
    images = split(jnp.concatenate(images, axis=0))
    low_half = tile_lane & 8 == 0
    low_rows = tile_row & 1 == 0
    diagonal_of = (tile_lane + tile_row) & 7
    settle(pull_rs, pull_got)

    def edge(dx, dz):
        return jnp.broadcast_to(pull_got[pull_rows[(dx, dz)], :], (8, 128))

    def both_ends(dx):
        return jnp.where(low_half, edge(dx, REACH), edge(dx, -REACH))

    middle = range(-REACH + 1, REACH)
    spans = []
    for dx in middle:
        ends = both_ends(dx)
        parts_z = [bundle if (dx, dz) == (0, 0) else pull_got[pull_rows[(dx, dz)], :] for dz in middle]
        for tile in range(tiles):
            pieces = [jnp.where(block_of == tile, part, 0.0) for part in parts_z]
            kept = jnp.logical_and(block_of == tile, diagonal_of == (7 - tile) % 8)
            pieces.append(jnp.where(kept, ends, 0.0))
            spans.append(jnp.concatenate(pieces, axis=1))
    pieces = [
        jnp.where(block_of == tile_row, jnp.where(low_rows, edge(REACH, dz), edge(-REACH, dz)), 0.0)
        for dz in middle
    ]
    kept = jnp.logical_and(
        block_of == tile_row, (tile_lane + tile_row + (tile_row & 1)) & 7 == 7
    )
    ends = jnp.where(low_rows, both_ends(REACH), both_ends(-REACH))
    pieces.append(jnp.where(kept, ends, 0.0))
    spans.append(jnp.concatenate(pieces, axis=1))
    spans.append(jnp.zeros((8, 512), F32))
    spans_hi, spans_lo = split(jnp.concatenate(spans, axis=0))
    reached = jnp.dot(spans_hi, along_z[...], preferred_element_type=F32)
    reached = (reached[:, :128] + reached[:, 128:]) + jnp.dot(
        spans_lo, along_z[:, :128], preferred_element_type=F32
    )
    by_plane = []
    for plane in range(4):
        kept = [
            reached[ix * 64 + plane * length_x : ix * 64 + (plane + 1) * length_x]
            for ix in range(len(middle))
        ]
        last = reached[64 * len(middle) : 64 * len(middle) + 8]
        kept.append(jnp.where(tile_row // 2 == plane, last, 0.0))
        kept.append(jnp.zeros((8, 128), F32))
        by_plane.append(jnp.concatenate(kept, axis=0))
    stacked_hi, stacked_lo = split(jnp.concatenate(by_plane, axis=1))
    both_ways = jnp.dot(
        along_x[...],
        jnp.concatenate([stacked_hi, stacked_lo, stacked_hi], axis=0),
        preferred_element_type=F32,
    )
    block_lane = lax.broadcasted_iota(jnp.int32, (length_x, 128), 1) // length_z
    keep_row = lax.rem(lax.broadcasted_iota(jnp.int32, (rows, 256), 0), length_z)
    keep_lane = lax.rem(lax.broadcasted_iota(jnp.int32, (rows, 256), 1), length_z)
    wall_lane = lax.broadcasted_iota(jnp.int32, (rows, length_y), 1)
    tractions = []
    for index in range(2):
        blocks = []
        for side in range(2):
            plane = index * 2 + side
            total = jnp.zeros((length_x, 128), F32)
            for block, word_x, word_z in TERMS:
                piece = both_ways[
                    word_x * length_x : (word_x + 1) * length_x, plane * 128 : plane * 128 + 128
                ]
                shift = ((block - word_z) * length_z) % 128
                moved = pltpu.roll(piece, shift, 1) if shift else piece
                total = total + jnp.where(block_lane == block, moved, 0.0)
            blocks.append(total)
        wide = jnp.concatenate(blocks, axis=1)
        tall = jnp.concatenate(
            [jnp.broadcast_to(wide[x : x + 1], (length_z, 256)) for x in range(length_x)], axis=0
        )
        tall = jnp.where(keep_row == keep_lane, tall, 0.0)
        deep = dot3(split(tall), images, NN)
        level_two, shallow = deep[:, :length_y], deep[:, length_y:]
        tip = jnp.logical_or(wall_lane == 0, wall_lane == length_y - 1)
        level_zero = jnp.where(tip, pltpu.roll(shallow, length_y // 2, 1), 0.0)
        outside = jnp.logical_or(wall_lane < length_y // 4, wall_lane >= 3 * length_y // 4)
        level_one = jnp.where(outside, shallow, 0.0)
        tractions.append((level_zero, level_one, level_two))
    t1, t2 = shifts
    for c in range(3):
        chain = [field[level, c] for level in range(3)]
        if c != 1:
            taus = tractions[c // 2]
            chain = [chain[level] + taus[level] for level in range(3)]
        v1 = chain[1] - t1 * chain[0]
        field[0, c] = chain[0]
        field[1, c] = v1
        field[2, c] = chain[2] - t1 * chain[1] - t2 * v1
    for newest in range(2):
        inner_products(newest)
    add_faces(1)
    highs = [field[2, c].astype(BF16) for c in range(3)]
    along_y = jnp.dot(
        jnp.concatenate(highs, axis=0), lines_packed[:length_y], preferred_element_type=F32
    )
    wide = jnp.concatenate(highs, axis=1)
    across = jnp.dot(sheet[0], wide, preferred_element_type=F32)
    across_low = jnp.dot(sheet[1], wide, preferred_element_type=F32)
    inner_products(2)
    for c in range(3):
        here = slice(c * length_y, (c + 1) * length_y)
        tall = along_y[c * rows : (c + 1) * rows]
        tall = tall[:, :length_y] + tall[:, length_y:]
        image = (across[:, here] + across_low[:, here]) * mass_row + tall * columns[1]
        value = field[2, c]
        partner = value + (value - highs[c].astype(F32))
        inner(6, c, partner * columns[3] * image)

    total_rows = parts.shape[0]
    r_iota = lax.broadcasted_iota(jnp.int32, (total_rows, 128), 0)
    l_iota = lax.broadcasted_iota(jnp.int32, (total_rows, 128), 1)
    diagonal = r_iota == l_iota
    end_lane = lax.broadcasted_iota(jnp.int32, (total_rows, 128), 1)
    shared = jnp.logical_or(end_lane % 8 == 0, end_lane % 8 == 7)
    tips = jnp.logical_or(end_lane == 0, end_lane == length_y - 1)
    weight_y = jnp.where(jnp.logical_and(shared, jnp.logical_not(tips)), 0.5, 1.0)
    summed = jnp.sum(parts[...] * weight_y, axis=1, keepdims=True)
    row = jnp.sum(jnp.where(diagonal, summed, 0.0), axis=0, keepdims=True)

    def gather_sum(stage, row, count, got, rs, place):
        sum_send[stage : stage + 1, :] = row
        for k in range(1, count):
            remote(
                sum_send.at[pl.ds(stage, 1), :], got.at[pl.ds(k - 1, 1), :], sent, rs, place(k)
            ).start()
        settle(rs, got)
        return row + jnp.sum(got[...], axis=0, keepdims=True)

    sum_rows = 0
    if single:
        every = n_wall * n_span
        row = gather_sum(0, row, every, wall_got, wall_rs, lambda k: at(k // n_span, k % n_span))
        sum_rows = every - 1
    else:
        row = gather_sum(0, row, n_wall, wall_got, wall_rs, lambda k: at(k, 0))
        row = gather_sum(1, row, n_span, span_got, span_rs[0], lambda k: at(0, k))
        sum_rows = n_wall + n_span - 2
    sent_rows = 2 * 2 * 64 + pull_got.shape[0] + ROUNDS * face_total + sum_rows
    settle(sent, everything.at[pl.ds(0, sent_rows), :])
    totals = jnp.sum(jnp.where(diagonal, row, 0.0), axis=1, keepdims=True)
    m00, m01, m11, m02, m12, m22, e22 = [totals[q * 8 : q * 8 + 8, :] for q in range(7)]
    t1, t2 = shifts
    a00 = m01 + t1 * m00
    a01 = m11 + t1 * m01
    a02 = m12 + t1 * m02
    a11 = m12 + t2 * m11
    a12 = m22 + t2 * m12
    l10 = a01 / a00
    l20 = a02 / a00
    d1 = a11 - l10 * a01
    u12 = a12 - l10 * a02
    l21 = u12 / d1
    d2 = e22 - l20 * a02 - l21 * u12
    y1 = m01 - l10 * m00
    y2 = m02 - l20 * m00 - l21 * y1
    x2 = y2 / d2
    x1 = y1 / d1 - l21 * x2
    x0 = m00 / a00 - l10 * x1 - l20 * x2
    for index, value in enumerate((x0, x1, x2)):
        factors[index] = jnp.broadcast_to(value, (8, 128))


def combine(field, factors, neumann_in, out, neumann, stage, sems):
    small = pltpu.make_async_copy(neumann_in, neumann, sems.at[3])
    small.start()
    copies = []
    for c in range(3):
        result = factors[0, c : c + 1] * field[0, c]
        for level in range(1, 3):
            result += factors[level, c : c + 1] * field[level, c]
        stage[c] = result.reshape(stage.shape[1:])
        copy = pltpu.make_async_copy(stage.at[c], out.at[c], sems.at[c])
        copy.start()
        copies.append(copy)
    for copy in copies:
        copy.wait()
    small.wait()


def body(n_wall, n_span, velocity_old, heights, owner_device, owner_element, ref_coords, roughness):
    sizes = velocity_old.shape[1:]
    length_x, length_z, length_y = sizes
    rows = length_x * length_z
    points = owner_device.shape[0]
    plane, lines, columns, along_x, along_z = tables(*sizes)
    along_x_hi, along_x_lo = split_np(along_x)
    every = n_wall * n_span
    first = every if every <= SINGLE_STAGE else n_wall
    faces = -(-(6 * (length_x + length_z) + 12) // 8) * 8
    vmem = pl.BlockSpec(memory_space=pltpu.VMEM)
    hbm = pl.BlockSpec(memory_space=pltpu.HBM)
    operands = (
        velocity_old,
        heights.reshape(1, -1),
        owner_device.reshape(1, -1),
        owner_element.reshape(1, -1),
        ref_coords,
        roughness.reshape(1, -1),
        jnp.stack(split_np(plane)),
        jnp.asarray(lines, F32),
        jnp.asarray(columns, F32),
        jnp.concatenate([along_x_hi, along_x_hi, along_x_lo], axis=1),
        jnp.concatenate(split_np(along_z), axis=1),
    )
    dma = pltpu.SemaphoreType.DMA
    field, factors, neumann = pl.pallas_call(
        functools.partial(kernel, n_wall, n_span, sizes),
        out_shape=(
            pltpu.VMEM((3, 3, rows, length_y), F32),
            pltpu.VMEM((3, 8, 128), F32),
            pltpu.VMEM((2, points), F32),
        ),
        in_specs=[hbm] * 11,
        out_specs=(vmem, vmem, vmem),
        scratch_shapes=[pltpu.VMEM(value.shape, value.dtype) for value in operands]
        + [
            dma((12,)),
            pltpu.VMEM((2, 64, length_y), F32),
            pltpu.VMEM((2, 2, 64, length_y), F32),
            pltpu.VMEM((ROUNDS, 3, rows, length_y), F32),
            pltpu.VMEM((ROUNDS, faces, length_y), F32),
            pltpu.VMEM((ROUNDS, faces, length_y), F32),
            pltpu.VMEM((56, length_y), F32),
            pltpu.VMEM((2, 128), F32),
            pltpu.VMEM((first - 1, 128), F32),
            pltpu.VMEM((n_span - 1, 128), F32),
            pltpu.VMEM((8, 128), F32),
            pltpu.VMEM((8, 128), F32),
            pltpu.VMEM((80, 128), F32),
            pltpu.VMEM((896, length_y), F32),
            dma,
            dma,
            dma,
            dma((ROUNDS,)),
            dma,
            pltpu.SemaphoreType.REGULAR,
            pltpu.SemaphoreType.REGULAR,
        ]
        + ([] if every <= SINGLE_STAGE else [dma]),
        compiler_params=pltpu.CompilerParams(
            collective_id=0, has_side_effects=True, vmem_limit_bytes=VMEM_LIMIT
        ),
    )(*[pltpu.with_memory_space_constraint(value, pltpu.HBM) for value in operands])
    return pl.pallas_call(
        combine,
        out_shape=(
            jax.ShapeDtypeStruct(velocity_old.shape, F32),
            jax.ShapeDtypeStruct((2, points), F32),
        ),
        in_specs=[vmem] * 3,
        out_specs=(hbm, hbm),
        scratch_shapes=[pltpu.VMEM(velocity_old.shape, F32), dma((4,))],
        compiler_params=pltpu.CompilerParams(vmem_limit_bytes=VMEM_LIMIT),
    )(field, factors, neumann)


def solution(mesh):
    placed = (
        P(None, "wall", "span", None),
        P(),
        P(("wall", "span"), None),
        P(("wall", "span"), None),
        P(None, ("wall", "span")),
        P(("wall", "span")),
    )
    return jax.shard_map(
        functools.partial(body, mesh.shape["wall"], mesh.shape["span"]),
        mesh=mesh,
        in_specs=placed,
        out_specs=(P(None, "wall", "span", None), P(None, ("wall", "span"))),
        check_vma=False,
    )
```

```python
import functools

import jax
import jax.numpy as jnp
import numpy as np
from jax import lax
from jax.experimental import pallas as pl
from jax.experimental.pallas import tpu as pltpu
from jax.sharding import PartitionSpec as P

GLL_NODES = (
    -1.0,
    -0.8717401485096066,
    -0.5917001814331423,
    -0.2092992179024789,
    0.2092992179024789,
    0.5917001814331423,
    0.8717401485096066,
    1.0,
)
GLL_WEIGHTS = (
    0.03571428571428571,
    0.2107042271435061,
    0.3411226924835044,
    0.4124587946587038,
    0.4124587946587038,
    0.3411226924835044,
    0.2107042271435061,
    0.03571428571428571,
)
viscosity = 0.02
inverse_step = 20.0
karman = 0.41
sample_height = 0.1
speed_floor = 0.01
element_dx = 0.05
element_dz = 0.13
NEAR = 2
ROUNDS = 2
REACH = 2
TERMS = (
    (0, 0, 0),
    (1, 1, 2),
    (1, 2, 1),
    (2, 2, 2),
    (3, 3, 6),
    (3, 4, 5),
    (3, 5, 4),
    (3, 6, 3),
    (4, 4, 6),
    (4, 6, 4),
    (5, 5, 6),
    (5, 6, 5),
    (6, 6, 6),
)
SINGLE_STAGE = 64
VMEM_LIMIT = 32 * 2**20
MESH = pl.DeviceIdType.MESH
F32 = jnp.float32
BF16 = jnp.bfloat16


def stiffness_table():
    points = np.array(GLL_NODES)
    weights = np.array(GLL_WEIGHTS)
    previous = np.ones(8)
    current = points.copy()
    for degree in range(1, 7):
        previous, current = (
            current,
            ((2 * degree + 1) * points * current - degree * previous) / (degree + 1),
        )
    derivative = np.zeros((8, 8))
    for target in range(8):
        for source in range(8):
            if target != source:
                derivative[target, source] = (
                    current[target] / current[source] / (points[target] - points[source])
                )
    derivative[0, 0] = -14.0
    derivative[7, 7] = 14.0
    return derivative.T @ (weights[:, None] * derivative)


def join_matrix(length):
    joined = np.eye(length)
    for left in range(7, length - 1, 8):
        joined[left, left + 1] = 1.0
        joined[left + 1, left] = 1.0
    return joined


def face_weights(length, open_ends):
    values = np.ones(length)
    position = np.arange(length) % 8
    values[(position == 0) | (position == 7)] = 0.5
    if open_ends:
        values[0] = 1.0
        values[-1] = 1.0
    return values


def split_np(matrix):
    single = jnp.asarray(matrix, F32)
    high = single.astype(BF16)
    low = (jnp.asarray(matrix, F32) - high.astype(F32)).astype(BF16)
    return high, low


def tables(length_x, length_z, length_y):
    weights = np.array(GLL_WEIGHTS)
    stiffness = stiffness_table()
    count_x, count_z, count_y = length_x // 8, length_z // 8, length_y // 8
    mass_x = np.tile(0.5 * element_dx * weights, count_x)
    mass_z = np.tile(0.5 * element_dz * weights, count_z)
    stiff_x = np.kron(np.eye(count_x), stiffness * (2.0 / element_dx))
    stiff_z = np.kron(np.eye(count_z), stiffness * (2.0 / element_dz))
    mass_xz = np.kron(mass_x, mass_z)
    join_xz = np.kron(join_matrix(length_x), join_matrix(length_z))
    join_y = join_matrix(length_y)
    plane = viscosity * (
        np.kron(stiff_x, np.diag(mass_z)) + np.kron(np.diag(mass_x), stiff_z)
    ) + inverse_step * np.diag(mass_xz)
    plane = join_xz @ plane
    mass_plane = join_xz @ mass_xz
    lines_mass = np.tile(0.5 * weights, count_y)[:, None] * join_y
    lines_stiff = viscosity * 2.0 * (np.kron(np.eye(count_y), stiffness) @ join_y)
    lines = np.stack([lines_mass, lines_stiff])
    ring_x = join_matrix(length_x) @ mass_x
    ring_z = join_matrix(length_z) @ mass_z
    ring_x[0] *= 2.0
    ring_x[-1] *= 2.0
    ring_z[0] *= 2.0
    ring_z[-1] *= 2.0
    assembled = inverse_step * np.kron(ring_x, ring_z)
    inner_x = face_weights(length_x, True)
    inner_z = face_weights(length_z, True)
    outer_x = face_weights(length_x, False)
    outer_z = face_weights(length_z, False)
    columns = np.stack(
        [assembled, mass_plane, np.kron(outer_x, outer_z), np.kron(inner_x, inner_z)]
    )
    columns = columns[:, :, None] * np.ones(length_y)[None, None]
    reach = 2 * REACH + 1

    def words(length, mass, stiff, extra):
        size = reach * length
        join = join_matrix(size)
        light = join @ np.diag(np.tile(mass, reach))
        heavy = viscosity * join @ np.kron(np.eye(size // 8), stiff) + extra * light
        chains = [
            light,
            heavy @ light,
            light @ light,
            heavy @ heavy @ light,
            heavy @ light @ light,
            light @ heavy @ light,
            light @ light @ light,
        ]
        middle = REACH * length
        chains = [chain[middle : middle + length] for chain in chains]
        return np.concatenate(chains + [np.zeros((128 - 7 * length, size))], axis=0)

    words_x = words(length_x, mass_x, stiffness * (2.0 / element_dx), 0.0)
    words_z = words(length_z, mass_z, stiffness * (2.0 / element_dz), inverse_step)
    full = range(REACH - 1, REACH + 2)
    turned = words_z.T
    ends_z = [2 * REACH * length_z] * 8 + [length_z - 1] * 8
    along_z = np.concatenate(
        [np.tile(turned[iz * length_z : (iz + 1) * length_z], (8, 1)) for iz in full]
        + [np.tile(turned[ends_z], (8, 1))],
        axis=0,
    )
    ends = [2 * REACH * length_x, length_x - 1] * 4
    inner = [ix * length_x + half + (-r) % 8 for ix in full for half in (0, 8) for r in range(8)]
    along_x = np.concatenate(
        [words_x[:, inner], words_x[:, ends]]
        + [np.zeros((128, 8))],
        axis=1,
    )
    return plane, lines, columns, along_x, along_z


def split(value):
    high = value.astype(BF16)
    low = (value - high.astype(F32)).astype(BF16)
    return high, low


def dot3(left, right, dims):
    def one(a, b):
        return lax.dot_general(a, b, (dims, ((), ())), preferred_element_type=F32)

    return one(left[0], right[0]) + (one(left[0], right[1]) + one(left[1], right[0]))


NN = ((1,), (0,))
NT = ((1,), (1,))
TN = ((0,), (0,))
DIRS = ((1, 1), (1, -1), (-1, 1), (-1, -1))


def lagrange_rows(coord):
    points = np.array(GLL_NODES)
    scale = 1.0 / np.prod(points[:, None] - points[None, :] + np.eye(8), axis=1)
    shape = (8, coord.shape[1])
    node = lax.broadcasted_iota(jnp.int32, shape, 0)
    total = jnp.zeros(shape, F32)
    for a in range(8):
        total = jnp.where(node == a, F32(scale[a]), total)
    for b in range(8):
        total = total * jnp.where(node == b, F32(1.0), coord - F32(points[b]))
    return total


def kernel(
    n_wall,
    n_span,
    sizes,
    vel_in,
    heights_in,
    owner_in,
    element_in,
    coords_in,
    roughness_in,
    plane_in,
    lines_in,
    columns_in,
    along_x_in,
    along_z_in,
    field,
    factors,
    neumann,
    vel,
    heights,
    owner,
    element,
    coords,
    roughness,
    sheet,
    lines,
    columns,
    along_x,
    along_z,
    load_sem,
    near,
    near_got,
    local,
    face_send,
    face_got,
    parts,
    sum_send,
    wall_got,
    span_got,
    pull_send,
    edge_send,
    pull_got,
    everything,
    sent,
    near_rs,
    pull_rs,
    face_rs,
    wall_rs,
    step_one,
    step_two,
    *span_rs,
):
    length_x, length_z, length_y = sizes
    rows = length_x * length_z
    count_z, count_y = length_z // 8, length_y // 8
    w = lax.axis_index("wall")
    s = lax.axis_index("span")

    def at(dx, dz):
        return (lax.rem(w + (dx + n_wall), n_wall), lax.rem(s + (dz + n_span), n_span))

    loads = {
        name: pltpu.make_async_copy(source, target, load_sem.at[index])
        for index, (name, source, target) in enumerate(
            (
                ("vel", vel_in, vel),
                ("heights", heights_in, heights),
                ("lines", lines_in, lines),
                ("scale", columns_in.at[pl.ds(0, 2)], columns.at[pl.ds(0, 2)]),
                ("plane", plane_in, sheet),
                ("coords", coords_in, coords),
                ("owner", owner_in, owner),
                ("element", element_in, element),
                ("roughness", roughness_in, roughness),
                ("along_x", along_x_in, along_x),
                ("along_z", along_z_in, along_z),
                ("weights", columns_in.at[pl.ds(2, 2)], columns.at[pl.ds(2, 2)]),
            )
        )
    }
    for load in loads.values():
        load.start()

    def loaded(*names):
        for name in names:
            loads[name].wait()

    single = n_wall * n_span <= SINGLE_STAGE
    stepwise = single and 3 <= n_wall <= 4 * REACH and 3 <= n_span <= 4 * REACH
    across_wall = ((1, 0), (-1, 0))
    if stepwise:
        greeted = across_wall + tuple((0, k) for k in range(1, n_span))
    elif single:
        greeted = [divmod(k, n_span) for k in range(1, n_wall * n_span)]
    else:
        greeted = [(k, 0) for k in range(1, n_wall)] + [(0, k) for k in range(1, n_span)]
        greeted += sorted(
            {
                ((dx + n_wall) % n_wall, (dz + n_span) % n_span)
                for dx in range(-REACH, REACH + 1)
                for dz in range(-REACH, REACH + 1)
            }
            - {(0, 0)}
            - set(greeted)
        )
    barrier = pltpu.get_barrier_semaphore()

    def greet(semaphore, places):
        for dx, dz in places:
            pl.semaphore_signal(semaphore, inc=1, device_id=at(dx, dz), device_id_type=MESH)

    greet(barrier, greeted)

    loaded("vel")
    lane = lax.broadcasted_iota(jnp.int32, (64, length_y), 1)
    groups = (length_x // 8) * count_z
    depth = 8 * NEAR
    strips = length_y // depth
    packed = [jnp.zeros((64, length_y), F32)] * 2
    for index, comp in enumerate((0, 2)):
        for group in range(groups):
            ex, ez = group // count_z, group % count_z
            block = vel[comp, pl.ds(ex * 8, 8), pl.ds(ez * 8, 8), :].reshape(64, length_y)
            place = index * groups + group
            moved = pltpu.roll(block, place * depth, 1) if place else block
            for wall_side in range(2):
                strip = (place - wall_side) % strips
                packed[wall_side] = jnp.where(lane // depth == strip, moved, packed[wall_side])
    for wall_side in range(2):
        near[wall_side] = packed[wall_side]
    def remote(src, dst, ss, rs, where):
        return pltpu.make_async_remote_copy(
            src_ref=src,
            dst_ref=dst,
            send_sem=ss,
            recv_sem=rs,
            device_id=where,
            device_id_type=MESH,
        )

    near_copies = []
    for wall_side in range(2):
        for slot, dx in enumerate((1, -1)):
            target = near_got.at[wall_side, slot]
            near_copies.append(
                remote(near.at[wall_side], target, sent, near_rs.at[wall_side], at(dx, 0))
            )

    def enter():
        pl.semaphore_wait(barrier, len(greeted))
        if stepwise:
            greet(step_one, across_wall)
        for copy in near_copies:
            copy.start()

    if stepwise:
        enter()
    loaded("heights", "lines", "scale", "plane")

    layer_of = lax.broadcasted_iota(jnp.int32, (length_y, count_y), 0) // 8
    layer = lax.broadcasted_iota(jnp.int32, (length_y, count_y), 1)
    height_row = heights[...]
    height = jnp.sum(jnp.where(layer_of == layer, height_row, 0.0), axis=1, keepdims=True)
    lines_mass = height * lines[0]
    lines_stiff = lines[1] / height
    stiff_hi, stiff_lo = split(lines_stiff)
    lines_packed = jnp.concatenate(
        [
            jnp.concatenate([stiff_hi, stiff_lo], axis=1),
            jnp.concatenate([stiff_hi, jnp.zeros_like(stiff_lo)], axis=1),
        ],
        axis=0,
    )
    bound = jnp.max(0.1535 * height_row + 0.000182 / height_row, axis=1, keepdims=True)
    shifts = (0.15 * bound, 0.85 * bound)

    mass_row = jnp.sum(lines_mass, axis=0, keepdims=True)
    scale = columns[0] * mass_row
    for c in range(3):
        field[0, c] = vel[c].reshape(rows, length_y) * scale

    face_rows = []
    for slot, (dx, dz) in enumerate(DIRS + ((0, 1), (0, -1), (1, 0), (-1, 0))):
        size = 3 * (1 if dx and dz else length_z if dx else length_x)
        face_rows.append((sum(entry[1] for entry in face_rows), size, dx, dz))
    face_total = sum(entry[1] for entry in face_rows)
    z_first = {entry[3]: entry[0] for entry in face_rows if entry[2] == 0}

    def corner(dx, dz):
        return (rows - length_z if dx == 1 else 0) + (length_z - 1 if dz == 1 else 0)

    def face_part(slot, c, dx, dz):
        first, size = face_rows[slot][0] + c * (face_rows[slot][1] // 3), face_rows[slot][1] // 3
        if dx and dz:
            rows_of = pl.ds(corner(dx, dz), 1)
        elif dx:
            rows_of = pl.ds(rows - length_z if dx == 1 else 0, length_z)
        else:
            rows_of = pl.ds(length_z - 1 if dz == 1 else 0, length_x, stride=length_z)
        return pl.ds(first, size), rows_of

    def send_faces(turn):
        for c in range(3):
            for slot, (_, _, dx, dz) in enumerate(face_rows):
                packed_rows, rows_of = face_part(slot, c, dx, dz)
                face_send[turn, packed_rows, :] = local[turn, c, rows_of, :]
        first_turn = turn == 0 and stepwise
        if turn == 0 and not stepwise:
            enter()
        for stage in ((0,), (2, 1)) if first_turn else ((2, 0, 1),):
            if stage[0] == 2 and first_turn:
                pl.semaphore_wait(step_one, len(across_wall))
                greet(step_two, across_wall)
            for kind in stage:
                for first, size, dx, dz in face_rows:
                    if (2 if dx and dz else abs(dx)) != kind:
                        continue
                    if kind == 0:
                        swap = jnp.where(s == 0, -dz, dz)
                        first = pl.multiple_of(jnp.where(swap == 1, z_first[1], z_first[-1]), 4)
                        dz = swap
                    part = (turn, pl.ds(first, size), slice(None))
                    remote(
                        face_send.at[part],
                        face_got.at[part],
                        sent,
                        face_rs.at[turn],
                        at(dx, dz),
                    ).start()

    def settle(semaphore, ref):
        pltpu.make_async_copy(ref, ref, semaphore).wait()

    def add_faces(turn):
        settle(face_rs.at[turn], face_got.at[turn, pl.ds(0, face_total), :])
        for c in range(3):
            for slot, (_, _, dx, dz) in enumerate(face_rows):
                packed_rows, rows_of = face_part(slot, c, -dx, -dz)
                field[turn + 1, c, rows_of, :] = (
                    field[turn + 1, c, rows_of, :] + face_got[turn, packed_rows, :]
                )

    def inner(quantity, c, product):
        parts[quantity * 8 + c : quantity * 8 + c + 1, :] = jnp.sum(
            product, axis=0, keepdims=True
        )

    def operate(source, target):
        highs, lows = zip(*[split(field[source, c]) for c in range(3)])
        along_y = jnp.dot(
            jnp.concatenate(
                [jnp.concatenate([high, low], axis=1) for high, low in zip(highs, lows)], axis=0
            ),
            lines_packed,
            preferred_element_type=F32,
        )
        across = jnp.dot(
            sheet[0], jnp.concatenate(highs + lows, axis=1), preferred_element_type=F32
        )
        across_low = jnp.dot(sheet[1], jnp.concatenate(highs, axis=1), preferred_element_type=F32)
        for c in range(3):
            here = slice(c * length_y, (c + 1) * length_y)
            also = slice((3 + c) * length_y, (4 + c) * length_y)
            flat = across[:, here] + (across[:, also] + across_low[:, here])
            tall = along_y[c * rows : (c + 1) * rows]
            tall = tall[:, :length_y] + tall[:, length_y:]
            local[target, c] = flat * mass_row + tall * columns[1]

    slots = {(0, 0): 0, (0, 1): 1, (1, 1): 2, (0, 2): 3, (1, 2): 4, (2, 2): 5}

    def inner_products(newest):
        for c in range(3):
            weighted = field[newest, c] * columns[2]
            for other in range(newest + 1):
                inner(slots[(other, newest)], c, weighted * field[other, c])

    operate(0, 0)
    send_faces(0)
    for c in range(3):
        field[1, c] = local[0, c]
    parts[...] = jnp.zeros_like(parts)

    loaded("coords", "owner", "element", "roughness")
    points = owner.shape[1]
    row_x = lagrange_rows(coords[0:1, :])
    row_z = lagrange_rows(coords[1:2, :])
    row_y = lagrange_rows(coords[2:3, :])
    cross = jnp.concatenate([row_x[a : a + 1] * row_z for a in range(8)], axis=0)
    distance = lax.rem(owner[...] - w + n_wall, n_wall)
    from_next = distance == 1
    from_prev = distance == n_wall - 1
    own = jnp.logical_not(jnp.logical_or(from_next, from_prev))
    spread = jnp.concatenate(
        [jnp.where(mask, cross, 0.0) for mask in (own, from_prev, from_next)], axis=0
    )
    half = points // 2
    n_row = lax.broadcasted_iota(jnp.int32, (groups * depth, points), 0)
    side_of = lax.broadcasted_iota(jnp.int32, (groups * depth, points), 1) // half
    layer_y = (n_row % depth) // 8 + side_of * (count_y - NEAR)
    wanted = (n_row // depth) * count_y + layer_y == element[...]
    along = jnp.where(wanted, jnp.concatenate([row_y] * (groups * NEAR), axis=0), 0.0)
    spread = split(spread)
    drag = karman / jnp.log(sample_height / roughness[...])
    drag = drag * drag * (-1.0 / viscosity)

    sampled = []
    for wall_side in range(2):
        settle(near_rs.at[wall_side], near_got.at[wall_side])
        sources = jnp.concatenate(
            [near[wall_side], near_got[wall_side, 0], near_got[wall_side, 1]], axis=0
        )
        here = slice(wall_side * half, (wall_side + 1) * half)
        values = dot3(split(sources), tuple(part[:, here] for part in spread), TN)
        total = []
        for index in range(2):
            strip_rows = [
                (place - wall_side) % strips * depth
                for place in range(index * groups, (index + 1) * groups)
            ]
            own_rows = jnp.concatenate([values[k : k + depth] for k in strip_rows], axis=0)
            total.append(jnp.sum(own_rows * along[:, here], axis=0, keepdims=True))
        sampled.append(total)
    stream, spanwise = [jnp.concatenate(both, axis=1) for both in zip(*sampled)]
    speed = jnp.sqrt(stream * stream + spanwise * spanwise + speed_floor)
    factor = drag * speed
    gradient = (factor * stream, factor * spanwise)
    neumann[0:1, :] = gradient[0]
    neumann[1:2, :] = gradient[1]

    planes = []
    for index in range(2):
        pull = viscosity * gradient[index]
        planes += [pull[:, :rows], pull[:, rows:]]
    tiles = 4 * length_x // 8
    tile_lane = lax.broadcasted_iota(jnp.int32, (8, 128), 1)
    tile_row = lax.broadcasted_iota(jnp.int32, (8, 128), 0)
    block_of = tile_lane // length_z
    bundle = jnp.zeros((8, 128), F32)
    fringe = jnp.zeros((8, 128), F32)
    for tile in range(tiles):
        part = planes[tile // 2][:, 128 * (tile % 2) : 128 * (tile % 2) + 128]
        part = jnp.broadcast_to(part, (8, 128))
        spread_rows = pltpu.roll(part, 0, 1, stride=length_z, stride_axis=0)
        spread_rows = pltpu.roll(spread_rows, (8 - tile) % 8, 0)
        bundle = jnp.where(block_of == tile, spread_rows, bundle)
        for end in range(2):
            turned = pltpu.roll(part, 7 * (1 - end), 1, stride=length_z - 1, stride_axis=0)
            wanted_lane = tile * length_z + 8 * end + 7 - tile_row
            fringe = jnp.where(tile_lane == wanted_lane, turned, fringe)
    pull_send[...] = bundle
    edge_send[0:1, :] = jnp.sum(fringe, axis=0, keepdims=True)
    edge_send[1:2, :] = jnp.where(block_of[0:1] % 2 == 0, bundle[0:1], bundle[1:2])
    if stepwise:
        pl.semaphore_wait(step_two, len(across_wall))
    reach = 2 * REACH + 1
    offsets = [
        (dx, dz)
        for dx in range(-REACH, REACH + 1)
        for dz in range(-REACH, REACH + 1)
        if (dx, dz) != (0, 0)
    ]
    nearby = [place for place in offsets if max(abs(place[0]), abs(place[1])) < REACH]
    remaining = [place for place in offsets if place not in nearby]
    pull_rows = {place: pl.ds(8 * index, 8) for index, place in enumerate(nearby)}
    for index, place in enumerate(remaining):
        pull_rows[place] = pl.ds(8 * len(nearby) + index, 1)
    for dx, dz in sorted(offsets, key=lambda pair: -abs(pair[0]) - abs(pair[1])):
        if (dx, dz) in nearby:
            source = pull_send
        else:
            source = edge_send.at[pl.ds(0 if abs(dz) == REACH else 1, 1), :]
        remote(
            source, pull_got.at[pull_rows[(-dx, -dz)], :], sent, pull_rs, at(dx, dz)
        ).start()

    add_faces(0)
    operate(1, 1)
    send_faces(1)
    for c in range(3):
        field[2, c] = local[1, c]
    loaded("along_x", "along_z", "weights")
    lines_rows = jnp.concatenate([lines_mass, lines_stiff], axis=1)
    ends = [lines_rows[0:1], lines_rows[length_y - 1 : length_y]]
    once = [(end[:, :length_y], end[:, length_y:]) for end in ends]
    twice = dot3(
        split(jnp.concatenate([once[0][0], once[0][1], once[1][0], once[1][1]] * 2, axis=0)),
        split(lines_rows),
        NN,
    )
    one_lane = lax.broadcasted_iota(jnp.int32, (1, length_y), 1)
    zero = jnp.zeros((1, length_y), F32)
    images = []
    for side in range(2):
        by_mass, by_stiff = twice[2 * side : 2 * side + 1], twice[2 * side + 1 : 2 * side + 2]
        moved_tip = jnp.where(one_lane == length_y // 2 - side, 1.0, 0.0)
        rows_of = [
            (zero, moved_tip),
            (zero, once[side][0]),
            (zero, once[side][1]),
            (by_mass[:, :length_y], zero),
            (by_stiff[:, :length_y], zero),
            (by_mass[:, length_y:], zero),
            (by_stiff[:, length_y:], zero),
        ]
        for entry in rows_of:
            image = jnp.concatenate(entry, axis=1)
            images.append(jnp.broadcast_to(image, (length_z, 2 * length_y)))
        images.append(jnp.zeros((128 - 7 * length_z, 2 * length_y), F32))
    images = split(jnp.concatenate(images, axis=0))
    low_half = tile_lane & 8 == 0
    low_rows = tile_row & 1 == 0
    diagonal_of = (tile_lane + tile_row) & 7
    settle(pull_rs, pull_got)

    def edge(dx, dz):
        return jnp.broadcast_to(pull_got[pull_rows[(dx, dz)], :], (8, 128))

    def both_ends(dx):
        return jnp.where(low_half, edge(dx, REACH), edge(dx, -REACH))

    middle = range(-REACH + 1, REACH)
    spans = []
    for dx in middle:
        ends = both_ends(dx)
        parts_z = [bundle if (dx, dz) == (0, 0) else pull_got[pull_rows[(dx, dz)], :] for dz in middle]
        for tile in range(tiles):
            pieces = [jnp.where(block_of == tile, part, 0.0) for part in parts_z]
            kept = jnp.logical_and(block_of == tile, diagonal_of == (7 - tile) % 8)
            pieces.append(jnp.where(kept, ends, 0.0))
            spans.append(jnp.concatenate(pieces, axis=1))
    pieces = [
        jnp.where(block_of == tile_row, jnp.where(low_rows, edge(REACH, dz), edge(-REACH, dz)), 0.0)
        for dz in middle
    ]
    kept = jnp.logical_and(
        block_of == tile_row, (tile_lane + tile_row + (tile_row & 1)) & 7 == 7
    )
    ends = jnp.where(low_rows, both_ends(REACH), both_ends(-REACH))
    pieces.append(jnp.where(kept, ends, 0.0))
    spans.append(jnp.concatenate(pieces, axis=1))
    spans.append(jnp.zeros((8, 512), F32))
    spans_hi, spans_lo = split(jnp.concatenate(spans, axis=0))
    reached = jnp.dot(spans_hi, along_z[...], preferred_element_type=F32)
    reached = (reached[:, :128] + reached[:, 128:]) + jnp.dot(
        spans_lo, along_z[:, :128], preferred_element_type=F32
    )
    by_plane = []
    for plane in range(4):
        kept = [
            reached[ix * 64 + plane * length_x : ix * 64 + (plane + 1) * length_x]
            for ix in range(len(middle))
        ]
        last = reached[64 * len(middle) : 64 * len(middle) + 8]
        kept.append(jnp.where(tile_row // 2 == plane, last, 0.0))
        kept.append(jnp.zeros((8, 128), F32))
        by_plane.append(jnp.concatenate(kept, axis=0))
    stacked_hi, stacked_lo = split(jnp.concatenate(by_plane, axis=1))
    both_ways = jnp.dot(
        along_x[...],
        jnp.concatenate([stacked_hi, stacked_lo, stacked_hi], axis=0),
        preferred_element_type=F32,
    )
    block_lane = lax.broadcasted_iota(jnp.int32, (length_x, 128), 1) // length_z
    keep_row = lax.rem(lax.broadcasted_iota(jnp.int32, (rows, 256), 0), length_z)
    keep_lane = lax.rem(lax.broadcasted_iota(jnp.int32, (rows, 256), 1), length_z)
    wall_lane = lax.broadcasted_iota(jnp.int32, (rows, length_y), 1)
    tractions = []
    for index in range(2):
        blocks = []
        for side in range(2):
            plane = index * 2 + side
            total = jnp.zeros((length_x, 128), F32)
            for block, word_x, word_z in TERMS:
                piece = both_ways[
                    word_x * length_x : (word_x + 1) * length_x, plane * 128 : plane * 128 + 128
                ]
                shift = ((block - word_z) * length_z) % 128
                moved = pltpu.roll(piece, shift, 1) if shift else piece
                total = total + jnp.where(block_lane == block, moved, 0.0)
            blocks.append(total)
        wide = jnp.concatenate(blocks, axis=1)
        tall = jnp.concatenate(
            [jnp.broadcast_to(wide[x : x + 1], (length_z, 256)) for x in range(length_x)], axis=0
        )
        tall = jnp.where(keep_row == keep_lane, tall, 0.0)
        deep = dot3(split(tall), images, NN)
        level_two, shallow = deep[:, :length_y], deep[:, length_y:]
        tip = jnp.logical_or(wall_lane == 0, wall_lane == length_y - 1)
        level_zero = jnp.where(tip, pltpu.roll(shallow, length_y // 2, 1), 0.0)
        outside = jnp.logical_or(wall_lane < length_y // 4, wall_lane >= 3 * length_y // 4)
        level_one = jnp.where(outside, shallow, 0.0)
        tractions.append((level_zero, level_one, level_two))
    t1, t2 = shifts
    for c in range(3):
        chain = [field[level, c] for level in range(3)]
        if c != 1:
            taus = tractions[c // 2]
            chain = [chain[level] + taus[level] for level in range(3)]
        v1 = chain[1] - t1 * chain[0]
        field[0, c] = chain[0]
        field[1, c] = v1
        field[2, c] = chain[2] - t1 * chain[1] - t2 * v1
    for newest in range(2):
        inner_products(newest)
    add_faces(1)
    highs = [field[2, c].astype(BF16) for c in range(3)]
    along_y = jnp.dot(
        jnp.concatenate(highs, axis=0), lines_packed[:length_y], preferred_element_type=F32
    )
    wide = jnp.concatenate(highs, axis=1)
    across = jnp.dot(sheet[0], wide, preferred_element_type=F32)
    across_low = jnp.dot(sheet[1], wide, preferred_element_type=F32)
    inner_products(2)
    for c in range(3):
        here = slice(c * length_y, (c + 1) * length_y)
        tall = along_y[c * rows : (c + 1) * rows]
        tall = tall[:, :length_y] + tall[:, length_y:]
        image = (across[:, here] + across_low[:, here]) * mass_row + tall * columns[1]
        value = field[2, c]
        partner = value + (value - highs[c].astype(F32))
        inner(6, c, partner * columns[3] * image)

    total_rows = parts.shape[0]
    r_iota = lax.broadcasted_iota(jnp.int32, (total_rows, 128), 0)
    l_iota = lax.broadcasted_iota(jnp.int32, (total_rows, 128), 1)
    diagonal = r_iota == l_iota
    end_lane = lax.broadcasted_iota(jnp.int32, (total_rows, 128), 1)
    shared = jnp.logical_or(end_lane % 8 == 0, end_lane % 8 == 7)
    tips = jnp.logical_or(end_lane == 0, end_lane == length_y - 1)
    weight_y = jnp.where(jnp.logical_and(shared, jnp.logical_not(tips)), 0.5, 1.0)
    summed = jnp.sum(parts[...] * weight_y, axis=1, keepdims=True)
    row = jnp.sum(jnp.where(diagonal, summed, 0.0), axis=0, keepdims=True)

    def gather_sum(stage, row, count, got, rs, place):
        sum_send[stage : stage + 1, :] = row
        for k in range(1, count):
            remote(
                sum_send.at[pl.ds(stage, 1), :], got.at[pl.ds(k - 1, 1), :], sent, rs, place(k)
            ).start()
        settle(rs, got)
        return row + jnp.sum(got[...], axis=0, keepdims=True)

    sum_rows = 0
    if single:
        every = n_wall * n_span
        row = gather_sum(0, row, every, wall_got, wall_rs, lambda k: at(k // n_span, k % n_span))
        sum_rows = every - 1
    else:
        row = gather_sum(0, row, n_wall, wall_got, wall_rs, lambda k: at(k, 0))
        row = gather_sum(1, row, n_span, span_got, span_rs[0], lambda k: at(0, k))
        sum_rows = n_wall + n_span - 2
    sent_rows = 2 * 2 * 64 + pull_got.shape[0] + ROUNDS * face_total + sum_rows
    settle(sent, everything.at[pl.ds(0, sent_rows), :])
    totals = jnp.sum(jnp.where(diagonal, row, 0.0), axis=1, keepdims=True)
    m00, m01, m11, m02, m12, m22, e22 = [totals[q * 8 : q * 8 + 8, :] for q in range(7)]
    t1, t2 = shifts
    a00 = m01 + t1 * m00
    a01 = m11 + t1 * m01
    a02 = m12 + t1 * m02
    a11 = m12 + t2 * m11
    a12 = m22 + t2 * m12
    l10 = a01 / a00
    l20 = a02 / a00
    d1 = a11 - l10 * a01
    u12 = a12 - l10 * a02
    l21 = u12 / d1
    d2 = e22 - l20 * a02 - l21 * u12
    y1 = m01 - l10 * m00
    y2 = m02 - l20 * m00 - l21 * y1
    x2 = y2 / d2
    x1 = y1 / d1 - l21 * x2
    x0 = m00 / a00 - l10 * x1 - l20 * x2
    for index, value in enumerate((x0, x1, x2)):
        factors[index] = jnp.broadcast_to(value, (8, 128))


def combine(field, factors, neumann_in, out, neumann, stage, sems):
    small = pltpu.make_async_copy(neumann_in, neumann, sems.at[3])
    small.start()
    copies = []
    for c in range(3):
        result = factors[0, c : c + 1] * field[0, c]
        for level in range(1, 3):
            result += factors[level, c : c + 1] * field[level, c]
        stage[c] = result.reshape(stage.shape[1:])
        copy = pltpu.make_async_copy(stage.at[c], out.at[c], sems.at[c])
        copy.start()
        copies.append(copy)
    for copy in copies:
        copy.wait()
    small.wait()


def body(n_wall, n_span, velocity_old, heights, owner_device, owner_element, ref_coords, roughness):
    sizes = velocity_old.shape[1:]
    length_x, length_z, length_y = sizes
    rows = length_x * length_z
    points = owner_device.shape[0]
    plane, lines, columns, along_x, along_z = tables(*sizes)
    along_x_hi, along_x_lo = split_np(along_x)
    every = n_wall * n_span
    first = every if every <= SINGLE_STAGE else n_wall
    faces = -(-(6 * (length_x + length_z) + 12) // 8) * 8
    vmem = pl.BlockSpec(memory_space=pltpu.VMEM)
    hbm = pl.BlockSpec(memory_space=pltpu.HBM)
    operands = (
        velocity_old,
        heights.reshape(1, -1),
        owner_device.reshape(1, -1),
        owner_element.reshape(1, -1),
        ref_coords,
        roughness.reshape(1, -1),
        jnp.stack(split_np(plane)),
        jnp.asarray(lines, F32),
        jnp.asarray(columns, F32),
        jnp.concatenate([along_x_hi, along_x_hi, along_x_lo], axis=1),
        jnp.concatenate(split_np(along_z), axis=1),
    )
    dma = pltpu.SemaphoreType.DMA
    field, factors, neumann = pl.pallas_call(
        functools.partial(kernel, n_wall, n_span, sizes),
        out_shape=(
            pltpu.VMEM((3, 3, rows, length_y), F32),
            pltpu.VMEM((3, 8, 128), F32),
            pltpu.VMEM((2, points), F32),
        ),
        in_specs=[hbm] * 11,
        out_specs=(vmem, vmem, vmem),
        scratch_shapes=[pltpu.VMEM(value.shape, value.dtype) for value in operands]
        + [
            dma((12,)),
            pltpu.VMEM((2, 64, length_y), F32),
            pltpu.VMEM((2, 2, 64, length_y), F32),
            pltpu.VMEM((ROUNDS, 3, rows, length_y), F32),
            pltpu.VMEM((ROUNDS, faces, length_y), F32),
            pltpu.VMEM((ROUNDS, faces, length_y), F32),
            pltpu.VMEM((56, length_y), F32),
            pltpu.VMEM((2, 128), F32),
            pltpu.VMEM((first - 1, 128), F32),
            pltpu.VMEM((n_span - 1, 128), F32),
            pltpu.VMEM((8, 128), F32),
            pltpu.VMEM((8, 128), F32),
            pltpu.VMEM((80, 128), F32),
            pltpu.VMEM((896, length_y), F32),
            dma,
            dma((2,)),
            dma,
            dma((ROUNDS,)),
            dma,
            pltpu.SemaphoreType.REGULAR,
            pltpu.SemaphoreType.REGULAR,
        ]
        + ([] if every <= SINGLE_STAGE else [dma]),
        compiler_params=pltpu.CompilerParams(
            collective_id=0, has_side_effects=True, vmem_limit_bytes=VMEM_LIMIT
        ),
    )(*[pltpu.with_memory_space_constraint(value, pltpu.HBM) for value in operands])
    return pl.pallas_call(
        combine,
        out_shape=(
            jax.ShapeDtypeStruct(velocity_old.shape, F32),
            jax.ShapeDtypeStruct((2, points), F32),
        ),
        in_specs=[vmem] * 3,
        out_specs=(hbm, hbm),
        scratch_shapes=[pltpu.VMEM(velocity_old.shape, F32), dma((4,))],
        compiler_params=pltpu.CompilerParams(vmem_limit_bytes=VMEM_LIMIT),
    )(field, factors, neumann)


def solution(mesh):
    placed = (
        P(None, "wall", "span", None),
        P(),
        P(("wall", "span"), None),
        P(("wall", "span"), None),
        P(None, ("wall", "span")),
        P(("wall", "span")),
    )
    return jax.shard_map(
        functools.partial(body, mesh.shape["wall"], mesh.shape["span"]),
        mesh=mesh,
        in_specs=placed,
        out_specs=(P(None, "wall", "span", None), P(None, ("wall", "span"))),
        check_vma=False,
    )
```

```python
import functools

import jax
import jax.numpy as jnp
import numpy as np
from jax import lax
from jax.experimental import pallas as pl
from jax.experimental.pallas import tpu as pltpu
from jax.sharding import PartitionSpec as P

GLL_NODES = (
    -1.0,
    -0.8717401485096066,
    -0.5917001814331423,
    -0.2092992179024789,
    0.2092992179024789,
    0.5917001814331423,
    0.8717401485096066,
    1.0,
)
GLL_WEIGHTS = (
    0.03571428571428571,
    0.2107042271435061,
    0.3411226924835044,
    0.4124587946587038,
    0.4124587946587038,
    0.3411226924835044,
    0.2107042271435061,
    0.03571428571428571,
)
viscosity = 0.02
inverse_step = 20.0
karman = 0.41
sample_height = 0.1
speed_floor = 0.01
element_dx = 0.05
element_dz = 0.13
NEAR = 2
ROUNDS = 2
REACH = 2
TERMS = (
    (0, 0, 0),
    (1, 1, 2),
    (1, 2, 1),
    (2, 2, 2),
    (3, 3, 6),
    (3, 4, 5),
    (3, 5, 4),
    (3, 6, 3),
    (4, 4, 6),
    (4, 6, 4),
    (5, 5, 6),
    (5, 6, 5),
    (6, 6, 6),
)
SINGLE_STAGE = 64
VMEM_LIMIT = 32 * 2**20
MESH = pl.DeviceIdType.MESH
F32 = jnp.float32
BF16 = jnp.bfloat16


def stiffness_table():
    points = np.array(GLL_NODES)
    weights = np.array(GLL_WEIGHTS)
    previous = np.ones(8)
    current = points.copy()
    for degree in range(1, 7):
        previous, current = (
            current,
            ((2 * degree + 1) * points * current - degree * previous) / (degree + 1),
        )
    derivative = np.zeros((8, 8))
    for target in range(8):
        for source in range(8):
            if target != source:
                derivative[target, source] = (
                    current[target] / current[source] / (points[target] - points[source])
                )
    derivative[0, 0] = -14.0
    derivative[7, 7] = 14.0
    return derivative.T @ (weights[:, None] * derivative)


def join_matrix(length):
    joined = np.eye(length)
    for left in range(7, length - 1, 8):
        joined[left, left + 1] = 1.0
        joined[left + 1, left] = 1.0
    return joined


def face_weights(length, open_ends):
    values = np.ones(length)
    position = np.arange(length) % 8
    values[(position == 0) | (position == 7)] = 0.5
    if open_ends:
        values[0] = 1.0
        values[-1] = 1.0
    return values


def split_np(matrix):
    single = jnp.asarray(matrix, F32)
    high = single.astype(BF16)
    low = (jnp.asarray(matrix, F32) - high.astype(F32)).astype(BF16)
    return high, low


def tables(length_x, length_z, length_y):
    weights = np.array(GLL_WEIGHTS)
    stiffness = stiffness_table()
    count_x, count_z, count_y = length_x // 8, length_z // 8, length_y // 8
    mass_x = np.tile(0.5 * element_dx * weights, count_x)
    mass_z = np.tile(0.5 * element_dz * weights, count_z)
    stiff_x = np.kron(np.eye(count_x), stiffness * (2.0 / element_dx))
    stiff_z = np.kron(np.eye(count_z), stiffness * (2.0 / element_dz))
    mass_xz = np.kron(mass_x, mass_z)
    join_xz = np.kron(join_matrix(length_x), join_matrix(length_z))
    join_y = join_matrix(length_y)
    plane = viscosity * (
        np.kron(stiff_x, np.diag(mass_z)) + np.kron(np.diag(mass_x), stiff_z)
    ) + inverse_step * np.diag(mass_xz)
    plane = join_xz @ plane
    mass_plane = join_xz @ mass_xz
    lines_mass = np.tile(0.5 * weights, count_y)[:, None] * join_y
    lines_stiff = viscosity * 2.0 * (np.kron(np.eye(count_y), stiffness) @ join_y)
    lines = np.stack([lines_mass, lines_stiff])
    ring_x = join_matrix(length_x) @ mass_x
    ring_z = join_matrix(length_z) @ mass_z
    ring_x[0] *= 2.0
    ring_x[-1] *= 2.0
    ring_z[0] *= 2.0
    ring_z[-1] *= 2.0
    assembled = inverse_step * np.kron(ring_x, ring_z)
    inner_x = face_weights(length_x, True)
    inner_z = face_weights(length_z, True)
    outer_x = face_weights(length_x, False)
    outer_z = face_weights(length_z, False)
    steps_x, steps_z = np.arange(length_x), np.arange(length_z)
    fringe = np.concatenate(
        [
            steps_x * length_z + length_z - 1,
            steps_x * length_z,
            (length_x - 1) * length_z + steps_z,
            steps_z,
        ]
    )
    outer, inner = np.kron(outer_x, outer_z), np.kron(inner_x, inner_z)
    columns = np.concatenate([assembled, mass_plane, mass_plane[fringe], outer, inner])
    columns = columns.reshape(-1, 1) * np.ones(length_y)[None]
    plane = np.concatenate([plane, plane[fringe]], axis=0)
    reach = 2 * REACH + 1

    def words(length, mass, stiff, extra):
        size = reach * length
        join = join_matrix(size)
        light = join @ np.diag(np.tile(mass, reach))
        heavy = viscosity * join @ np.kron(np.eye(size // 8), stiff) + extra * light
        chains = [
            light,
            heavy @ light,
            light @ light,
            heavy @ heavy @ light,
            heavy @ light @ light,
            light @ heavy @ light,
            light @ light @ light,
        ]
        middle = REACH * length
        chains = [chain[middle : middle + length] for chain in chains]
        return np.concatenate(chains + [np.zeros((128 - 7 * length, size))], axis=0)

    words_x = words(length_x, mass_x, stiffness * (2.0 / element_dx), 0.0)
    words_z = words(length_z, mass_z, stiffness * (2.0 / element_dz), inverse_step)
    full = range(REACH - 1, REACH + 2)
    turned = words_z.T
    ends_z = [2 * REACH * length_z] * 8 + [length_z - 1] * 8
    along_z = np.concatenate(
        [np.tile(turned[iz * length_z : (iz + 1) * length_z], (8, 1)) for iz in full]
        + [np.tile(turned[ends_z], (8, 1))],
        axis=0,
    )
    ends = [2 * REACH * length_x, length_x - 1] * 4
    inner = [ix * length_x + half + (-r) % 8 for ix in full for half in (0, 8) for r in range(8)]
    along_x = np.concatenate(
        [words_x[:, inner], words_x[:, ends]]
        + [np.zeros((128, 8))],
        axis=1,
    )
    return plane, lines, columns, along_x, along_z


def split(value):
    high = value.astype(BF16)
    low = (value - high.astype(F32)).astype(BF16)
    return high, low


def dot3(left, right, dims):
    def one(a, b):
        return lax.dot_general(a, b, (dims, ((), ())), preferred_element_type=F32)

    return one(left[0], right[0]) + (one(left[0], right[1]) + one(left[1], right[0]))


NN = ((1,), (0,))
NT = ((1,), (1,))
TN = ((0,), (0,))
DIRS = ((1, 1), (1, -1), (-1, 1), (-1, -1))


def lagrange_rows(coord):
    points = np.array(GLL_NODES)
    scale = 1.0 / np.prod(points[:, None] - points[None, :] + np.eye(8), axis=1)
    shape = (8, coord.shape[1])
    node = lax.broadcasted_iota(jnp.int32, shape, 0)
    total = jnp.zeros(shape, F32)
    for a in range(8):
        total = jnp.where(node == a, F32(scale[a]), total)
    for b in range(8):
        total = total * jnp.where(node == b, F32(1.0), coord - F32(points[b]))
    return total


def kernel(
    n_wall,
    n_span,
    sizes,
    vel_in,
    heights_in,
    owner_in,
    element_in,
    coords_in,
    roughness_in,
    plane_in,
    lines_in,
    columns_in,
    along_x_in,
    along_z_in,
    field,
    factors,
    neumann,
    vel,
    heights,
    owner,
    element,
    coords,
    roughness,
    sheet,
    lines,
    columns,
    along_x,
    along_z,
    load_sem,
    near,
    near_got,
    face_send,
    face_got,
    parts,
    sum_send,
    wall_got,
    span_got,
    pull_send,
    edge_send,
    pull_got,
    everything,
    sent,
    near_rs,
    pull_rs,
    face_rs,
    wall_rs,
    step_one,
    step_two,
    *span_rs,
):
    length_x, length_z, length_y = sizes
    rows = length_x * length_z
    count_z, count_y = length_z // 8, length_y // 8
    w = lax.axis_index("wall")
    s = lax.axis_index("span")

    def at(dx, dz):
        return (lax.rem(w + (dx + n_wall), n_wall), lax.rem(s + (dz + n_span), n_span))

    edges = 2 * (length_x + length_z)
    early, late = pl.ds(0, 2 * rows + edges), pl.ds(2 * rows + edges, 2 * rows)

    def column(index):
        first = index * rows + (edges if index > 1 else 0)
        return columns[first : first + rows, :]

    loads = {
        name: pltpu.make_async_copy(source, target, load_sem.at[index])
        for index, (name, source, target) in enumerate(
            (
                ("vel", vel_in, vel),
                ("heights", heights_in, heights),
                ("lines", lines_in, lines),
                ("scale", columns_in.at[early], columns.at[early]),
                ("plane", plane_in, sheet),
                ("coords", coords_in, coords),
                ("owner", owner_in, owner),
                ("element", element_in, element),
                ("roughness", roughness_in, roughness),
                ("along_x", along_x_in, along_x),
                ("along_z", along_z_in, along_z),
                ("weights", columns_in.at[late], columns.at[late]),
            )
        )
    }
    for load in loads.values():
        load.start()

    def loaded(*names):
        for name in names:
            loads[name].wait()

    single = n_wall * n_span <= SINGLE_STAGE
    stepwise = single and 3 <= n_wall <= 4 * REACH and 3 <= n_span <= 4 * REACH
    across_wall = ((1, 0), (-1, 0))
    if stepwise:
        greeted = across_wall + tuple((0, k) for k in range(1, n_span))
    elif single:
        greeted = [divmod(k, n_span) for k in range(1, n_wall * n_span)]
    else:
        greeted = [(k, 0) for k in range(1, n_wall)] + [(0, k) for k in range(1, n_span)]
        greeted += sorted(
            {
                ((dx + n_wall) % n_wall, (dz + n_span) % n_span)
                for dx in range(-REACH, REACH + 1)
                for dz in range(-REACH, REACH + 1)
            }
            - {(0, 0)}
            - set(greeted)
        )
    barrier = pltpu.get_barrier_semaphore()

    def greet(semaphore, places):
        for dx, dz in places:
            pl.semaphore_signal(semaphore, inc=1, device_id=at(dx, dz), device_id_type=MESH)

    greet(barrier, greeted)

    loaded("vel")
    lane = lax.broadcasted_iota(jnp.int32, (64, length_y), 1)
    groups = (length_x // 8) * count_z
    depth = 8 * NEAR
    strips = length_y // depth
    packed = [jnp.zeros((64, length_y), F32)] * 2
    for index, comp in enumerate((0, 2)):
        for group in range(groups):
            ex, ez = group // count_z, group % count_z
            block = vel[comp, pl.ds(ex * 8, 8), pl.ds(ez * 8, 8), :].reshape(64, length_y)
            place = index * groups + group
            moved = pltpu.roll(block, place * depth, 1) if place else block
            for wall_side in range(2):
                strip = (place - wall_side) % strips
                packed[wall_side] = jnp.where(lane // depth == strip, moved, packed[wall_side])
    for wall_side in range(2):
        near[wall_side] = packed[wall_side]
    def remote(src, dst, ss, rs, where):
        return pltpu.make_async_remote_copy(
            src_ref=src,
            dst_ref=dst,
            send_sem=ss,
            recv_sem=rs,
            device_id=where,
            device_id_type=MESH,
        )

    near_copies = []
    for wall_side in range(2):
        for slot, dx in enumerate((1, -1)):
            target = near_got.at[wall_side, slot]
            near_copies.append(
                remote(near.at[wall_side], target, sent, near_rs.at[wall_side], at(dx, 0))
            )

    def enter():
        pl.semaphore_wait(barrier, len(greeted))
        if stepwise:
            greet(step_one, across_wall)
        for copy in near_copies:
            copy.start()

    if stepwise:
        enter()
    loaded("heights", "lines", "scale", "plane")

    layer_of = lax.broadcasted_iota(jnp.int32, (length_y, count_y), 0) // 8
    layer = lax.broadcasted_iota(jnp.int32, (length_y, count_y), 1)
    height_row = heights[...]
    height = jnp.sum(jnp.where(layer_of == layer, height_row, 0.0), axis=1, keepdims=True)
    lines_mass = height * lines[0]
    lines_stiff = lines[1] / height
    stiff_hi, stiff_lo = split(lines_stiff)
    lines_packed = jnp.concatenate(
        [
            jnp.concatenate([stiff_hi, stiff_lo], axis=1),
            jnp.concatenate([stiff_hi, jnp.zeros_like(stiff_lo)], axis=1),
        ],
        axis=0,
    )
    bound = jnp.max(0.1535 * height_row + 0.000182 / height_row, axis=1, keepdims=True)
    shifts = (0.15 * bound, 0.85 * bound)

    mass_row = jnp.sum(lines_mass, axis=0, keepdims=True)
    scale = column(0) * mass_row
    for c in range(3):
        field[0, c] = vel[c].reshape(rows, length_y) * scale

    face_rows = []
    for slot, (dx, dz) in enumerate(DIRS + ((0, 1), (0, -1), (1, 0), (-1, 0))):
        size = 3 * (1 if dx and dz else length_z if dx else length_x)
        face_rows.append((sum(entry[1] for entry in face_rows), size, dx, dz))
    face_total = sum(entry[1] for entry in face_rows)
    z_first = {entry[3]: entry[0] for entry in face_rows if entry[2] == 0}

    def corner(dx, dz):
        return (rows - length_z if dx == 1 else 0) + (length_z - 1 if dz == 1 else 0)

    def face_part(slot, c, dx, dz):
        first, size = face_rows[slot][0] + c * (face_rows[slot][1] // 3), face_rows[slot][1] // 3
        if dx and dz:
            rows_of = pl.ds(corner(dx, dz), 1)
        elif dx:
            rows_of = pl.ds(rows - length_z if dx == 1 else 0, length_z)
        else:
            rows_of = pl.ds(length_z - 1 if dz == 1 else 0, length_x, stride=length_z)
        return pl.ds(first, size), rows_of

    def send_faces(turn, fringe):
        for c in range(3):
            for slot, (first, size, dx, dz) in enumerate(face_rows):
                size //= 3
                if dx and dz:
                    begin = 2 * length_x + (length_z if dx == -1 else 0)
                    begin += length_z - 1 if dz == 1 else 0
                elif dx:
                    begin = 2 * length_x + (length_z if dx == -1 else 0)
                else:
                    begin = length_x if dz == -1 else 0
                rows_here = slice(first + c * size, first + (c + 1) * size)
                face_send[turn, rows_here, :] = fringe[c][begin : begin + size]
        first_turn = turn == 0 and stepwise
        if turn == 0 and not stepwise:
            enter()
        for stage in ((0,), (2, 1)) if first_turn else ((2, 0, 1),):
            if stage[0] == 2 and first_turn:
                pl.semaphore_wait(step_one, len(across_wall))
                greet(step_two, across_wall)
            for kind in stage:
                for first, size, dx, dz in face_rows:
                    if (2 if dx and dz else abs(dx)) != kind:
                        continue
                    if kind == 0:
                        swap = jnp.where(s == 0, -dz, dz)
                        first = pl.multiple_of(jnp.where(swap == 1, z_first[1], z_first[-1]), 4)
                        dz = swap
                    part = (turn, pl.ds(first, size), slice(None))
                    remote(
                        face_send.at[part],
                        face_got.at[part],
                        sent,
                        face_rs.at[turn],
                        at(dx, dz),
                    ).start()

    def settle(semaphore, ref):
        pltpu.make_async_copy(ref, ref, semaphore).wait()

    def add_faces(turn):
        settle(face_rs.at[turn], face_got.at[turn, pl.ds(0, face_total), :])
        for c in range(3):
            for slot, (_, _, dx, dz) in enumerate(face_rows):
                packed_rows, rows_of = face_part(slot, c, -dx, -dz)
                field[turn + 1, c, rows_of, :] = (
                    field[turn + 1, c, rows_of, :] + face_got[turn, packed_rows, :]
                )

    def inner(quantity, c, product):
        parts[quantity * 8 + c : quantity * 8 + c + 1, :] = jnp.sum(
            product, axis=0, keepdims=True
        )

    def operate(turn):
        highs, lows = zip(*[split(field[turn, c]) for c in range(3)])
        packed = [jnp.concatenate(pair, axis=1) for pair in zip(highs, lows)]
        wide = jnp.concatenate(highs + lows, axis=1)
        wide_high = jnp.concatenate(highs, axis=1)

        def image(first, count, lines_of, weight):
            along_y = jnp.dot(
                jnp.concatenate(lines_of, axis=0), lines_packed, preferred_element_type=F32
            )
            part = slice(first, first + count)
            across = jnp.dot(sheet[0, part], wide, preferred_element_type=F32)
            across_low = jnp.dot(sheet[1, part], wide_high, preferred_element_type=F32)
            results = []
            for c in range(3):
                here = slice(c * length_y, (c + 1) * length_y)
                also = slice((3 + c) * length_y, (4 + c) * length_y)
                flat = across[:, here] + (across[:, also] + across_low[:, here])
                tall = along_y[c * count : (c + 1) * count]
                tall = tall[:, :length_y] + tall[:, length_y:]
                results.append(flat * mass_row + tall * weight)
            return results

        lines_of = []
        for c in range(3):
            value = jnp.concatenate(
                [
                    field[turn, c, pl.ds(length_z - 1, length_x, stride=length_z), :],
                    field[turn, c, pl.ds(0, length_x, stride=length_z), :],
                    field[turn, c, pl.ds(rows - length_z, length_z), :],
                    field[turn, c, pl.ds(0, length_z), :],
                ],
                axis=0,
            )
            lines_of.append(jnp.concatenate(split(value), axis=1))
        weight = columns[2 * rows : 2 * rows + edges, :]
        send_faces(turn, image(rows, edges, lines_of, weight))
        for c, value in enumerate(image(0, rows, packed, column(1))):
            field[turn + 1, c] = value

    slots = {(0, 0): 0, (0, 1): 1, (1, 1): 2, (0, 2): 3, (1, 2): 4, (2, 2): 5}

    def inner_products(newest):
        for c in range(3):
            weighted = field[newest, c] * column(2)
            for other in range(newest + 1):
                inner(slots[(other, newest)], c, weighted * field[other, c])

    operate(0)
    parts[...] = jnp.zeros_like(parts)

    loaded("coords", "owner", "element", "roughness")
    points = owner.shape[1]
    row_x = lagrange_rows(coords[0:1, :])
    row_z = lagrange_rows(coords[1:2, :])
    row_y = lagrange_rows(coords[2:3, :])
    cross = jnp.concatenate([row_x[a : a + 1] * row_z for a in range(8)], axis=0)
    distance = lax.rem(owner[...] - w + n_wall, n_wall)
    from_next = distance == 1
    from_prev = distance == n_wall - 1
    own = jnp.logical_not(jnp.logical_or(from_next, from_prev))
    spread = jnp.concatenate(
        [jnp.where(mask, cross, 0.0) for mask in (own, from_prev, from_next)], axis=0
    )
    half = points // 2
    n_row = lax.broadcasted_iota(jnp.int32, (groups * depth, points), 0)
    side_of = lax.broadcasted_iota(jnp.int32, (groups * depth, points), 1) // half
    layer_y = (n_row % depth) // 8 + side_of * (count_y - NEAR)
    wanted = (n_row // depth) * count_y + layer_y == element[...]
    along = jnp.where(wanted, jnp.concatenate([row_y] * (groups * NEAR), axis=0), 0.0)
    spread = split(spread)
    drag = karman / jnp.log(sample_height / roughness[...])
    drag = drag * drag * (-1.0 / viscosity)

    sampled = []
    for wall_side in range(2):
        settle(near_rs.at[wall_side], near_got.at[wall_side])
        sources = jnp.concatenate(
            [near[wall_side], near_got[wall_side, 0], near_got[wall_side, 1]], axis=0
        )
        here = slice(wall_side * half, (wall_side + 1) * half)
        values = dot3(split(sources), tuple(part[:, here] for part in spread), TN)
        total = []
        for index in range(2):
            strip_rows = [
                (place - wall_side) % strips * depth
                for place in range(index * groups, (index + 1) * groups)
            ]
            own_rows = jnp.concatenate([values[k : k + depth] for k in strip_rows], axis=0)
            total.append(jnp.sum(own_rows * along[:, here], axis=0, keepdims=True))
        sampled.append(total)
    stream, spanwise = [jnp.concatenate(both, axis=1) for both in zip(*sampled)]
    speed = jnp.sqrt(stream * stream + spanwise * spanwise + speed_floor)
    factor = drag * speed
    gradient = (factor * stream, factor * spanwise)
    neumann[0:1, :] = gradient[0]
    neumann[1:2, :] = gradient[1]

    planes = []
    for index in range(2):
        pull = viscosity * gradient[index]
        planes += [pull[:, :rows], pull[:, rows:]]
    tiles = 4 * length_x // 8
    tile_lane = lax.broadcasted_iota(jnp.int32, (8, 128), 1)
    tile_row = lax.broadcasted_iota(jnp.int32, (8, 128), 0)
    block_of = tile_lane // length_z
    bundle = jnp.zeros((8, 128), F32)
    fringe = jnp.zeros((8, 128), F32)
    for tile in range(tiles):
        part = planes[tile // 2][:, 128 * (tile % 2) : 128 * (tile % 2) + 128]
        part = jnp.broadcast_to(part, (8, 128))
        spread_rows = pltpu.roll(part, 0, 1, stride=length_z, stride_axis=0)
        spread_rows = pltpu.roll(spread_rows, (8 - tile) % 8, 0)
        bundle = jnp.where(block_of == tile, spread_rows, bundle)
        for end in range(2):
            turned = pltpu.roll(part, 7 * (1 - end), 1, stride=length_z - 1, stride_axis=0)
            wanted_lane = tile * length_z + 8 * end + 7 - tile_row
            fringe = jnp.where(tile_lane == wanted_lane, turned, fringe)
    pull_send[...] = bundle
    edge_send[0:1, :] = jnp.sum(fringe, axis=0, keepdims=True)
    edge_send[1:2, :] = jnp.where(block_of[0:1] % 2 == 0, bundle[0:1], bundle[1:2])
    if stepwise:
        pl.semaphore_wait(step_two, len(across_wall))
    reach = 2 * REACH + 1
    offsets = [
        (dx, dz)
        for dx in range(-REACH, REACH + 1)
        for dz in range(-REACH, REACH + 1)
        if (dx, dz) != (0, 0)
    ]
    nearby = [place for place in offsets if max(abs(place[0]), abs(place[1])) < REACH]
    remaining = [place for place in offsets if place not in nearby]
    pull_rows = {place: pl.ds(8 * index, 8) for index, place in enumerate(nearby)}
    for index, place in enumerate(remaining):
        pull_rows[place] = pl.ds(8 * len(nearby) + index, 1)
    for dx, dz in sorted(offsets, key=lambda pair: -abs(pair[0]) - abs(pair[1])):
        if (dx, dz) in nearby:
            source = pull_send
        else:
            source = edge_send.at[pl.ds(0 if abs(dz) == REACH else 1, 1), :]
        remote(
            source, pull_got.at[pull_rows[(-dx, -dz)], :], sent, pull_rs, at(dx, dz)
        ).start()

    add_faces(0)
    operate(1)
    loaded("along_x", "along_z", "weights")
    lines_rows = jnp.concatenate([lines_mass, lines_stiff], axis=1)
    ends = [lines_rows[0:1], lines_rows[length_y - 1 : length_y]]
    once = [(end[:, :length_y], end[:, length_y:]) for end in ends]
    twice = dot3(
        split(jnp.concatenate([once[0][0], once[0][1], once[1][0], once[1][1]] * 2, axis=0)),
        split(lines_rows),
        NN,
    )
    one_lane = lax.broadcasted_iota(jnp.int32, (1, length_y), 1)
    zero = jnp.zeros((1, length_y), F32)
    images = []
    for side in range(2):
        by_mass, by_stiff = twice[2 * side : 2 * side + 1], twice[2 * side + 1 : 2 * side + 2]
        moved_tip = jnp.where(one_lane == length_y // 2 - side, 1.0, 0.0)
        rows_of = [
            (zero, moved_tip),
            (zero, once[side][0]),
            (zero, once[side][1]),
            (by_mass[:, :length_y], zero),
            (by_stiff[:, :length_y], zero),
            (by_mass[:, length_y:], zero),
            (by_stiff[:, length_y:], zero),
        ]
        for entry in rows_of:
            image = jnp.concatenate(entry, axis=1)
            images.append(jnp.broadcast_to(image, (length_z, 2 * length_y)))
        images.append(jnp.zeros((128 - 7 * length_z, 2 * length_y), F32))
    images = split(jnp.concatenate(images, axis=0))
    low_half = tile_lane & 8 == 0
    low_rows = tile_row & 1 == 0
    diagonal_of = (tile_lane + tile_row) & 7
    settle(pull_rs, pull_got)

    def edge(dx, dz):
        return jnp.broadcast_to(pull_got[pull_rows[(dx, dz)], :], (8, 128))

    def both_ends(dx):
        return jnp.where(low_half, edge(dx, REACH), edge(dx, -REACH))

    middle = range(-REACH + 1, REACH)
    spans = []
    for dx in middle:
        ends = both_ends(dx)
        parts_z = [bundle if (dx, dz) == (0, 0) else pull_got[pull_rows[(dx, dz)], :] for dz in middle]
        for tile in range(tiles):
            pieces = [jnp.where(block_of == tile, part, 0.0) for part in parts_z]
            kept = jnp.logical_and(block_of == tile, diagonal_of == (7 - tile) % 8)
            pieces.append(jnp.where(kept, ends, 0.0))
            spans.append(jnp.concatenate(pieces, axis=1))
    pieces = [
        jnp.where(block_of == tile_row, jnp.where(low_rows, edge(REACH, dz), edge(-REACH, dz)), 0.0)
        for dz in middle
    ]
    kept = jnp.logical_and(
        block_of == tile_row, (tile_lane + tile_row + (tile_row & 1)) & 7 == 7
    )
    ends = jnp.where(low_rows, both_ends(REACH), both_ends(-REACH))
    pieces.append(jnp.where(kept, ends, 0.0))
    spans.append(jnp.concatenate(pieces, axis=1))
    spans.append(jnp.zeros((8, 512), F32))
    spans_hi, spans_lo = split(jnp.concatenate(spans, axis=0))
    reached = jnp.dot(spans_hi, along_z[...], preferred_element_type=F32)
    reached = (reached[:, :128] + reached[:, 128:]) + jnp.dot(
        spans_lo, along_z[:, :128], preferred_element_type=F32
    )
    by_plane = []
    for plane in range(4):
        kept = [
            reached[ix * 64 + plane * length_x : ix * 64 + (plane + 1) * length_x]
            for ix in range(len(middle))
        ]
        last = reached[64 * len(middle) : 64 * len(middle) + 8]
        kept.append(jnp.where(tile_row // 2 == plane, last, 0.0))
        kept.append(jnp.zeros((8, 128), F32))
        by_plane.append(jnp.concatenate(kept, axis=0))
    stacked_hi, stacked_lo = split(jnp.concatenate(by_plane, axis=1))
    both_ways = jnp.dot(
        along_x[...],
        jnp.concatenate([stacked_hi, stacked_lo, stacked_hi], axis=0),
        preferred_element_type=F32,
    )
    block_lane = lax.broadcasted_iota(jnp.int32, (length_x, 128), 1) // length_z
    keep_row = lax.rem(lax.broadcasted_iota(jnp.int32, (rows, 256), 0), length_z)
    keep_lane = lax.rem(lax.broadcasted_iota(jnp.int32, (rows, 256), 1), length_z)
    wall_lane = lax.broadcasted_iota(jnp.int32, (rows, length_y), 1)
    tractions = []
    for index in range(2):
        blocks = []
        for side in range(2):
            plane = index * 2 + side
            total = jnp.zeros((length_x, 128), F32)
            for block, word_x, word_z in TERMS:
                piece = both_ways[
                    word_x * length_x : (word_x + 1) * length_x, plane * 128 : plane * 128 + 128
                ]
                shift = ((block - word_z) * length_z) % 128
                moved = pltpu.roll(piece, shift, 1) if shift else piece
                total = total + jnp.where(block_lane == block, moved, 0.0)
            blocks.append(total)
        wide = jnp.concatenate(blocks, axis=1)
        tall = jnp.concatenate(
            [jnp.broadcast_to(wide[x : x + 1], (length_z, 256)) for x in range(length_x)], axis=0
        )
        tall = jnp.where(keep_row == keep_lane, tall, 0.0)
        deep = dot3(split(tall), images, NN)
        level_two, shallow = deep[:, :length_y], deep[:, length_y:]
        tip = jnp.logical_or(wall_lane == 0, wall_lane == length_y - 1)
        level_zero = jnp.where(tip, pltpu.roll(shallow, length_y // 2, 1), 0.0)
        outside = jnp.logical_or(wall_lane < length_y // 4, wall_lane >= 3 * length_y // 4)
        level_one = jnp.where(outside, shallow, 0.0)
        tractions.append((level_zero, level_one, level_two))
    t1, t2 = shifts
    for c in range(3):
        chain = [field[level, c] for level in range(3)]
        if c != 1:
            taus = tractions[c // 2]
            chain = [chain[level] + taus[level] for level in range(3)]
        v1 = chain[1] - t1 * chain[0]
        field[0, c] = chain[0]
        field[1, c] = v1
        field[2, c] = chain[2] - t1 * chain[1] - t2 * v1
    for newest in range(2):
        inner_products(newest)
    add_faces(1)
    highs = [field[2, c].astype(BF16) for c in range(3)]
    along_y = jnp.dot(
        jnp.concatenate(highs, axis=0), lines_packed[:length_y], preferred_element_type=F32
    )
    wide = jnp.concatenate(highs, axis=1)
    across = jnp.dot(sheet[0, :rows], wide, preferred_element_type=F32)
    across_low = jnp.dot(sheet[1, :rows], wide, preferred_element_type=F32)
    inner_products(2)
    for c in range(3):
        here = slice(c * length_y, (c + 1) * length_y)
        tall = along_y[c * rows : (c + 1) * rows]
        tall = tall[:, :length_y] + tall[:, length_y:]
        image = (across[:, here] + across_low[:, here]) * mass_row + tall * column(1)
        value = field[2, c]
        partner = value + (value - highs[c].astype(F32))
        inner(6, c, partner * column(3) * image)

    total_rows = parts.shape[0]
    r_iota = lax.broadcasted_iota(jnp.int32, (total_rows, 128), 0)
    l_iota = lax.broadcasted_iota(jnp.int32, (total_rows, 128), 1)
    diagonal = r_iota == l_iota
    end_lane = lax.broadcasted_iota(jnp.int32, (total_rows, 128), 1)
    shared = jnp.logical_or(end_lane % 8 == 0, end_lane % 8 == 7)
    tips = jnp.logical_or(end_lane == 0, end_lane == length_y - 1)
    weight_y = jnp.where(jnp.logical_and(shared, jnp.logical_not(tips)), 0.5, 1.0)
    summed = jnp.sum(parts[...] * weight_y, axis=1, keepdims=True)
    row = jnp.sum(jnp.where(diagonal, summed, 0.0), axis=0, keepdims=True)

    def gather_sum(stage, row, count, got, rs, place):
        sum_send[stage : stage + 1, :] = row
        for k in range(1, count):
            remote(
                sum_send.at[pl.ds(stage, 1), :], got.at[pl.ds(k - 1, 1), :], sent, rs, place(k)
            ).start()
        settle(rs, got)
        return row + jnp.sum(got[...], axis=0, keepdims=True)

    sum_rows = 0
    if single:
        every = n_wall * n_span
        row = gather_sum(0, row, every, wall_got, wall_rs, lambda k: at(k // n_span, k % n_span))
        sum_rows = every - 1
    else:
        row = gather_sum(0, row, n_wall, wall_got, wall_rs, lambda k: at(k, 0))
        row = gather_sum(1, row, n_span, span_got, span_rs[0], lambda k: at(0, k))
        sum_rows = n_wall + n_span - 2
    sent_rows = 2 * 2 * 64 + pull_got.shape[0] + ROUNDS * face_total + sum_rows
    settle(sent, everything.at[pl.ds(0, sent_rows), :])
    totals = jnp.sum(jnp.where(diagonal, row, 0.0), axis=1, keepdims=True)
    m00, m01, m11, m02, m12, m22, e22 = [totals[q * 8 : q * 8 + 8, :] for q in range(7)]
    t1, t2 = shifts
    a00 = m01 + t1 * m00
    a01 = m11 + t1 * m01
    a02 = m12 + t1 * m02
    a11 = m12 + t2 * m11
    a12 = m22 + t2 * m12
    l10 = a01 / a00
    l20 = a02 / a00
    d1 = a11 - l10 * a01
    u12 = a12 - l10 * a02
    l21 = u12 / d1
    d2 = e22 - l20 * a02 - l21 * u12
    y1 = m01 - l10 * m00
    y2 = m02 - l20 * m00 - l21 * y1
    x2 = y2 / d2
    x1 = y1 / d1 - l21 * x2
    x0 = m00 / a00 - l10 * x1 - l20 * x2
    for index, value in enumerate((x0, x1, x2)):
        factors[index] = jnp.broadcast_to(value, (8, 128))


def combine(field, factors, neumann_in, out, neumann, stage, sems):
    small = pltpu.make_async_copy(neumann_in, neumann, sems.at[3])
    small.start()
    copies = []
    for c in range(3):
        result = factors[0, c : c + 1] * field[0, c]
        for level in range(1, 3):
            result += factors[level, c : c + 1] * field[level, c]
        stage[c] = result.reshape(stage.shape[1:])
        copy = pltpu.make_async_copy(stage.at[c], out.at[c], sems.at[c])
        copy.start()
        copies.append(copy)
    for copy in copies:
        copy.wait()
    small.wait()


def body(n_wall, n_span, velocity_old, heights, owner_device, owner_element, ref_coords, roughness):
    sizes = velocity_old.shape[1:]
    length_x, length_z, length_y = sizes
    rows = length_x * length_z
    points = owner_device.shape[0]
    plane, lines, columns, along_x, along_z = tables(*sizes)
    along_x_hi, along_x_lo = split_np(along_x)
    every = n_wall * n_span
    first = every if every <= SINGLE_STAGE else n_wall
    faces = -(-(6 * (length_x + length_z) + 12) // 8) * 8
    vmem = pl.BlockSpec(memory_space=pltpu.VMEM)
    hbm = pl.BlockSpec(memory_space=pltpu.HBM)
    operands = (
        velocity_old,
        heights.reshape(1, -1),
        owner_device.reshape(1, -1),
        owner_element.reshape(1, -1),
        ref_coords,
        roughness.reshape(1, -1),
        jnp.stack(split_np(plane)),
        jnp.asarray(lines, F32),
        jnp.asarray(columns, F32),
        jnp.concatenate([along_x_hi, along_x_hi, along_x_lo], axis=1),
        jnp.concatenate(split_np(along_z), axis=1),
    )
    dma = pltpu.SemaphoreType.DMA
    field, factors, neumann = pl.pallas_call(
        functools.partial(kernel, n_wall, n_span, sizes),
        out_shape=(
            pltpu.VMEM((3, 3, rows, length_y), F32),
            pltpu.VMEM((3, 8, 128), F32),
            pltpu.VMEM((2, points), F32),
        ),
        in_specs=[hbm] * 11,
        out_specs=(vmem, vmem, vmem),
        scratch_shapes=[pltpu.VMEM(value.shape, value.dtype) for value in operands]
        + [
            dma((12,)),
            pltpu.VMEM((2, 64, length_y), F32),
            pltpu.VMEM((2, 2, 64, length_y), F32),
            pltpu.VMEM((ROUNDS, faces, length_y), F32),
            pltpu.VMEM((ROUNDS, faces, length_y), F32),
            pltpu.VMEM((56, length_y), F32),
            pltpu.VMEM((2, 128), F32),
            pltpu.VMEM((first - 1, 128), F32),
            pltpu.VMEM((n_span - 1, 128), F32),
            pltpu.VMEM((8, 128), F32),
            pltpu.VMEM((8, 128), F32),
            pltpu.VMEM((80, 128), F32),
            pltpu.VMEM((896, length_y), F32),
            dma,
            dma((2,)),
            dma,
            dma((ROUNDS,)),
            dma,
            pltpu.SemaphoreType.REGULAR,
            pltpu.SemaphoreType.REGULAR,
        ]
        + ([] if every <= SINGLE_STAGE else [dma]),
        compiler_params=pltpu.CompilerParams(
            collective_id=0, has_side_effects=True, vmem_limit_bytes=VMEM_LIMIT
        ),
    )(*[pltpu.with_memory_space_constraint(value, pltpu.HBM) for value in operands])
    return pl.pallas_call(
        combine,
        out_shape=(
            jax.ShapeDtypeStruct(velocity_old.shape, F32),
            jax.ShapeDtypeStruct((2, points), F32),
        ),
        in_specs=[vmem] * 3,
        out_specs=(hbm, hbm),
        scratch_shapes=[pltpu.VMEM(velocity_old.shape, F32), dma((4,))],
        compiler_params=pltpu.CompilerParams(vmem_limit_bytes=VMEM_LIMIT),
    )(field, factors, neumann)


def solution(mesh):
    placed = (
        P(None, "wall", "span", None),
        P(),
        P(("wall", "span"), None),
        P(("wall", "span"), None),
        P(None, ("wall", "span")),
        P(("wall", "span")),
    )
    return jax.shard_map(
        functools.partial(body, mesh.shape["wall"], mesh.shape["span"]),
        mesh=mesh,
        in_specs=placed,
        out_specs=(P(None, "wall", "span", None), P(None, ("wall", "span"))),
        check_vma=False,
    )
```

```python
import functools

import jax
import jax.numpy as jnp
import numpy as np
from jax import lax
from jax.experimental import pallas as pl
from jax.experimental.pallas import tpu as pltpu
from jax.sharding import PartitionSpec as P

GLL_NODES = (
    -1.0,
    -0.8717401485096066,
    -0.5917001814331423,
    -0.2092992179024789,
    0.2092992179024789,
    0.5917001814331423,
    0.8717401485096066,
    1.0,
)
GLL_WEIGHTS = (
    0.03571428571428571,
    0.2107042271435061,
    0.3411226924835044,
    0.4124587946587038,
    0.4124587946587038,
    0.3411226924835044,
    0.2107042271435061,
    0.03571428571428571,
)
viscosity = 0.02
inverse_step = 20.0
karman = 0.41
sample_height = 0.1
speed_floor = 0.01
element_dx = 0.05
element_dz = 0.13
NEAR = 2
ROUNDS = 2
REACH = 2
TERMS = (
    (0, 0, 0),
    (1, 1, 2),
    (1, 2, 1),
    (2, 2, 2),
    (3, 3, 6),
    (3, 4, 5),
    (3, 5, 4),
    (3, 6, 3),
    (4, 4, 6),
    (4, 6, 4),
    (5, 5, 6),
    (5, 6, 5),
    (6, 6, 6),
)
SINGLE_STAGE = 64
VMEM_LIMIT = 32 * 2**20
MESH = pl.DeviceIdType.MESH
F32 = jnp.float32
BF16 = jnp.bfloat16


def stiffness_table():
    points = np.array(GLL_NODES)
    weights = np.array(GLL_WEIGHTS)
    previous = np.ones(8)
    current = points.copy()
    for degree in range(1, 7):
        previous, current = (
            current,
            ((2 * degree + 1) * points * current - degree * previous) / (degree + 1),
        )
    derivative = np.zeros((8, 8))
    for target in range(8):
        for source in range(8):
            if target != source:
                derivative[target, source] = (
                    current[target] / current[source] / (points[target] - points[source])
                )
    derivative[0, 0] = -14.0
    derivative[7, 7] = 14.0
    return derivative.T @ (weights[:, None] * derivative)


def join_matrix(length):
    joined = np.eye(length)
    for left in range(7, length - 1, 8):
        joined[left, left + 1] = 1.0
        joined[left + 1, left] = 1.0
    return joined


def face_weights(length, open_ends):
    values = np.ones(length)
    position = np.arange(length) % 8
    values[(position == 0) | (position == 7)] = 0.5
    if open_ends:
        values[0] = 1.0
        values[-1] = 1.0
    return values


def split_np(matrix):
    single = jnp.asarray(matrix, F32)
    high = single.astype(BF16)
    low = (jnp.asarray(matrix, F32) - high.astype(F32)).astype(BF16)
    return high, low


def tables(length_x, length_z, length_y):
    weights = np.array(GLL_WEIGHTS)
    stiffness = stiffness_table()
    count_x, count_z, count_y = length_x // 8, length_z // 8, length_y // 8
    mass_x = np.tile(0.5 * element_dx * weights, count_x)
    mass_z = np.tile(0.5 * element_dz * weights, count_z)
    stiff_x = np.kron(np.eye(count_x), stiffness * (2.0 / element_dx))
    stiff_z = np.kron(np.eye(count_z), stiffness * (2.0 / element_dz))
    mass_xz = np.kron(mass_x, mass_z)
    join_xz = np.kron(join_matrix(length_x), join_matrix(length_z))
    join_y = join_matrix(length_y)
    plane = viscosity * (
        np.kron(stiff_x, np.diag(mass_z)) + np.kron(np.diag(mass_x), stiff_z)
    ) + inverse_step * np.diag(mass_xz)
    plane = join_xz @ plane
    mass_plane = join_xz @ mass_xz
    lines_mass = np.tile(0.5 * weights, count_y)[:, None] * join_y
    lines_stiff = viscosity * 2.0 * (np.kron(np.eye(count_y), stiffness) @ join_y)
    lines = np.stack([lines_mass, lines_stiff])
    ring_x = join_matrix(length_x) @ mass_x
    ring_z = join_matrix(length_z) @ mass_z
    ring_x[0] *= 2.0
    ring_x[-1] *= 2.0
    ring_z[0] *= 2.0
    ring_z[-1] *= 2.0
    assembled = inverse_step * np.kron(ring_x, ring_z)
    inner_x = face_weights(length_x, True)
    inner_z = face_weights(length_z, True)
    outer_x = face_weights(length_x, False)
    outer_z = face_weights(length_z, False)
    steps_x, steps_z = np.arange(length_x), np.arange(length_z)
    fringe = np.concatenate(
        [
            steps_x * length_z + length_z - 1,
            steps_x * length_z,
            (length_x - 1) * length_z + steps_z,
            steps_z,
        ]
    )
    outer, inner = np.kron(outer_x, outer_z), np.kron(inner_x, inner_z)
    columns = np.concatenate([assembled, mass_plane, mass_plane[fringe], outer, inner])
    columns = columns.reshape(-1, 1) * np.ones(length_y)[None]
    plane = np.concatenate([plane, plane[fringe]], axis=0)
    reach = 2 * REACH + 1

    def words(length, mass, stiff, extra):
        size = reach * length
        join = join_matrix(size)
        light = join @ np.diag(np.tile(mass, reach))
        heavy = viscosity * join @ np.kron(np.eye(size // 8), stiff) + extra * light
        chains = [
            light,
            heavy @ light,
            light @ light,
            heavy @ heavy @ light,
            heavy @ light @ light,
            light @ heavy @ light,
            light @ light @ light,
        ]
        middle = REACH * length
        chains = [chain[middle : middle + length] for chain in chains]
        return np.concatenate(chains + [np.zeros((128 - 7 * length, size))], axis=0)

    words_x = words(length_x, mass_x, stiffness * (2.0 / element_dx), 0.0)
    words_z = words(length_z, mass_z, stiffness * (2.0 / element_dz), inverse_step)
    full = range(REACH - 1, REACH + 2)
    turned = words_z.T
    ends_z = [2 * REACH * length_z] * 8 + [length_z - 1] * 8
    along_z = np.concatenate(
        [np.tile(turned[iz * length_z : (iz + 1) * length_z], (8, 1)) for iz in full]
        + [np.tile(turned[ends_z], (8, 1))],
        axis=0,
    )
    ends = [2 * REACH * length_x, length_x - 1] * 4
    inner = [ix * length_x + half + (-r) % 8 for ix in full for half in (0, 8) for r in range(8)]
    along_x = np.concatenate(
        [words_x[:, inner], words_x[:, ends]]
        + [np.zeros((128, 8))],
        axis=1,
    )
    return plane, lines, columns, along_x, along_z


def split(value):
    high = value.astype(BF16)
    low = (value - high.astype(F32)).astype(BF16)
    return high, low


def dot3(left, right, dims):
    def one(a, b):
        return lax.dot_general(a, b, (dims, ((), ())), preferred_element_type=F32)

    return one(left[0], right[0]) + (one(left[0], right[1]) + one(left[1], right[0]))


NN = ((1,), (0,))
NT = ((1,), (1,))
TN = ((0,), (0,))
DIRS = ((1, 1), (1, -1), (-1, 1), (-1, -1))


def lagrange_rows(coord):
    points = np.array(GLL_NODES)
    scale = 1.0 / np.prod(points[:, None] - points[None, :] + np.eye(8), axis=1)
    shape = (8, coord.shape[1])
    node = lax.broadcasted_iota(jnp.int32, shape, 0)
    total = jnp.zeros(shape, F32)
    for a in range(8):
        total = jnp.where(node == a, F32(scale[a]), total)
    for b in range(8):
        total = total * jnp.where(node == b, F32(1.0), coord - F32(points[b]))
    return total


def kernel(
    n_wall,
    n_span,
    sizes,
    vel_in,
    heights_in,
    owner_in,
    element_in,
    coords_in,
    roughness_in,
    plane_in,
    lines_in,
    columns_in,
    along_x_in,
    along_z_in,
    field,
    factors,
    neumann,
    vel,
    heights,
    owner,
    element,
    coords,
    roughness,
    sheet,
    lines,
    columns,
    along_x,
    along_z,
    load_sem,
    near,
    near_got,
    face_send,
    face_got,
    parts,
    sum_send,
    wall_got,
    span_got,
    pull_send,
    edge_send,
    pull_got,
    everything,
    sent,
    near_rs,
    pull_rs,
    face_rs,
    wall_rs,
    step_one,
    step_two,
    *span_rs,
):
    length_x, length_z, length_y = sizes
    rows = length_x * length_z
    count_z, count_y = length_z // 8, length_y // 8
    w = lax.axis_index("wall")
    s = lax.axis_index("span")

    def turned(place, count):
        return place & (count - 1) if count & (count - 1) == 0 else lax.rem(place, count)

    def at(dx, dz):
        return (turned(w + (dx + n_wall), n_wall), turned(s + (dz + n_span), n_span))

    edges = 2 * (length_x + length_z)
    early, late = pl.ds(0, 2 * rows + edges), pl.ds(2 * rows + edges, 2 * rows)

    def column(index):
        first = index * rows + (edges if index > 1 else 0)
        return columns[first : first + rows, :]

    loads = {
        name: pltpu.make_async_copy(source, target, load_sem.at[index])
        for index, (name, source, target) in enumerate(
            (
                ("vel", vel_in, vel),
                ("heights", heights_in, heights),
                ("lines", lines_in, lines),
                ("scale", columns_in.at[early], columns.at[early]),
                ("plane", plane_in, sheet),
                ("coords", coords_in, coords),
                ("owner", owner_in, owner),
                ("element", element_in, element),
                ("roughness", roughness_in, roughness),
                ("along_x", along_x_in, along_x),
                ("along_z", along_z_in, along_z),
                ("weights", columns_in.at[late], columns.at[late]),
            )
        )
    }
    for load in loads.values():
        load.start()

    def loaded(*names):
        for name in names:
            loads[name].wait()

    single = n_wall * n_span <= SINGLE_STAGE
    stepwise = single and 3 <= n_wall <= 4 * REACH and 3 <= n_span <= 4 * REACH
    across_wall = ((1, 0), (-1, 0))
    if stepwise:
        greeted = across_wall + tuple((0, k) for k in range(1, n_span))
    elif single:
        greeted = [divmod(k, n_span) for k in range(1, n_wall * n_span)]
    else:
        greeted = [(k, 0) for k in range(1, n_wall)] + [(0, k) for k in range(1, n_span)]
        greeted += sorted(
            {
                ((dx + n_wall) % n_wall, (dz + n_span) % n_span)
                for dx in range(-REACH, REACH + 1)
                for dz in range(-REACH, REACH + 1)
            }
            - {(0, 0)}
            - set(greeted)
        )
    barrier = pltpu.get_barrier_semaphore()

    def greet(semaphore, places):
        for dx, dz in places:
            pl.semaphore_signal(semaphore, inc=1, device_id=at(dx, dz), device_id_type=MESH)

    greet(barrier, greeted)

    loaded("vel")
    lane = lax.broadcasted_iota(jnp.int32, (64, length_y), 1)
    groups = (length_x // 8) * count_z
    depth = 8 * NEAR
    strips = length_y // depth
    packed = [jnp.zeros((64, length_y), F32)] * 2
    for index, comp in enumerate((0, 2)):
        for group in range(groups):
            ex, ez = group // count_z, group % count_z
            block = vel[comp, pl.ds(ex * 8, 8), pl.ds(ez * 8, 8), :].reshape(64, length_y)
            place = index * groups + group
            moved = pltpu.roll(block, place * depth, 1) if place else block
            for wall_side in range(2):
                strip = (place - wall_side) % strips
                packed[wall_side] = jnp.where(lane // depth == strip, moved, packed[wall_side])
    for wall_side in range(2):
        near[wall_side] = packed[wall_side]
    def remote(src, dst, ss, rs, where):
        return pltpu.make_async_remote_copy(
            src_ref=src,
            dst_ref=dst,
            send_sem=ss,
            recv_sem=rs,
            device_id=where,
            device_id_type=MESH,
        )

    near_copies = []
    for wall_side in range(2):
        for slot, dx in enumerate((1, -1)):
            target = near_got.at[wall_side, slot]
            near_copies.append(
                remote(near.at[wall_side], target, sent, near_rs.at[wall_side], at(dx, 0))
            )

    def enter():
        pl.semaphore_wait(barrier, len(greeted))
        if stepwise:
            greet(step_one, across_wall)
        for copy in near_copies:
            copy.start()

    if stepwise:
        enter()
    loaded("heights", "lines", "scale", "plane")

    layer_of = lax.broadcasted_iota(jnp.int32, (length_y, count_y), 0) // 8
    layer = lax.broadcasted_iota(jnp.int32, (length_y, count_y), 1)
    height_row = heights[...]
    height = jnp.sum(jnp.where(layer_of == layer, height_row, 0.0), axis=1, keepdims=True)
    lines_mass = height * lines[0]
    lines_stiff = lines[1] / height
    stiff_hi, stiff_lo = split(lines_stiff)
    lines_packed = jnp.concatenate(
        [
            jnp.concatenate([stiff_hi, stiff_lo], axis=1),
            jnp.concatenate([stiff_hi, jnp.zeros_like(stiff_lo)], axis=1),
        ],
        axis=0,
    )
    bound = jnp.max(0.1535 * height_row + 0.000182 / height_row, axis=1, keepdims=True)
    shifts = (0.15 * bound, 0.85 * bound)

    mass_row = jnp.sum(lines_mass, axis=0, keepdims=True)
    scale = column(0) * mass_row
    for c in range(3):
        field[0, c] = vel[c].reshape(rows, length_y) * scale

    face_rows = []
    for slot, (dx, dz) in enumerate(DIRS + ((0, 1), (0, -1), (1, 0), (-1, 0))):
        size = 3 * (1 if dx and dz else length_z if dx else length_x)
        face_rows.append((sum(entry[1] for entry in face_rows), size, dx, dz))
    face_total = sum(entry[1] for entry in face_rows)
    z_first = {entry[3]: entry[0] for entry in face_rows if entry[2] == 0}

    def corner(dx, dz):
        return (rows - length_z if dx == 1 else 0) + (length_z - 1 if dz == 1 else 0)

    def face_part(slot, c, dx, dz):
        first, size = face_rows[slot][0] + c * (face_rows[slot][1] // 3), face_rows[slot][1] // 3
        if dx and dz:
            rows_of = pl.ds(corner(dx, dz), 1)
        elif dx:
            rows_of = pl.ds(rows - length_z if dx == 1 else 0, length_z)
        else:
            rows_of = pl.ds(length_z - 1 if dz == 1 else 0, length_x, stride=length_z)
        return pl.ds(first, size), rows_of

    def send_faces(turn, fringe):
        for c in range(3):
            for slot, (first, size, dx, dz) in enumerate(face_rows):
                size //= 3
                if dx and dz:
                    begin = 2 * length_x + (length_z if dx == -1 else 0)
                    begin += length_z - 1 if dz == 1 else 0
                elif dx:
                    begin = 2 * length_x + (length_z if dx == -1 else 0)
                else:
                    begin = length_x if dz == -1 else 0
                rows_here = slice(first + c * size, first + (c + 1) * size)
                face_send[turn, rows_here, :] = fringe[c][begin : begin + size]
        first_turn = turn == 0 and stepwise
        if turn == 0 and not stepwise:
            enter()
        for stage in ((0,), (2, 1)) if first_turn else ((2, 0, 1),):
            if stage[0] == 2 and first_turn:
                pl.semaphore_wait(step_one, len(across_wall))
                greet(step_two, across_wall)
            for kind in stage:
                for first, size, dx, dz in face_rows:
                    if (2 if dx and dz else abs(dx)) != kind:
                        continue
                    if kind == 0:
                        swap = jnp.where(s == 0, -dz, dz)
                        first = pl.multiple_of(jnp.where(swap == 1, z_first[1], z_first[-1]), 4)
                        dz = swap
                    part = (turn, pl.ds(first, size), slice(None))
                    remote(
                        face_send.at[part],
                        face_got.at[part],
                        sent,
                        face_rs.at[turn],
                        at(dx, dz),
                    ).start()

    def settle(semaphore, ref):
        pltpu.make_async_copy(ref, ref, semaphore).wait()

    def add_faces(turn):
        settle(face_rs.at[turn], face_got.at[turn, pl.ds(0, face_total), :])
        for c in range(3):
            for slot, (_, _, dx, dz) in enumerate(face_rows):
                packed_rows, rows_of = face_part(slot, c, -dx, -dz)
                field[turn + 1, c, rows_of, :] = (
                    field[turn + 1, c, rows_of, :] + face_got[turn, packed_rows, :]
                )

    def inner(quantity, c, product):
        parts[quantity * 8 + c : quantity * 8 + c + 1, :] = jnp.sum(
            product, axis=0, keepdims=True
        )

    def operate(turn):
        highs, lows = zip(*[split(field[turn, c]) for c in range(3)])
        packed = [jnp.concatenate(pair, axis=1) for pair in zip(highs, lows)]
        wide = jnp.concatenate(highs + lows, axis=1)
        wide_high = jnp.concatenate(highs, axis=1)

        def image(first, count, lines_of, weight):
            along_y = jnp.dot(
                jnp.concatenate(lines_of, axis=0), lines_packed, preferred_element_type=F32
            )
            part = slice(first, first + count)
            across = jnp.dot(sheet[0, part], wide, preferred_element_type=F32)
            across_low = jnp.dot(sheet[1, part], wide_high, preferred_element_type=F32)
            results = []
            for c in range(3):
                here = slice(c * length_y, (c + 1) * length_y)
                also = slice((3 + c) * length_y, (4 + c) * length_y)
                flat = across[:, here] + (across[:, also] + across_low[:, here])
                tall = along_y[c * count : (c + 1) * count]
                tall = tall[:, :length_y] + tall[:, length_y:]
                results.append(flat * mass_row + tall * weight)
            return results

        lines_of = []
        for c in range(3):
            value = jnp.concatenate(
                [
                    field[turn, c, pl.ds(length_z - 1, length_x, stride=length_z), :],
                    field[turn, c, pl.ds(0, length_x, stride=length_z), :],
                    field[turn, c, pl.ds(rows - length_z, length_z), :],
                    field[turn, c, pl.ds(0, length_z), :],
                ],
                axis=0,
            )
            lines_of.append(jnp.concatenate(split(value), axis=1))
        weight = columns[2 * rows : 2 * rows + edges, :]
        send_faces(turn, image(rows, edges, lines_of, weight))
        for c, value in enumerate(image(0, rows, packed, column(1))):
            field[turn + 1, c] = value

    slots = {(0, 0): 0, (0, 1): 1, (1, 1): 2, (0, 2): 3, (1, 2): 4, (2, 2): 5}

    def inner_products(newest):
        for c in range(3):
            weighted = field[newest, c] * column(2)
            for other in range(newest + 1):
                inner(slots[(other, newest)], c, weighted * field[other, c])

    operate(0)
    parts[...] = jnp.zeros_like(parts)

    loaded("coords", "owner", "element", "roughness")
    points = owner.shape[1]
    row_x = lagrange_rows(coords[0:1, :])
    row_z = lagrange_rows(coords[1:2, :])
    row_y = lagrange_rows(coords[2:3, :])
    cross = jnp.concatenate([row_x[a : a + 1] * row_z for a in range(8)], axis=0)
    distance = lax.rem(owner[...] - w + n_wall, n_wall)
    from_next = distance == 1
    from_prev = distance == n_wall - 1
    own = jnp.logical_not(jnp.logical_or(from_next, from_prev))
    spread = jnp.concatenate(
        [jnp.where(mask, cross, 0.0) for mask in (own, from_prev, from_next)], axis=0
    )
    half = points // 2
    n_row = lax.broadcasted_iota(jnp.int32, (groups * depth, points), 0)
    side_of = lax.broadcasted_iota(jnp.int32, (groups * depth, points), 1) // half
    layer_y = (n_row % depth) // 8 + side_of * (count_y - NEAR)
    wanted = (n_row // depth) * count_y + layer_y == element[...]
    along = jnp.where(wanted, jnp.concatenate([row_y] * (groups * NEAR), axis=0), 0.0)
    spread = split(spread)
    drag = karman / jnp.log(sample_height / roughness[...])
    drag = drag * drag * (-1.0 / viscosity)

    sampled = []
    for wall_side in range(2):
        settle(near_rs.at[wall_side], near_got.at[wall_side])
        sources = jnp.concatenate(
            [near[wall_side], near_got[wall_side, 0], near_got[wall_side, 1]], axis=0
        )
        here = slice(wall_side * half, (wall_side + 1) * half)
        values = dot3(split(sources), tuple(part[:, here] for part in spread), TN)
        total = []
        for index in range(2):
            strip_rows = [
                (place - wall_side) % strips * depth
                for place in range(index * groups, (index + 1) * groups)
            ]
            own_rows = jnp.concatenate([values[k : k + depth] for k in strip_rows], axis=0)
            total.append(jnp.sum(own_rows * along[:, here], axis=0, keepdims=True))
        sampled.append(total)
    stream, spanwise = [jnp.concatenate(both, axis=1) for both in zip(*sampled)]
    speed = jnp.sqrt(stream * stream + spanwise * spanwise + speed_floor)
    factor = drag * speed
    gradient = (factor * stream, factor * spanwise)
    neumann[0:1, :] = gradient[0]
    neumann[1:2, :] = gradient[1]

    planes = []
    for index in range(2):
        pull = viscosity * gradient[index]
        planes += [pull[:, :rows], pull[:, rows:]]
    tiles = 4 * length_x // 8
    tile_lane = lax.broadcasted_iota(jnp.int32, (8, 128), 1)
    tile_row = lax.broadcasted_iota(jnp.int32, (8, 128), 0)
    block_of = tile_lane // length_z
    bundle = jnp.zeros((8, 128), F32)
    fringe = jnp.zeros((8, 128), F32)
    for tile in range(tiles):
        part = planes[tile // 2][:, 128 * (tile % 2) : 128 * (tile % 2) + 128]
        part = jnp.broadcast_to(part, (8, 128))
        spread_rows = pltpu.roll(part, 0, 1, stride=length_z, stride_axis=0)
        spread_rows = pltpu.roll(spread_rows, (8 - tile) % 8, 0)
        bundle = jnp.where(block_of == tile, spread_rows, bundle)
        for end in range(2):
            slanted = pltpu.roll(part, 7 * (1 - end), 1, stride=length_z - 1, stride_axis=0)
            wanted_lane = tile * length_z + 8 * end + 7 - tile_row
            fringe = jnp.where(tile_lane == wanted_lane, slanted, fringe)
    pull_send[...] = bundle
    edge_send[0:1, :] = jnp.sum(fringe, axis=0, keepdims=True)
    edge_send[1:2, :] = jnp.where(block_of[0:1] % 2 == 0, bundle[0:1], bundle[1:2])
    if stepwise:
        pl.semaphore_wait(step_two, len(across_wall))
    reach = 2 * REACH + 1
    offsets = [
        (dx, dz)
        for dx in range(-REACH, REACH + 1)
        for dz in range(-REACH, REACH + 1)
        if (dx, dz) != (0, 0)
    ]
    nearby = [place for place in offsets if max(abs(place[0]), abs(place[1])) < REACH]
    remaining = [place for place in offsets if place not in nearby]
    pull_rows = {place: pl.ds(8 * index, 8) for index, place in enumerate(nearby)}
    for index, place in enumerate(remaining):
        pull_rows[place] = pl.ds(8 * len(nearby) + index, 1)
    for dx, dz in sorted(offsets, key=lambda pair: -abs(pair[0]) - abs(pair[1])):
        if (dx, dz) in nearby:
            source = pull_send
        else:
            source = edge_send.at[pl.ds(0 if abs(dz) == REACH else 1, 1), :]
        remote(
            source, pull_got.at[pull_rows[(-dx, -dz)], :], sent, pull_rs, at(dx, dz)
        ).start()

    add_faces(0)
    operate(1)
    loaded("along_x", "along_z", "weights")
    lines_rows = jnp.concatenate([lines_mass, lines_stiff], axis=1)
    ends = [lines_rows[0:1], lines_rows[length_y - 1 : length_y]]
    once = [(end[:, :length_y], end[:, length_y:]) for end in ends]
    twice = dot3(
        split(jnp.concatenate([once[0][0], once[0][1], once[1][0], once[1][1]] * 2, axis=0)),
        split(lines_rows),
        NN,
    )
    one_lane = lax.broadcasted_iota(jnp.int32, (1, length_y), 1)
    zero = jnp.zeros((1, length_y), F32)
    images = []
    for side in range(2):
        by_mass, by_stiff = twice[2 * side : 2 * side + 1], twice[2 * side + 1 : 2 * side + 2]
        moved_tip = jnp.where(one_lane == length_y // 2 - side, 1.0, 0.0)
        rows_of = [
            (zero, moved_tip),
            (zero, once[side][0]),
            (zero, once[side][1]),
            (by_mass[:, :length_y], zero),
            (by_stiff[:, :length_y], zero),
            (by_mass[:, length_y:], zero),
            (by_stiff[:, length_y:], zero),
        ]
        for entry in rows_of:
            image = jnp.concatenate(entry, axis=1)
            images.append(jnp.broadcast_to(image, (length_z, 2 * length_y)))
        images.append(jnp.zeros((128 - 7 * length_z, 2 * length_y), F32))
    images = split(jnp.concatenate(images, axis=0))
    low_half = tile_lane & 8 == 0
    low_rows = tile_row & 1 == 0
    diagonal_of = (tile_lane + tile_row) & 7

    def halves(value):
        return split(value)

    def both_tiles(pair, mask_of):
        masks = [jnp.where(mask_of(tile), 1.0, 0.0) for tile in (2 * pair, 2 * pair + 1)]
        return jnp.concatenate(masks, axis=0).astype(BF16)

    block_masks = [both_tiles(pair, lambda tile: block_of == tile) for pair in range(tiles // 2)]
    end_masks = [
        both_tiles(
            pair,
            lambda tile: jnp.logical_and(block_of == tile, diagonal_of == (7 - tile) % 8),
        )
        for pair in range(tiles // 2)
    ]
    settle(pull_rs, pull_got)

    def edge(dx, dz):
        return jnp.broadcast_to(pull_got[pull_rows[(dx, dz)], :], (8, 128))

    def both_ends(dx):
        return jnp.where(low_half, edge(dx, REACH), edge(dx, -REACH))

    middle = range(-REACH + 1, REACH)

    def doubled(part):
        return [jnp.concatenate([half, half], axis=0) for half in (part[0], part[1])]

    spans = ([], [])
    for dx in middle:
        parts_z = [bundle if (dx, dz) == (0, 0) else pull_got[pull_rows[(dx, dz)], :] for dz in middle]
        pairs = [doubled(halves(part)) for part in parts_z]
        ends = doubled(halves(both_ends(dx)))
        for pair in range(tiles // 2):
            for out, which in zip(spans, range(2)):
                pieces = [part[which] * block_masks[pair] for part in pairs]
                pieces.append(ends[which] * end_masks[pair])
                out.append(jnp.concatenate(pieces, axis=1))
    pieces = [
        jnp.where(block_of == tile_row, jnp.where(low_rows, edge(REACH, dz), edge(-REACH, dz)), 0.0)
        for dz in middle
    ]
    kept = jnp.logical_and(
        block_of == tile_row, (tile_lane + tile_row + (tile_row & 1)) & 7 == 7
    )
    ends = jnp.where(low_rows, both_ends(REACH), both_ends(-REACH))
    pieces.append(jnp.where(kept, ends, 0.0))
    last = jnp.concatenate([jnp.concatenate(pieces, axis=1), jnp.zeros((8, 512), F32)], axis=0)
    for out, half in zip(spans, split(last)):
        out.append(half)
    spans_hi, spans_lo = [jnp.concatenate(out, axis=0) for out in spans]
    reached = jnp.dot(spans_hi, along_z[...], preferred_element_type=F32)
    reached = (reached[:, :128] + reached[:, 128:]) + jnp.dot(
        spans_lo, along_z[:, :128], preferred_element_type=F32
    )
    by_plane = []
    for plane in range(4):
        kept = [
            reached[ix * 64 + plane * length_x : ix * 64 + (plane + 1) * length_x]
            for ix in range(len(middle))
        ]
        last = reached[64 * len(middle) : 64 * len(middle) + 8]
        kept.append(jnp.where(tile_row // 2 == plane, last, 0.0))
        kept.append(jnp.zeros((8, 128), F32))
        by_plane.append(jnp.concatenate(kept, axis=0))
    stacked_hi, stacked_lo = split(jnp.concatenate(by_plane, axis=1))
    both_ways = jnp.dot(
        along_x[...],
        jnp.concatenate([stacked_hi, stacked_lo, stacked_hi], axis=0),
        preferred_element_type=F32,
    )
    block_lane = lax.broadcasted_iota(jnp.int32, (length_x, 128), 1) // length_z
    keep_row = lax.rem(lax.broadcasted_iota(jnp.int32, (rows, 256), 0), length_z)
    keep_lane = lax.rem(lax.broadcasted_iota(jnp.int32, (rows, 256), 1), length_z)
    wall_lane = lax.broadcasted_iota(jnp.int32, (rows, length_y), 1)
    tractions = []
    for index in range(2):
        blocks = []
        for side in range(2):
            plane = index * 2 + side
            total = jnp.zeros((length_x, 128), F32)
            for block, word_x, word_z in TERMS:
                piece = both_ways[
                    word_x * length_x : (word_x + 1) * length_x, plane * 128 : plane * 128 + 128
                ]
                shift = ((block - word_z) * length_z) % 128
                moved = pltpu.roll(piece, shift, 1) if shift else piece
                total = total + jnp.where(block_lane == block, moved, 0.0)
            blocks.append(total)
        wide = jnp.concatenate(blocks, axis=1)
        tall = jnp.concatenate(
            [jnp.broadcast_to(wide[x : x + 1], (length_z, 256)) for x in range(length_x)], axis=0
        )
        tall = jnp.where(keep_row == keep_lane, tall, 0.0)
        deep = dot3(split(tall), images, NN)
        level_two, shallow = deep[:, :length_y], deep[:, length_y:]
        tip = jnp.logical_or(wall_lane == 0, wall_lane == length_y - 1)
        level_zero = jnp.where(tip, pltpu.roll(shallow, length_y // 2, 1), 0.0)
        outside = jnp.logical_or(wall_lane < length_y // 4, wall_lane >= 3 * length_y // 4)
        level_one = jnp.where(outside, shallow, 0.0)
        tractions.append((level_zero, level_one, level_two))
    t1, t2 = shifts
    for c in range(3):
        chain = [field[level, c] for level in range(3)]
        if c != 1:
            taus = tractions[c // 2]
            chain = [chain[level] + taus[level] for level in range(3)]
        v1 = chain[1] - t1 * chain[0]
        field[0, c] = chain[0]
        field[1, c] = v1
        field[2, c] = chain[2] - t1 * chain[1] - t2 * v1
    for newest in range(2):
        inner_products(newest)
    add_faces(1)
    highs = [field[2, c].astype(BF16) for c in range(3)]
    along_y = jnp.dot(
        jnp.concatenate(highs, axis=0), lines_packed[:length_y], preferred_element_type=F32
    )
    wide = jnp.concatenate(highs, axis=1)
    across = jnp.dot(sheet[0, :rows], wide, preferred_element_type=F32)
    across_low = jnp.dot(sheet[1, :rows], wide, preferred_element_type=F32)
    inner_products(2)
    for c in range(3):
        here = slice(c * length_y, (c + 1) * length_y)
        tall = along_y[c * rows : (c + 1) * rows]
        tall = tall[:, :length_y] + tall[:, length_y:]
        image = (across[:, here] + across_low[:, here]) * mass_row + tall * column(1)
        value = field[2, c]
        partner = value + (value - highs[c].astype(F32))
        inner(6, c, partner * column(3) * image)

    total_rows = parts.shape[0]
    r_iota = lax.broadcasted_iota(jnp.int32, (total_rows, 128), 0)
    l_iota = lax.broadcasted_iota(jnp.int32, (total_rows, 128), 1)
    diagonal = r_iota == l_iota
    end_lane = lax.broadcasted_iota(jnp.int32, (total_rows, 128), 1)
    shared = jnp.logical_or(end_lane % 8 == 0, end_lane % 8 == 7)
    tips = jnp.logical_or(end_lane == 0, end_lane == length_y - 1)
    weight_y = jnp.where(jnp.logical_and(shared, jnp.logical_not(tips)), 0.5, 1.0)
    summed = jnp.sum(parts[...] * weight_y, axis=1, keepdims=True)
    row = jnp.sum(jnp.where(diagonal, summed, 0.0), axis=0, keepdims=True)

    def gather_sum(stage, row, count, got, rs, place):
        sum_send[stage : stage + 1, :] = row
        def ring(place, size):
            return min(place % size, -place % size)

        def reach_of(k):
            if count != n_wall * n_span:
                return ring(k, count)
            return ring(k // n_span, n_wall) + ring(k % n_span, n_span)

        for k in sorted(range(1, count), key=reach_of, reverse=True):
            remote(
                sum_send.at[pl.ds(stage, 1), :], got.at[pl.ds(k - 1, 1), :], sent, rs, place(k)
            ).start()
        settle(rs, got)
        return row + jnp.sum(got[...], axis=0, keepdims=True)

    sum_rows = 0
    if single:
        every = n_wall * n_span
        row = gather_sum(0, row, every, wall_got, wall_rs, lambda k: at(k // n_span, k % n_span))
        sum_rows = every - 1
    else:
        row = gather_sum(0, row, n_wall, wall_got, wall_rs, lambda k: at(k, 0))
        row = gather_sum(1, row, n_span, span_got, span_rs[0], lambda k: at(0, k))
        sum_rows = n_wall + n_span - 2
    sent_rows = 2 * 2 * 64 + pull_got.shape[0] + ROUNDS * face_total + sum_rows
    settle(sent, everything.at[pl.ds(0, sent_rows), :])
    totals = jnp.sum(jnp.where(diagonal, row, 0.0), axis=1, keepdims=True)
    m00, m01, m11, m02, m12, m22, e22 = [totals[q * 8 : q * 8 + 8, :] for q in range(7)]
    t1, t2 = shifts
    a00 = m01 + t1 * m00
    a01 = m11 + t1 * m01
    a02 = m12 + t1 * m02
    a11 = m12 + t2 * m11
    a12 = m22 + t2 * m12
    l10 = a01 / a00
    l20 = a02 / a00
    d1 = a11 - l10 * a01
    u12 = a12 - l10 * a02
    l21 = u12 / d1
    d2 = e22 - l20 * a02 - l21 * u12
    y1 = m01 - l10 * m00
    y2 = m02 - l20 * m00 - l21 * y1
    x2 = y2 / d2
    x1 = y1 / d1 - l21 * x2
    x0 = m00 / a00 - l10 * x1 - l20 * x2
    for index, value in enumerate((x0, x1, x2)):
        factors[index] = jnp.broadcast_to(value, (8, 128))


def combine(field, factors, neumann_in, out, neumann, stage, sems):
    small = pltpu.make_async_copy(neumann_in, neumann, sems.at[3])
    small.start()
    copies = []
    for c in range(3):
        result = factors[0, c : c + 1] * field[0, c]
        for level in range(1, 3):
            result += factors[level, c : c + 1] * field[level, c]
        stage[c] = result.reshape(stage.shape[1:])
        copy = pltpu.make_async_copy(stage.at[c], out.at[c], sems.at[c])
        copy.start()
        copies.append(copy)
    for copy in copies:
        copy.wait()
    small.wait()


def body(n_wall, n_span, velocity_old, heights, owner_device, owner_element, ref_coords, roughness):
    sizes = velocity_old.shape[1:]
    length_x, length_z, length_y = sizes
    rows = length_x * length_z
    points = owner_device.shape[0]
    plane, lines, columns, along_x, along_z = tables(*sizes)
    along_x_hi, along_x_lo = split_np(along_x)
    every = n_wall * n_span
    first = every if every <= SINGLE_STAGE else n_wall
    faces = -(-(6 * (length_x + length_z) + 12) // 8) * 8
    vmem = pl.BlockSpec(memory_space=pltpu.VMEM)
    hbm = pl.BlockSpec(memory_space=pltpu.HBM)
    operands = (
        velocity_old,
        heights.reshape(1, -1),
        owner_device.reshape(1, -1),
        owner_element.reshape(1, -1),
        ref_coords,
        roughness.reshape(1, -1),
        jnp.stack(split_np(plane)),
        jnp.asarray(lines, F32),
        jnp.asarray(columns, F32),
        jnp.concatenate([along_x_hi, along_x_hi, along_x_lo], axis=1),
        jnp.concatenate(split_np(along_z), axis=1),
    )
    dma = pltpu.SemaphoreType.DMA
    field, factors, neumann = pl.pallas_call(
        functools.partial(kernel, n_wall, n_span, sizes),
        out_shape=(
            pltpu.VMEM((3, 3, rows, length_y), F32),
            pltpu.VMEM((3, 8, 128), F32),
            pltpu.VMEM((2, points), F32),
        ),
        in_specs=[hbm] * 11,
        out_specs=(vmem, vmem, vmem),
        scratch_shapes=[pltpu.VMEM(value.shape, value.dtype) for value in operands]
        + [
            dma((12,)),
            pltpu.VMEM((2, 64, length_y), F32),
            pltpu.VMEM((2, 2, 64, length_y), F32),
            pltpu.VMEM((ROUNDS, faces, length_y), F32),
            pltpu.VMEM((ROUNDS, faces, length_y), F32),
            pltpu.VMEM((56, length_y), F32),
            pltpu.VMEM((2, 128), F32),
            pltpu.VMEM((first - 1, 128), F32),
            pltpu.VMEM((n_span - 1, 128), F32),
            pltpu.VMEM((8, 128), F32),
            pltpu.VMEM((8, 128), F32),
            pltpu.VMEM((80, 128), F32),
            pltpu.VMEM((896, length_y), F32),
            dma,
            dma((2,)),
            dma,
            dma((ROUNDS,)),
            dma,
            pltpu.SemaphoreType.REGULAR,
            pltpu.SemaphoreType.REGULAR,
        ]
        + ([] if every <= SINGLE_STAGE else [dma]),
        compiler_params=pltpu.CompilerParams(
            collective_id=0, has_side_effects=True, vmem_limit_bytes=VMEM_LIMIT
        ),
    )(*[pltpu.with_memory_space_constraint(value, pltpu.HBM) for value in operands])
    return pl.pallas_call(
        combine,
        out_shape=(
            jax.ShapeDtypeStruct(velocity_old.shape, F32),
            jax.ShapeDtypeStruct((2, points), F32),
        ),
        in_specs=[vmem] * 3,
        out_specs=(hbm, hbm),
        scratch_shapes=[pltpu.VMEM(velocity_old.shape, F32), dma((4,))],
        compiler_params=pltpu.CompilerParams(vmem_limit_bytes=VMEM_LIMIT),
    )(field, factors, neumann)


def solution(mesh):
    placed = (
        P(None, "wall", "span", None),
        P(),
        P(("wall", "span"), None),
        P(("wall", "span"), None),
        P(None, ("wall", "span")),
        P(("wall", "span")),
    )
    return jax.shard_map(
        functools.partial(body, mesh.shape["wall"], mesh.shape["span"]),
        mesh=mesh,
        in_specs=placed,
        out_specs=(P(None, "wall", "span", None), P(None, ("wall", "span"))),
        check_vma=False,
    )
```

```python
import functools
import math

import jax
import jax.numpy as jnp
import numpy as np
from jax import lax
from jax.experimental import pallas as pl
from jax.experimental.pallas import tpu as pltpu
from jax.sharding import PartitionSpec as P

GLL_NODES = (
    -1.0,
    -0.8717401485096066,
    -0.5917001814331423,
    -0.2092992179024789,
    0.2092992179024789,
    0.5917001814331423,
    0.8717401485096066,
    1.0,
)
GLL_WEIGHTS = (
    0.03571428571428571,
    0.2107042271435061,
    0.3411226924835044,
    0.4124587946587038,
    0.4124587946587038,
    0.3411226924835044,
    0.2107042271435061,
    0.03571428571428571,
)
viscosity = 0.02
inverse_step = 20.0
karman = 0.41
sample_height = 0.1
speed_floor = 0.01
element_dx = 0.05
element_dz = 0.13
NEAR = 2
ROUNDS = 2
REACH = 2
TERMS = (
    (0, 0, 0),
    (1, 1, 2),
    (1, 2, 1),
    (2, 2, 2),
    (3, 3, 6),
    (3, 4, 5),
    (3, 5, 4),
    (3, 6, 3),
    (4, 4, 6),
    (4, 6, 4),
    (5, 5, 6),
    (5, 6, 5),
    (6, 6, 6),
)
SINGLE_STAGE = 64
VMEM_LIMIT = 32 * 2**20
MESH = pl.DeviceIdType.MESH
F32 = jnp.float32
BF16 = jnp.bfloat16


def stiffness_table():
    points = np.array(GLL_NODES)
    weights = np.array(GLL_WEIGHTS)
    previous = np.ones(8)
    current = points.copy()
    for degree in range(1, 7):
        previous, current = (
            current,
            ((2 * degree + 1) * points * current - degree * previous) / (degree + 1),
        )
    derivative = np.zeros((8, 8))
    for target in range(8):
        for source in range(8):
            if target != source:
                derivative[target, source] = (
                    current[target] / current[source] / (points[target] - points[source])
                )
    derivative[0, 0] = -14.0
    derivative[7, 7] = 14.0
    return derivative.T @ (weights[:, None] * derivative)


def join_matrix(length):
    joined = np.eye(length)
    for left in range(7, length - 1, 8):
        joined[left, left + 1] = 1.0
        joined[left + 1, left] = 1.0
    return joined


def face_weights(length, open_ends):
    values = np.ones(length)
    position = np.arange(length) % 8
    values[(position == 0) | (position == 7)] = 0.5
    if open_ends:
        values[0] = 1.0
        values[-1] = 1.0
    return values


def split_np(matrix):
    single = jnp.asarray(matrix, F32)
    high = single.astype(BF16)
    low = (jnp.asarray(matrix, F32) - high.astype(F32)).astype(BF16)
    return high, low


def tables(length_x, length_z, length_y):
    weights = np.array(GLL_WEIGHTS)
    stiffness = stiffness_table()
    count_x, count_z, count_y = length_x // 8, length_z // 8, length_y // 8
    mass_x = np.tile(0.5 * element_dx * weights, count_x)
    mass_z = np.tile(0.5 * element_dz * weights, count_z)
    stiff_x = np.kron(np.eye(count_x), stiffness * (2.0 / element_dx))
    stiff_z = np.kron(np.eye(count_z), stiffness * (2.0 / element_dz))
    mass_xz = np.kron(mass_x, mass_z)
    join_xz = np.kron(join_matrix(length_x), join_matrix(length_z))
    join_y = join_matrix(length_y)
    plane = viscosity * (
        np.kron(stiff_x, np.diag(mass_z)) + np.kron(np.diag(mass_x), stiff_z)
    ) + inverse_step * np.diag(mass_xz)
    plane = join_xz @ plane
    mass_plane = join_xz @ mass_xz
    lines_mass = np.tile(0.5 * weights, count_y)[:, None] * join_y
    lines_stiff = viscosity * 2.0 * (np.kron(np.eye(count_y), stiffness) @ join_y)
    lines = np.stack([lines_mass, lines_stiff])
    ring_x = join_matrix(length_x) @ mass_x
    ring_z = join_matrix(length_z) @ mass_z
    ring_x[0] *= 2.0
    ring_x[-1] *= 2.0
    ring_z[0] *= 2.0
    ring_z[-1] *= 2.0
    assembled = inverse_step * np.kron(ring_x, ring_z)
    inner_x = face_weights(length_x, True)
    inner_z = face_weights(length_z, True)
    outer_x = face_weights(length_x, False)
    outer_z = face_weights(length_z, False)
    steps_x, steps_z = np.arange(length_x), np.arange(length_z)
    fringe = np.concatenate(
        [
            steps_x * length_z + length_z - 1,
            steps_x * length_z,
            (length_x - 1) * length_z + steps_z,
            steps_z,
        ]
    )
    outer, inner = np.kron(outer_x, outer_z), np.kron(inner_x, inner_z)
    columns = np.concatenate([assembled, mass_plane, mass_plane[fringe], outer, inner])
    columns = columns.reshape(-1, 1) * np.ones(length_y)[None]
    plane = np.concatenate([plane, plane[fringe]], axis=0)
    reach = 2 * REACH + 1

    def words(length, mass, stiff, extra):
        size = reach * length
        join = join_matrix(size)
        light = join @ np.diag(np.tile(mass, reach))
        heavy = viscosity * join @ np.kron(np.eye(size // 8), stiff) + extra * light
        chains = [
            light,
            heavy @ light,
            light @ light,
            heavy @ heavy @ light,
            heavy @ light @ light,
            light @ heavy @ light,
            light @ light @ light,
        ]
        middle = REACH * length
        chains = [chain[middle : middle + length] for chain in chains]
        return np.concatenate(chains + [np.zeros((128 - 7 * length, size))], axis=0)

    words_x = words(length_x, mass_x, stiffness * (2.0 / element_dx), 0.0)
    words_z = words(length_z, mass_z, stiffness * (2.0 / element_dz), inverse_step)
    full = range(REACH - 1, REACH + 2)
    turned = words_z.T
    ends_z = [2 * REACH * length_z] * 8 + [length_z - 1] * 8
    along_z = np.concatenate(
        [np.tile(turned[iz * length_z : (iz + 1) * length_z], (8, 1)) for iz in full]
        + [np.tile(turned[ends_z], (8, 1))],
        axis=0,
    )
    ends = [2 * REACH * length_x, length_x - 1] * 4
    inner = [ix * length_x + half + (-r) % 8 for ix in full for half in (0, 8) for r in range(8)]
    along_x = np.concatenate(
        [words_x[:, inner], words_x[:, ends]]
        + [np.zeros((128, 8))],
        axis=1,
    )
    return plane, lines, columns, along_x, along_z


def split(value):
    high = value.astype(BF16)
    low = (value - high.astype(F32)).astype(BF16)
    return high, low


def dot3(left, right, dims):
    def one(a, b):
        return lax.dot_general(a, b, (dims, ((), ())), preferred_element_type=F32)

    return one(left[0], right[0]) + (one(left[0], right[1]) + one(left[1], right[0]))


NN = ((1,), (0,))
NT = ((1,), (1,))
TN = ((0,), (0,))
DIRS = ((1, 1), (1, -1), (-1, 1), (-1, -1))


def lagrange_rows(coord):
    points = np.array(GLL_NODES)
    scale = 1.0 / np.prod(points[:, None] - points[None, :] + np.eye(8), axis=1)
    shape = (8, coord.shape[1])
    node = lax.broadcasted_iota(jnp.int32, shape, 0)
    total = jnp.zeros(shape, F32)
    for a in range(8):
        total = jnp.where(node == a, F32(scale[a]), total)
    for b in range(8):
        total = total * jnp.where(node == b, F32(1.0), coord - F32(points[b]))
    return total


def kernel(
    n_wall,
    n_span,
    sizes,
    vel_in,
    heights_in,
    owner_in,
    element_in,
    coords_in,
    roughness_in,
    plane_in,
    lines_in,
    columns_in,
    along_x_in,
    along_z_in,
    field,
    factors,
    neumann,
    vel,
    heights,
    owner,
    element,
    coords,
    roughness,
    sheet,
    lines,
    columns,
    along_x,
    along_z,
    load_sem,
    near,
    near_got,
    face_send,
    face_got,
    parts,
    sum_send,
    wall_got,
    span_got,
    pull_send,
    edge_send,
    pull_got,
    everything,
    sent,
    near_rs,
    pull_rs,
    face_rs,
    wall_rs,
    step_one,
    step_two,
    *span_rs,
):
    length_x, length_z, length_y = sizes
    rows = length_x * length_z
    count_z, count_y = length_z // 8, length_y // 8
    w = lax.axis_index("wall")
    s = lax.axis_index("span")

    def turned(place, count):
        return place & (count - 1) if count & (count - 1) == 0 else lax.rem(place, count)

    def at(dx, dz):
        return (turned(w + (dx + n_wall), n_wall), turned(s + (dz + n_span), n_span))

    pltpu.make_async_copy(vel_in, vel, load_sem.at[0]).start()
    single = n_wall * n_span <= SINGLE_STAGE
    stepwise = single and 3 <= n_wall <= 4 * REACH and 3 <= n_span <= 4 * REACH
    across_wall = ((1, 0), (-1, 0))
    if stepwise:
        greeted = across_wall + tuple((0, k) for k in range(1, n_span))
    elif single:
        greeted = [divmod(k, n_span) for k in range(1, n_wall * n_span)]
    else:
        greeted = [(k, 0) for k in range(1, n_wall)] + [(0, k) for k in range(1, n_span)]
        greeted += sorted(
            {
                ((dx + n_wall) % n_wall, (dz + n_span) % n_span)
                for dx in range(-REACH, REACH + 1)
                for dz in range(-REACH, REACH + 1)
            }
            - {(0, 0)}
            - set(greeted)
        )
    barrier = pltpu.get_barrier_semaphore()

    def greet(semaphore, places):
        for dx, dz in places:
            pl.semaphore_signal(semaphore, inc=1, device_id=at(dx, dz), device_id_type=MESH)

    greet(barrier, greeted)

    edges = 2 * (length_x + length_z)
    early, late = pl.ds(0, 2 * rows + edges), pl.ds(2 * rows + edges, 2 * rows)

    def column(index):
        first = index * rows + (edges if index > 1 else 0)
        return columns[first : first + rows, :]

    loads = {
        "vel": [(vel_in, vel)],
        "heights": [(heights_in, heights)],
        "operator": [
            (lines_in, lines),
            (columns_in.at[early], columns.at[early]),
            (plane_in, sheet),
        ],
        "coords": [(coords_in, coords)],
        "points": [(owner_in, owner), (element_in, element), (roughness_in, roughness)],
        "words": [
            (along_x_in, along_x),
            (along_z_in, along_z),
            (columns_in.at[late], columns.at[late]),
        ],
    }
    for index, group in list(enumerate(loads.values()))[1:]:
        for source, target in group:
            pltpu.make_async_copy(source, target, load_sem.at[index]).start()

    def loaded(*names):
        for name in names:
            index, group = list(loads).index(name), loads[name]
            whole = group[0][1]
            if len(group) > 1:
                size = sum(math.prod(ref.shape) * ref.dtype.itemsize for _, ref in group)
                whole = everything.at[pl.ds(0, size // (4 * length_y)), :]
            pltpu.make_async_copy(whole, whole, load_sem.at[index]).wait()

    loaded("vel")
    lane = lax.broadcasted_iota(jnp.int32, (64, length_y), 1)
    groups = (length_x // 8) * count_z
    depth = 8 * NEAR
    strips = length_y // depth
    packed = [jnp.zeros((64, length_y), F32)] * 2
    for index, comp in enumerate((0, 2)):
        for group in range(groups):
            ex, ez = group // count_z, group % count_z
            block = vel[comp, pl.ds(ex * 8, 8), pl.ds(ez * 8, 8), :].reshape(64, length_y)
            place = index * groups + group
            moved = pltpu.roll(block, place * depth, 1) if place else block
            for wall_side in range(2):
                strip = (place - wall_side) % strips
                packed[wall_side] = jnp.where(lane // depth == strip, moved, packed[wall_side])
    for wall_side in range(2):
        near[wall_side] = packed[wall_side]
    def remote(src, dst, ss, rs, where):
        return pltpu.make_async_remote_copy(
            src_ref=src,
            dst_ref=dst,
            send_sem=ss,
            recv_sem=rs,
            device_id=where,
            device_id_type=MESH,
        )

    near_copies = []
    for wall_side in range(2):
        for slot, dx in enumerate((1, -1)):
            target = near_got.at[wall_side, slot]
            near_copies.append(
                remote(near.at[wall_side], target, sent, near_rs.at[wall_side], at(dx, 0))
            )

    def enter():
        pl.semaphore_wait(barrier, len(greeted))
        if stepwise:
            greet(step_one, across_wall)
        for copy in near_copies:
            copy.start()

    if stepwise:
        enter()
    loaded("heights", "operator")

    layer_of = lax.broadcasted_iota(jnp.int32, (length_y, count_y), 0) // 8
    layer = lax.broadcasted_iota(jnp.int32, (length_y, count_y), 1)
    height_row = heights[...]
    height = jnp.sum(jnp.where(layer_of == layer, height_row, 0.0), axis=1, keepdims=True)
    lines_mass = height * lines[0]
    lines_stiff = lines[1] / height
    stiff_hi, stiff_lo = split(lines_stiff)
    lines_packed = jnp.concatenate(
        [
            jnp.concatenate([stiff_hi, stiff_lo], axis=1),
            jnp.concatenate([stiff_hi, jnp.zeros_like(stiff_lo)], axis=1),
        ],
        axis=0,
    )
    bound = jnp.max(0.1535 * height_row + 0.000182 / height_row, axis=1, keepdims=True)
    shifts = (0.15 * bound, 0.85 * bound)

    mass_row = jnp.sum(lines_mass, axis=0, keepdims=True)
    scale = column(0) * mass_row
    for c in range(3):
        field[0, c] = vel[c].reshape(rows, length_y) * scale

    face_rows = []
    for slot, (dx, dz) in enumerate(DIRS + ((0, 1), (0, -1), (1, 0), (-1, 0))):
        size = 3 * (1 if dx and dz else length_z if dx else length_x)
        face_rows.append((sum(entry[1] for entry in face_rows), size, dx, dz))
    face_total = sum(entry[1] for entry in face_rows)
    z_first = {entry[3]: entry[0] for entry in face_rows if entry[2] == 0}

    def corner(dx, dz):
        return (rows - length_z if dx == 1 else 0) + (length_z - 1 if dz == 1 else 0)

    def face_part(slot, c, dx, dz):
        first, size = face_rows[slot][0] + c * (face_rows[slot][1] // 3), face_rows[slot][1] // 3
        if dx and dz:
            rows_of = pl.ds(corner(dx, dz), 1)
        elif dx:
            rows_of = pl.ds(rows - length_z if dx == 1 else 0, length_z)
        else:
            rows_of = pl.ds(length_z - 1 if dz == 1 else 0, length_x, stride=length_z)
        return pl.ds(first, size), rows_of

    def send_faces(turn, fringe):
        for c in range(3):
            for slot, (first, size, dx, dz) in enumerate(face_rows):
                size //= 3
                if dx and dz:
                    begin = 2 * length_x + (length_z if dx == -1 else 0)
                    begin += length_z - 1 if dz == 1 else 0
                elif dx:
                    begin = 2 * length_x + (length_z if dx == -1 else 0)
                else:
                    begin = length_x if dz == -1 else 0
                rows_here = slice(first + c * size, first + (c + 1) * size)
                face_send[turn, rows_here, :] = fringe[c][begin : begin + size]
        first_turn = turn == 0 and stepwise
        if turn == 0 and not stepwise:
            enter()
        for stage in ((0,), (2, 1)) if first_turn else ((2, 0, 1),):
            if stage[0] == 2 and first_turn:
                pl.semaphore_wait(step_one, len(across_wall))
                greet(step_two, across_wall)
            for kind in stage:
                for first, size, dx, dz in face_rows:
                    if (2 if dx and dz else abs(dx)) != kind:
                        continue
                    if kind == 0:
                        swap = jnp.where(s == 0, -dz, dz)
                        first = pl.multiple_of(jnp.where(swap == 1, z_first[1], z_first[-1]), 4)
                        dz = swap
                    part = (turn, pl.ds(first, size), slice(None))
                    remote(
                        face_send.at[part],
                        face_got.at[part],
                        sent,
                        face_rs.at[turn],
                        at(dx, dz),
                    ).start()

    def settle(semaphore, ref):
        pltpu.make_async_copy(ref, ref, semaphore).wait()

    def add_faces(turn):
        settle(face_rs.at[turn], face_got.at[turn, pl.ds(0, face_total), :])
        for c in range(3):
            for slot, (_, _, dx, dz) in enumerate(face_rows):
                packed_rows, rows_of = face_part(slot, c, -dx, -dz)
                field[turn + 1, c, rows_of, :] = (
                    field[turn + 1, c, rows_of, :] + face_got[turn, packed_rows, :]
                )

    def inner(quantity, c, product):
        parts[quantity * 8 + c : quantity * 8 + c + 1, :] = jnp.sum(
            product, axis=0, keepdims=True
        )

    def operate(turn):
        highs, lows = zip(*[split(field[turn, c]) for c in range(3)])
        packed = [jnp.concatenate(pair, axis=1) for pair in zip(highs, lows)]
        wide = jnp.concatenate(highs + lows, axis=1)
        wide_high = jnp.concatenate(highs, axis=1)

        def image(first, count, lines_of, weight):
            along_y = jnp.dot(
                jnp.concatenate(lines_of, axis=0), lines_packed, preferred_element_type=F32
            )
            part = slice(first, first + count)
            across = jnp.dot(sheet[0, part], wide, preferred_element_type=F32)
            across_low = jnp.dot(sheet[1, part], wide_high, preferred_element_type=F32)
            results = []
            for c in range(3):
                here = slice(c * length_y, (c + 1) * length_y)
                also = slice((3 + c) * length_y, (4 + c) * length_y)
                flat = across[:, here] + (across[:, also] + across_low[:, here])
                tall = along_y[c * count : (c + 1) * count]
                tall = tall[:, :length_y] + tall[:, length_y:]
                results.append(flat * mass_row + tall * weight)
            return results

        lines_of = []
        for c in range(3):
            value = jnp.concatenate(
                [
                    field[turn, c, pl.ds(length_z - 1, length_x, stride=length_z), :],
                    field[turn, c, pl.ds(0, length_x, stride=length_z), :],
                    field[turn, c, pl.ds(rows - length_z, length_z), :],
                    field[turn, c, pl.ds(0, length_z), :],
                ],
                axis=0,
            )
            lines_of.append(jnp.concatenate(split(value), axis=1))
        weight = columns[2 * rows : 2 * rows + edges, :]
        send_faces(turn, image(rows, edges, lines_of, weight))
        for c, value in enumerate(image(0, rows, packed, column(1))):
            field[turn + 1, c] = value

    slots = {(0, 0): 0, (0, 1): 1, (1, 1): 2, (0, 2): 3, (1, 2): 4, (2, 2): 5}

    def inner_products(newest):
        for c in range(3):
            weighted = field[newest, c] * column(2)
            for other in range(newest + 1):
                inner(slots[(other, newest)], c, weighted * field[other, c])

    operate(0)
    parts[...] = jnp.zeros_like(parts)

    loaded("coords", "points")
    points = owner.shape[1]
    row_x = lagrange_rows(coords[0:1, :])
    row_z = lagrange_rows(coords[1:2, :])
    row_y = lagrange_rows(coords[2:3, :])
    cross = jnp.concatenate([row_x[a : a + 1] * row_z for a in range(8)], axis=0)
    distance = lax.rem(owner[...] - w + n_wall, n_wall)
    from_next = distance == 1
    from_prev = distance == n_wall - 1
    own = jnp.logical_not(jnp.logical_or(from_next, from_prev))
    spread = jnp.concatenate(
        [jnp.where(mask, cross, 0.0) for mask in (own, from_prev, from_next)], axis=0
    )
    half = points // 2
    n_row = lax.broadcasted_iota(jnp.int32, (groups * depth, points), 0)
    side_of = lax.broadcasted_iota(jnp.int32, (groups * depth, points), 1) // half
    layer_y = (n_row % depth) // 8 + side_of * (count_y - NEAR)
    wanted = (n_row // depth) * count_y + layer_y == element[...]
    along = jnp.where(wanted, jnp.concatenate([row_y] * (groups * NEAR), axis=0), 0.0)
    spread = split(spread)
    drag = karman / jnp.log(sample_height / roughness[...])
    drag = drag * drag * (-1.0 / viscosity)

    sampled = []
    for wall_side in range(2):
        settle(near_rs.at[wall_side], near_got.at[wall_side])
        sources = jnp.concatenate(
            [near[wall_side], near_got[wall_side, 0], near_got[wall_side, 1]], axis=0
        )
        here = slice(wall_side * half, (wall_side + 1) * half)
        values = dot3(split(sources), tuple(part[:, here] for part in spread), TN)
        total = []
        for index in range(2):
            strip_rows = [
                (place - wall_side) % strips * depth
                for place in range(index * groups, (index + 1) * groups)
            ]
            own_rows = jnp.concatenate([values[k : k + depth] for k in strip_rows], axis=0)
            total.append(jnp.sum(own_rows * along[:, here], axis=0, keepdims=True))
        sampled.append(total)
    stream, spanwise = [jnp.concatenate(both, axis=1) for both in zip(*sampled)]
    speed = jnp.sqrt(stream * stream + spanwise * spanwise + speed_floor)
    factor = drag * speed
    gradient = (factor * stream, factor * spanwise)
    neumann[0:1, :] = gradient[0]
    neumann[1:2, :] = gradient[1]

    planes = []
    for index in range(2):
        pull = viscosity * gradient[index]
        planes += [pull[:, :rows], pull[:, rows:]]
    tiles = 4 * length_x // 8
    tile_lane = lax.broadcasted_iota(jnp.int32, (8, 128), 1)
    tile_row = lax.broadcasted_iota(jnp.int32, (8, 128), 0)
    block_of = tile_lane // length_z
    bundle = jnp.zeros((8, 128), F32)
    fringe = jnp.zeros((8, 128), F32)
    for tile in range(tiles):
        part = planes[tile // 2][:, 128 * (tile % 2) : 128 * (tile % 2) + 128]
        part = jnp.broadcast_to(part, (8, 128))
        spread_rows = pltpu.roll(part, 0, 1, stride=length_z, stride_axis=0)
        spread_rows = pltpu.roll(spread_rows, (8 - tile) % 8, 0)
        bundle = jnp.where(block_of == tile, spread_rows, bundle)
        for end in range(2):
            slanted = pltpu.roll(part, 7 * (1 - end), 1, stride=length_z - 1, stride_axis=0)
            wanted_lane = tile * length_z + 8 * end + 7 - tile_row
            fringe = jnp.where(tile_lane == wanted_lane, slanted, fringe)
    pull_send[...] = bundle
    edge_send[0:1, :] = jnp.sum(fringe, axis=0, keepdims=True)
    edge_send[1:2, :] = jnp.where(block_of[0:1] % 2 == 0, bundle[0:1], bundle[1:2])
    if stepwise:
        pl.semaphore_wait(step_two, len(across_wall))
    reach = 2 * REACH + 1
    offsets = [
        (dx, dz)
        for dx in range(-REACH, REACH + 1)
        for dz in range(-REACH, REACH + 1)
        if (dx, dz) != (0, 0)
    ]
    nearby = [place for place in offsets if max(abs(place[0]), abs(place[1])) < REACH]
    remaining = [place for place in offsets if place not in nearby]
    pull_rows = {place: pl.ds(8 * index, 8) for index, place in enumerate(nearby)}
    for index, place in enumerate(remaining):
        pull_rows[place] = pl.ds(8 * len(nearby) + index, 1)
    for dx, dz in sorted(offsets, key=lambda pair: -abs(pair[0]) - abs(pair[1])):
        if (dx, dz) in nearby:
            source = pull_send
        else:
            source = edge_send.at[pl.ds(0 if abs(dz) == REACH else 1, 1), :]
        remote(
            source, pull_got.at[pull_rows[(-dx, -dz)], :], sent, pull_rs, at(dx, dz)
        ).start()

    add_faces(0)
    operate(1)
    loaded("words")
    lines_rows = jnp.concatenate([lines_mass, lines_stiff], axis=1)
    ends = [lines_rows[0:1], lines_rows[length_y - 1 : length_y]]
    once = [(end[:, :length_y], end[:, length_y:]) for end in ends]
    twice = dot3(
        split(jnp.concatenate([once[0][0], once[0][1], once[1][0], once[1][1]] * 2, axis=0)),
        split(lines_rows),
        NN,
    )
    one_lane = lax.broadcasted_iota(jnp.int32, (1, length_y), 1)
    zero = jnp.zeros((1, length_y), F32)
    images = []
    for side in range(2):
        by_mass, by_stiff = twice[2 * side : 2 * side + 1], twice[2 * side + 1 : 2 * side + 2]
        moved_tip = jnp.where(one_lane == length_y // 2 - side, 1.0, 0.0)
        rows_of = [
            (zero, moved_tip),
            (zero, once[side][0]),
            (zero, once[side][1]),
            (by_mass[:, :length_y], zero),
            (by_stiff[:, :length_y], zero),
            (by_mass[:, length_y:], zero),
            (by_stiff[:, length_y:], zero),
        ]
        for entry in rows_of:
            image = jnp.concatenate(entry, axis=1)
            images.append(jnp.broadcast_to(image, (length_z, 2 * length_y)))
        images.append(jnp.zeros((128 - 7 * length_z, 2 * length_y), F32))
    images = split(jnp.concatenate(images, axis=0))
    low_half = tile_lane & 8 == 0
    low_rows = tile_row & 1 == 0
    diagonal_of = (tile_lane + tile_row) & 7

    def halves(value):
        return split(value)

    def both_tiles(pair, mask_of):
        masks = [jnp.where(mask_of(tile), 1.0, 0.0) for tile in (2 * pair, 2 * pair + 1)]
        return jnp.concatenate(masks, axis=0).astype(BF16)

    block_masks = [both_tiles(pair, lambda tile: block_of == tile) for pair in range(tiles // 2)]
    end_masks = [
        both_tiles(
            pair,
            lambda tile: jnp.logical_and(block_of == tile, diagonal_of == (7 - tile) % 8),
        )
        for pair in range(tiles // 2)
    ]
    settle(pull_rs, pull_got)

    def edge(dx, dz):
        return jnp.broadcast_to(pull_got[pull_rows[(dx, dz)], :], (8, 128))

    def both_ends(dx):
        return jnp.where(low_half, edge(dx, REACH), edge(dx, -REACH))

    middle = range(-REACH + 1, REACH)

    def doubled(part):
        return [jnp.concatenate([half, half], axis=0) for half in (part[0], part[1])]

    spans = ([], [])
    for dx in middle:
        parts_z = [bundle if (dx, dz) == (0, 0) else pull_got[pull_rows[(dx, dz)], :] for dz in middle]
        pairs = [doubled(halves(part)) for part in parts_z]
        ends = doubled(halves(both_ends(dx)))
        for pair in range(tiles // 2):
            for out, which in zip(spans, range(2)):
                pieces = [part[which] * block_masks[pair] for part in pairs]
                pieces.append(ends[which] * end_masks[pair])
                out.append(jnp.concatenate(pieces, axis=1))
    pieces = [
        jnp.where(block_of == tile_row, jnp.where(low_rows, edge(REACH, dz), edge(-REACH, dz)), 0.0)
        for dz in middle
    ]
    kept = jnp.logical_and(
        block_of == tile_row, (tile_lane + tile_row + (tile_row & 1)) & 7 == 7
    )
    ends = jnp.where(low_rows, both_ends(REACH), both_ends(-REACH))
    pieces.append(jnp.where(kept, ends, 0.0))
    last = jnp.concatenate([jnp.concatenate(pieces, axis=1), jnp.zeros((8, 512), F32)], axis=0)
    for out, half in zip(spans, split(last)):
        out.append(half)
    spans_hi, spans_lo = [jnp.concatenate(out, axis=0) for out in spans]
    reached = jnp.dot(spans_hi, along_z[...], preferred_element_type=F32)
    reached = (reached[:, :128] + reached[:, 128:]) + jnp.dot(
        spans_lo, along_z[:, :128], preferred_element_type=F32
    )
    by_plane = []
    for plane in range(4):
        kept = [
            reached[ix * 64 + plane * length_x : ix * 64 + (plane + 1) * length_x]
            for ix in range(len(middle))
        ]
        last = reached[64 * len(middle) : 64 * len(middle) + 8]
        kept.append(jnp.where(tile_row // 2 == plane, last, 0.0))
        kept.append(jnp.zeros((8, 128), F32))
        by_plane.append(jnp.concatenate(kept, axis=0))
    stacked_hi, stacked_lo = split(jnp.concatenate(by_plane, axis=1))
    both_ways = jnp.dot(
        along_x[:, : 3 * stacked_hi.shape[0]],
        jnp.concatenate([stacked_hi, stacked_lo, stacked_hi], axis=0),
        preferred_element_type=F32,
    )
    block_lane = lax.broadcasted_iota(jnp.int32, (length_x, 128), 1) // length_z
    keep_row = lax.rem(lax.broadcasted_iota(jnp.int32, (rows, 256), 0), length_z)
    keep_lane = lax.rem(lax.broadcasted_iota(jnp.int32, (rows, 256), 1), length_z)
    wall_lane = lax.broadcasted_iota(jnp.int32, (rows, length_y), 1)
    tractions = []
    for index in range(2):
        blocks = []
        for side in range(2):
            plane = index * 2 + side
            total = jnp.zeros((length_x, 128), F32)
            for block, word_x, word_z in TERMS:
                piece = both_ways[
                    word_x * length_x : (word_x + 1) * length_x, plane * 128 : plane * 128 + 128
                ]
                shift = ((block - word_z) * length_z) % 128
                moved = pltpu.roll(piece, shift, 1) if shift else piece
                total = total + jnp.where(block_lane == block, moved, 0.0)
            blocks.append(total)
        wide = jnp.concatenate(blocks, axis=1)
        tall = jnp.concatenate(
            [jnp.broadcast_to(wide[x : x + 1], (length_z, 256)) for x in range(length_x)], axis=0
        )
        tall = jnp.where(keep_row == keep_lane, tall, 0.0)
        deep = dot3(split(tall), images, NN)
        level_two, shallow = deep[:, :length_y], deep[:, length_y:]
        tip = jnp.logical_or(wall_lane == 0, wall_lane == length_y - 1)
        level_zero = jnp.where(tip, pltpu.roll(shallow, length_y // 2, 1), 0.0)
        outside = jnp.logical_or(wall_lane < length_y // 4, wall_lane >= 3 * length_y // 4)
        level_one = jnp.where(outside, shallow, 0.0)
        tractions.append((level_zero, level_one, level_two))
    t1, t2 = shifts
    for c in range(3):
        chain = [field[level, c] for level in range(3)]
        if c != 1:
            taus = tractions[c // 2]
            chain = [chain[level] + taus[level] for level in range(3)]
        v1 = chain[1] - t1 * chain[0]
        field[0, c] = chain[0]
        field[1, c] = v1
        field[2, c] = chain[2] - t1 * chain[1] - t2 * v1
    for newest in range(2):
        inner_products(newest)
    add_faces(1)
    highs = [field[2, c].astype(BF16) for c in range(3)]
    along_y = jnp.dot(
        jnp.concatenate(highs, axis=0), lines_packed[:length_y], preferred_element_type=F32
    )
    wide = jnp.concatenate(highs, axis=1)
    across = jnp.dot(sheet[0, :rows], wide, preferred_element_type=F32)
    across_low = jnp.dot(sheet[1, :rows], wide, preferred_element_type=F32)
    inner_products(2)
    for c in range(3):
        here = slice(c * length_y, (c + 1) * length_y)
        tall = along_y[c * rows : (c + 1) * rows]
        tall = tall[:, :length_y] + tall[:, length_y:]
        image = (across[:, here] + across_low[:, here]) * mass_row + tall * column(1)
        value = field[2, c]
        partner = value + (value - highs[c].astype(F32))
        inner(6, c, partner * column(3) * image)

    total_rows = parts.shape[0]
    r_iota = lax.broadcasted_iota(jnp.int32, (total_rows, 128), 0)
    l_iota = lax.broadcasted_iota(jnp.int32, (total_rows, 128), 1)
    diagonal = r_iota == l_iota
    end_lane = lax.broadcasted_iota(jnp.int32, (total_rows, 128), 1)
    shared = jnp.logical_or(end_lane % 8 == 0, end_lane % 8 == 7)
    tips = jnp.logical_or(end_lane == 0, end_lane == length_y - 1)
    weight_y = jnp.where(jnp.logical_and(shared, jnp.logical_not(tips)), 0.5, 1.0)
    summed = jnp.sum(parts[...] * weight_y, axis=1, keepdims=True)
    row = jnp.sum(jnp.where(diagonal, summed, 0.0), axis=0, keepdims=True)

    def gather_sum(stage, row, count, got, rs, place):
        sum_send[stage : stage + 1, :] = row
        def ring(place, size):
            return min(place % size, -place % size)

        def reach_of(k):
            if count != n_wall * n_span:
                return ring(k, count)
            return ring(k // n_span, n_wall) + ring(k % n_span, n_span)

        for k in sorted(range(1, count), key=reach_of, reverse=True):
            remote(
                sum_send.at[pl.ds(stage, 1), :], got.at[pl.ds(k - 1, 1), :], sent, rs, place(k)
            ).start()
        settle(rs, got)
        return row + jnp.sum(got[...], axis=0, keepdims=True)

    sum_rows = 0
    if single:
        every = n_wall * n_span
        row = gather_sum(0, row, every, wall_got, wall_rs, lambda k: at(k // n_span, k % n_span))
        sum_rows = every - 1
    else:
        row = gather_sum(0, row, n_wall, wall_got, wall_rs, lambda k: at(k, 0))
        row = gather_sum(1, row, n_span, span_got, span_rs[0], lambda k: at(0, k))
        sum_rows = n_wall + n_span - 2
    sent_rows = 2 * 2 * 64 + pull_got.shape[0] + ROUNDS * face_total + sum_rows
    settle(sent, everything.at[pl.ds(0, sent_rows), :])
    totals = jnp.sum(jnp.where(diagonal, row, 0.0), axis=1, keepdims=True)
    m00, m01, m11, m02, m12, m22, e22 = [totals[q * 8 : q * 8 + 8, :] for q in range(7)]
    t1, t2 = shifts
    a00 = m01 + t1 * m00
    a01 = m11 + t1 * m01
    a02 = m12 + t1 * m02
    a11 = m12 + t2 * m11
    a12 = m22 + t2 * m12
    l10 = a01 / a00
    l20 = a02 / a00
    d1 = a11 - l10 * a01
    u12 = a12 - l10 * a02
    l21 = u12 / d1
    d2 = e22 - l20 * a02 - l21 * u12
    y1 = m01 - l10 * m00
    y2 = m02 - l20 * m00 - l21 * y1
    x2 = y2 / d2
    x1 = y1 / d1 - l21 * x2
    x0 = m00 / a00 - l10 * x1 - l20 * x2
    for index, value in enumerate((x0, x1, x2)):
        factors[index] = jnp.broadcast_to(value, (8, 128))


def combine(field, factors, neumann_in, out, neumann, stage, sems):
    small = pltpu.make_async_copy(neumann_in, neumann, sems.at[3])
    small.start()
    copies = []
    for c in range(3):
        result = factors[0, c : c + 1] * field[0, c]
        for level in range(1, 3):
            result += factors[level, c : c + 1] * field[level, c]
        stage[c] = result.reshape(stage.shape[1:])
        copy = pltpu.make_async_copy(stage.at[c], out.at[c], sems.at[c])
        copy.start()
        copies.append(copy)
    for copy in copies:
        copy.wait()
    small.wait()


def body(n_wall, n_span, velocity_old, heights, owner_device, owner_element, ref_coords, roughness):
    sizes = velocity_old.shape[1:]
    length_x, length_z, length_y = sizes
    rows = length_x * length_z
    points = owner_device.shape[0]
    plane, lines, columns, along_x, along_z = tables(*sizes)
    along_x_hi, along_x_lo = split_np(along_x)
    every = n_wall * n_span
    first = every if every <= SINGLE_STAGE else n_wall
    faces = -(-(6 * (length_x + length_z) + 12) // 8) * 8
    vmem = pl.BlockSpec(memory_space=pltpu.VMEM)
    hbm = pl.BlockSpec(memory_space=pltpu.HBM)
    operands = (
        velocity_old,
        heights.reshape(1, -1),
        owner_device.reshape(1, -1),
        owner_element.reshape(1, -1),
        ref_coords,
        roughness.reshape(1, -1),
        jnp.stack(split_np(plane)),
        jnp.asarray(lines, F32),
        jnp.asarray(columns, F32),
        jnp.pad(jnp.concatenate([along_x_hi, along_x_hi, along_x_lo], axis=1), ((0, 0), (0, 64))),
        jnp.concatenate(split_np(along_z), axis=1),
    )
    dma = pltpu.SemaphoreType.DMA
    field, factors, neumann = pl.pallas_call(
        functools.partial(kernel, n_wall, n_span, sizes),
        out_shape=(
            pltpu.VMEM((3, 3, rows, length_y), F32),
            pltpu.VMEM((3, 8, 128), F32),
            pltpu.VMEM((2, points), F32),
        ),
        in_specs=[hbm] * 11,
        out_specs=(vmem, vmem, vmem),
        scratch_shapes=[pltpu.VMEM(value.shape, value.dtype) for value in operands]
        + [
            dma((6,)),
            pltpu.VMEM((2, 64, length_y), F32),
            pltpu.VMEM((2, 2, 64, length_y), F32),
            pltpu.VMEM((ROUNDS, faces, length_y), F32),
            pltpu.VMEM((ROUNDS, faces, length_y), F32),
            pltpu.VMEM((56, length_y), F32),
            pltpu.VMEM((2, 128), F32),
            pltpu.VMEM((first - 1, 128), F32),
            pltpu.VMEM((n_span - 1, 128), F32),
            pltpu.VMEM((8, 128), F32),
            pltpu.VMEM((8, 128), F32),
            pltpu.VMEM((80, 128), F32),
            pltpu.VMEM((1536, length_y), F32),
            dma,
            dma((2,)),
            dma,
            dma((ROUNDS,)),
            dma,
            pltpu.SemaphoreType.REGULAR,
            pltpu.SemaphoreType.REGULAR,
        ]
        + ([] if every <= SINGLE_STAGE else [dma]),
        compiler_params=pltpu.CompilerParams(
            collective_id=0, has_side_effects=True, vmem_limit_bytes=VMEM_LIMIT
        ),
    )(*[pltpu.with_memory_space_constraint(value, pltpu.HBM) for value in operands])
    return pl.pallas_call(
        combine,
        out_shape=(
            jax.ShapeDtypeStruct(velocity_old.shape, F32),
            jax.ShapeDtypeStruct((2, points), F32),
        ),
        in_specs=[vmem] * 3,
        out_specs=(hbm, hbm),
        scratch_shapes=[pltpu.VMEM(velocity_old.shape, F32), dma((4,))],
        compiler_params=pltpu.CompilerParams(vmem_limit_bytes=VMEM_LIMIT),
    )(field, factors, neumann)


def solution(mesh):
    placed = (
        P(None, "wall", "span", None),
        P(),
        P(("wall", "span"), None),
        P(("wall", "span"), None),
        P(None, ("wall", "span")),
        P(("wall", "span")),
    )
    return jax.shard_map(
        functools.partial(body, mesh.shape["wall"], mesh.shape["span"]),
        mesh=mesh,
        in_specs=placed,
        out_specs=(P(None, "wall", "span", None), P(None, ("wall", "span"))),
        check_vma=False,
    )
```

```python
import functools
import math

import jax
import jax.numpy as jnp
import numpy as np
from jax import lax
from jax.experimental import pallas as pl
from jax.experimental.pallas import tpu as pltpu
from jax.sharding import PartitionSpec as P

GLL_NODES = (
    -1.0,
    -0.8717401485096066,
    -0.5917001814331423,
    -0.2092992179024789,
    0.2092992179024789,
    0.5917001814331423,
    0.8717401485096066,
    1.0,
)
GLL_WEIGHTS = (
    0.03571428571428571,
    0.2107042271435061,
    0.3411226924835044,
    0.4124587946587038,
    0.4124587946587038,
    0.3411226924835044,
    0.2107042271435061,
    0.03571428571428571,
)
viscosity = 0.02
inverse_step = 20.0
karman = 0.41
sample_height = 0.1
speed_floor = 0.01
element_dx = 0.05
element_dz = 0.13
NEAR = 2
ROUNDS = 2
REACH = 2
TERMS = (
    (0, 0, 0),
    (1, 1, 2),
    (1, 2, 1),
    (2, 2, 2),
    (3, 3, 6),
    (3, 4, 5),
    (3, 5, 4),
    (3, 6, 3),
    (4, 4, 6),
    (4, 6, 4),
    (5, 5, 6),
    (5, 6, 5),
    (6, 6, 6),
)
SINGLE_STAGE = 64
VMEM_LIMIT = 32 * 2**20
MESH = pl.DeviceIdType.MESH
F32 = jnp.float32
BF16 = jnp.bfloat16


def stiffness_table():
    points = np.array(GLL_NODES)
    weights = np.array(GLL_WEIGHTS)
    previous = np.ones(8)
    current = points.copy()
    for degree in range(1, 7):
        previous, current = (
            current,
            ((2 * degree + 1) * points * current - degree * previous) / (degree + 1),
        )
    derivative = np.zeros((8, 8))
    for target in range(8):
        for source in range(8):
            if target != source:
                derivative[target, source] = (
                    current[target] / current[source] / (points[target] - points[source])
                )
    derivative[0, 0] = -14.0
    derivative[7, 7] = 14.0
    return derivative.T @ (weights[:, None] * derivative)


def join_matrix(length):
    joined = np.eye(length)
    for left in range(7, length - 1, 8):
        joined[left, left + 1] = 1.0
        joined[left + 1, left] = 1.0
    return joined


def face_weights(length, open_ends):
    values = np.ones(length)
    position = np.arange(length) % 8
    values[(position == 0) | (position == 7)] = 0.5
    if open_ends:
        values[0] = 1.0
        values[-1] = 1.0
    return values


def split_np(matrix):
    single = jnp.asarray(matrix, F32)
    high = single.astype(BF16)
    low = (jnp.asarray(matrix, F32) - high.astype(F32)).astype(BF16)
    return high, low


def tables(length_x, length_z, length_y):
    weights = np.array(GLL_WEIGHTS)
    stiffness = stiffness_table()
    count_x, count_z, count_y = length_x // 8, length_z // 8, length_y // 8
    mass_x = np.tile(0.5 * element_dx * weights, count_x)
    mass_z = np.tile(0.5 * element_dz * weights, count_z)
    stiff_x = np.kron(np.eye(count_x), stiffness * (2.0 / element_dx))
    stiff_z = np.kron(np.eye(count_z), stiffness * (2.0 / element_dz))
    mass_xz = np.kron(mass_x, mass_z)
    join_xz = np.kron(join_matrix(length_x), join_matrix(length_z))
    join_y = join_matrix(length_y)
    plane = viscosity * (
        np.kron(stiff_x, np.diag(mass_z)) + np.kron(np.diag(mass_x), stiff_z)
    ) + inverse_step * np.diag(mass_xz)
    plane = join_xz @ plane
    mass_plane = join_xz @ mass_xz
    lines_mass = np.tile(0.5 * weights, count_y)[:, None] * join_y
    lines_stiff = viscosity * 2.0 * (np.kron(np.eye(count_y), stiffness) @ join_y)
    lines = np.stack([lines_mass, lines_stiff])
    ring_x = join_matrix(length_x) @ mass_x
    ring_z = join_matrix(length_z) @ mass_z
    ring_x[0] *= 2.0
    ring_x[-1] *= 2.0
    ring_z[0] *= 2.0
    ring_z[-1] *= 2.0
    assembled = inverse_step * np.kron(ring_x, ring_z)
    inner_x = face_weights(length_x, True)
    inner_z = face_weights(length_z, True)
    outer_x = face_weights(length_x, False)
    outer_z = face_weights(length_z, False)
    steps_x, steps_z = np.arange(length_x), np.arange(length_z)
    fringe = np.concatenate(
        [
            steps_x * length_z + length_z - 1,
            steps_x * length_z,
            (length_x - 1) * length_z + steps_z,
            steps_z,
        ]
    )
    outer, inner = np.kron(outer_x, outer_z), np.kron(inner_x, inner_z)
    columns = np.concatenate([assembled, mass_plane, mass_plane[fringe], outer, inner])
    columns = columns.reshape(-1, 1) * np.ones(length_y)[None]
    plane = np.concatenate([plane, plane[fringe]], axis=0)
    reach = 2 * REACH + 1

    def words(length, mass, stiff, extra):
        size = reach * length
        join = join_matrix(size)
        light = join @ np.diag(np.tile(mass, reach))
        heavy = viscosity * join @ np.kron(np.eye(size // 8), stiff) + extra * light
        chains = [
            light,
            heavy @ light,
            light @ light,
            heavy @ heavy @ light,
            heavy @ light @ light,
            light @ heavy @ light,
            light @ light @ light,
        ]
        middle = REACH * length
        chains = [chain[middle : middle + length] for chain in chains]
        return np.concatenate(chains + [np.zeros((128 - 7 * length, size))], axis=0)

    words_x = words(length_x, mass_x, stiffness * (2.0 / element_dx), 0.0)
    words_z = words(length_z, mass_z, stiffness * (2.0 / element_dz), inverse_step)
    full = range(REACH - 1, REACH + 2)
    turned = words_z.T
    ends_z = [2 * REACH * length_z] * 8 + [length_z - 1] * 8
    along_z = np.concatenate(
        [np.tile(turned[iz * length_z : (iz + 1) * length_z], (8, 1)) for iz in full]
        + [np.tile(turned[ends_z], (8, 1))],
        axis=0,
    )
    ends = [2 * REACH * length_x, length_x - 1] * 4
    inner = [ix * length_x + half + (-r) % 8 for ix in full for half in (0, 8) for r in range(8)]
    along_x = np.concatenate(
        [words_x[:, inner], words_x[:, ends]]
        + [np.zeros((128, 8))],
        axis=1,
    )
    return plane, lines, columns, along_x, along_z


def split(value):
    high = value.astype(BF16)
    low = (value - high.astype(F32)).astype(BF16)
    return high, low


def dot3(left, right, dims):
    def one(a, b):
        return lax.dot_general(a, b, (dims, ((), ())), preferred_element_type=F32)

    return one(left[0], right[0]) + (one(left[0], right[1]) + one(left[1], right[0]))


NN = ((1,), (0,))
NT = ((1,), (1,))
TN = ((0,), (0,))
DIRS = ((1, 1), (1, -1), (-1, 1), (-1, -1))


def lagrange_rows(coord):
    points = np.array(GLL_NODES)
    scale = 1.0 / np.prod(points[:, None] - points[None, :] + np.eye(8), axis=1)
    shape = (8, coord.shape[1])
    node = lax.broadcasted_iota(jnp.int32, shape, 0)
    total = jnp.zeros(shape, F32)
    for a in range(8):
        total = jnp.where(node == a, F32(scale[a]), total)
    for b in range(8):
        total = total * jnp.where(node == b, F32(1.0), coord - F32(points[b]))
    return total


def kernel(
    n_wall,
    n_span,
    sizes,
    vel_in,
    heights_in,
    owner_in,
    element_in,
    coords_in,
    roughness_in,
    plane_in,
    lines_in,
    columns_in,
    along_x_in,
    along_z_in,
    field,
    factors,
    neumann,
    vel,
    heights,
    owner,
    element,
    coords,
    roughness,
    sheet,
    lines,
    columns,
    along_x,
    along_z,
    load_sem,
    near,
    near_got,
    face_send,
    face_got,
    parts,
    sum_send,
    wall_got,
    span_got,
    pull_send,
    edge_send,
    pull_got,
    everything,
    sent,
    near_rs,
    pull_rs,
    face_rs,
    wall_rs,
    step_one,
    step_two,
    *span_rs,
):
    length_x, length_z, length_y = sizes
    rows = length_x * length_z
    count_z, count_y = length_z // 8, length_y // 8
    w = lax.axis_index("wall")
    s = lax.axis_index("span")

    def turned(place, count):
        return place & (count - 1) if count & (count - 1) == 0 else lax.rem(place, count)

    def at(dx, dz):
        return (turned(w + (dx + n_wall), n_wall), turned(s + (dz + n_span), n_span))

    pltpu.make_async_copy(vel_in, vel, load_sem.at[0]).start()
    single = n_wall * n_span <= SINGLE_STAGE
    stepwise = single and 3 <= n_wall <= 4 * REACH and 3 <= n_span <= 4 * REACH
    across_wall = ((1, 0), (-1, 0))
    if stepwise:
        greeted = across_wall + tuple((0, k) for k in range(1, n_span))
    elif single:
        greeted = [divmod(k, n_span) for k in range(1, n_wall * n_span)]
    else:
        greeted = [(k, 0) for k in range(1, n_wall)] + [(0, k) for k in range(1, n_span)]
        greeted += sorted(
            {
                ((dx + n_wall) % n_wall, (dz + n_span) % n_span)
                for dx in range(-REACH, REACH + 1)
                for dz in range(-REACH, REACH + 1)
            }
            - {(0, 0)}
            - set(greeted)
        )
    barrier = pltpu.get_barrier_semaphore()

    def greet(semaphore, places):
        for dx, dz in places:
            pl.semaphore_signal(semaphore, inc=1, device_id=at(dx, dz), device_id_type=MESH)

    greet(barrier, greeted)

    edges = 2 * (length_x + length_z)
    early, late = pl.ds(0, 2 * rows + edges), pl.ds(2 * rows + edges, 2 * rows)

    def column(index):
        first = index * rows + (edges if index > 1 else 0)
        return columns[first : first + rows, :]

    loads = {
        "vel": [(vel_in, vel)],
        "heights": [(heights_in, heights)],
        "operator": [
            (lines_in, lines),
            (columns_in.at[early], columns.at[early]),
            (plane_in, sheet),
        ],
        "coords": [(coords_in, coords)],
        "points": [(owner_in, owner), (element_in, element), (roughness_in, roughness)],
        "words": [
            (along_x_in, along_x),
            (along_z_in, along_z),
            (columns_in.at[late], columns.at[late]),
        ],
    }
    for index, group in list(enumerate(loads.values()))[1:]:
        for source, target in group:
            pltpu.make_async_copy(source, target, load_sem.at[index]).start()

    def loaded(*names):
        for name in names:
            index, group = list(loads).index(name), loads[name]
            whole = group[0][1]
            if len(group) > 1:
                size = sum(math.prod(ref.shape) * ref.dtype.itemsize for _, ref in group)
                whole = everything.at[pl.ds(0, size // (4 * length_y)), :]
            pltpu.make_async_copy(whole, whole, load_sem.at[index]).wait()

    loaded("vel")
    lane = lax.broadcasted_iota(jnp.int32, (64, length_y), 1)
    groups = (length_x // 8) * count_z
    depth = 8 * NEAR
    strips = length_y // depth
    packed = [jnp.zeros((64, length_y), F32)] * 2
    for index, comp in enumerate((0, 2)):
        for group in range(groups):
            ex, ez = group // count_z, group % count_z
            block = vel[comp, pl.ds(ex * 8, 8), pl.ds(ez * 8, 8), :].reshape(64, length_y)
            place = index * groups + group
            moved = pltpu.roll(block, place * depth, 1) if place else block
            for wall_side in range(2):
                strip = (place - wall_side) % strips
                packed[wall_side] = jnp.where(lane // depth == strip, moved, packed[wall_side])
    for wall_side in range(2):
        near[wall_side] = packed[wall_side]
    def remote(src, dst, ss, rs, where):
        return pltpu.make_async_remote_copy(
            src_ref=src,
            dst_ref=dst,
            send_sem=ss,
            recv_sem=rs,
            device_id=where,
            device_id_type=MESH,
        )

    near_copies = []
    for wall_side in range(2):
        for slot, dx in enumerate((1, -1)):
            target = near_got.at[wall_side, slot]
            near_copies.append(
                remote(near.at[wall_side], target, sent, near_rs.at[wall_side], at(dx, 0))
            )

    def enter():
        pl.semaphore_wait(barrier, len(greeted))
        if stepwise:
            greet(step_one, across_wall)
        for copy in near_copies:
            copy.start()

    if stepwise:
        enter()
    loaded("heights", "operator")

    layer_of = lax.broadcasted_iota(jnp.int32, (length_y, count_y), 0) // 8
    layer = lax.broadcasted_iota(jnp.int32, (length_y, count_y), 1)
    height_row = heights[...]
    height = jnp.sum(jnp.where(layer_of == layer, height_row, 0.0), axis=1, keepdims=True)
    lines_mass = height * lines[0]
    lines_stiff = lines[1] / height
    stiff_hi, stiff_lo = split(lines_stiff)
    lines_packed = jnp.concatenate(
        [
            jnp.concatenate([stiff_hi, stiff_lo], axis=1),
            jnp.concatenate([stiff_hi, jnp.zeros_like(stiff_lo)], axis=1),
        ],
        axis=0,
    )
    bound = jnp.max(0.1535 * height_row + 0.000182 / height_row, axis=1, keepdims=True)
    shifts = (0.15 * bound, 0.85 * bound)

    mass_row = jnp.sum(lines_mass, axis=0, keepdims=True)
    scale = column(0) * mass_row
    for c in range(3):
        field[0, c] = vel[c].reshape(rows, length_y) * scale

    face_rows = []
    for slot, (dx, dz) in enumerate(DIRS + ((0, 1), (0, -1), (1, 0), (-1, 0))):
        size = 3 * (1 if dx and dz else length_z if dx else length_x)
        face_rows.append((sum(entry[1] for entry in face_rows), size, dx, dz))
    face_total = sum(entry[1] for entry in face_rows)
    z_first = {entry[3]: entry[0] for entry in face_rows if entry[2] == 0}

    def corner(dx, dz):
        return (rows - length_z if dx == 1 else 0) + (length_z - 1 if dz == 1 else 0)

    def face_part(slot, c, dx, dz):
        first, size = face_rows[slot][0] + c * (face_rows[slot][1] // 3), face_rows[slot][1] // 3
        if dx and dz:
            rows_of = pl.ds(corner(dx, dz), 1)
        elif dx:
            rows_of = pl.ds(rows - length_z if dx == 1 else 0, length_z)
        else:
            rows_of = pl.ds(length_z - 1 if dz == 1 else 0, length_x, stride=length_z)
        return pl.ds(first, size), rows_of

    def send_faces(turn, fringe):
        for c in range(3):
            for slot, (first, size, dx, dz) in enumerate(face_rows):
                size //= 3
                if dx and dz:
                    begin = 2 * length_x + (length_z if dx == -1 else 0)
                    begin += length_z - 1 if dz == 1 else 0
                elif dx:
                    begin = 2 * length_x + (length_z if dx == -1 else 0)
                else:
                    begin = length_x if dz == -1 else 0
                rows_here = slice(first + c * size, first + (c + 1) * size)
                face_send[turn, rows_here, :] = fringe[c][begin : begin + size]
        first_turn = turn == 0 and stepwise
        if turn == 0 and not stepwise:
            enter()
        for stage in ((0,), (2, 1)) if first_turn else ((2, 0, 1),):
            if stage[0] == 2 and first_turn:
                pl.semaphore_wait(step_one, len(across_wall))
                greet(step_two, across_wall)
            for kind in stage:
                for first, size, dx, dz in face_rows:
                    if (2 if dx and dz else abs(dx)) != kind:
                        continue
                    if kind == 0:
                        swap = jnp.where(s == 0, -dz, dz)
                        first = pl.multiple_of(jnp.where(swap == 1, z_first[1], z_first[-1]), 4)
                        dz = swap
                    part = (turn, pl.ds(first, size), slice(None))
                    remote(
                        face_send.at[part],
                        face_got.at[part],
                        sent,
                        face_rs.at[turn],
                        at(dx, dz),
                    ).start()

    def settle(semaphore, ref):
        pltpu.make_async_copy(ref, ref, semaphore).wait()

    def add_faces(turn):
        settle(face_rs.at[turn], face_got.at[turn, pl.ds(0, face_total), :])
        for c in range(3):
            for slot, (_, _, dx, dz) in enumerate(face_rows):
                packed_rows, rows_of = face_part(slot, c, -dx, -dz)
                field[turn + 1, c, rows_of, :] = (
                    field[turn + 1, c, rows_of, :] + face_got[turn, packed_rows, :]
                )

    def inner(quantity, c, product):
        parts[quantity * 8 + c : quantity * 8 + c + 1, :] = jnp.sum(
            product, axis=0, keepdims=True
        )

    def operate(turn):
        highs, lows = zip(*[split(field[turn, c]) for c in range(3)])
        packed = [jnp.concatenate(pair, axis=1) for pair in zip(highs, lows)]
        wide = jnp.concatenate(highs + lows, axis=1)
        wide_high = jnp.concatenate(highs, axis=1)

        def image(first, count, lines_of, weight):
            along_y = jnp.dot(
                jnp.concatenate(lines_of, axis=0), lines_packed, preferred_element_type=F32
            )
            part = slice(first, first + count)
            across = jnp.dot(sheet[0, part], wide, preferred_element_type=F32)
            across_low = jnp.dot(sheet[1, part], wide_high, preferred_element_type=F32)
            results = []
            for c in range(3):
                here = slice(c * length_y, (c + 1) * length_y)
                also = slice((3 + c) * length_y, (4 + c) * length_y)
                flat = across[:, here] + (across[:, also] + across_low[:, here])
                tall = along_y[c * count : (c + 1) * count]
                tall = tall[:, :length_y] + tall[:, length_y:]
                results.append(flat * mass_row + tall * weight)
            return results

        lines_of = []
        for c in range(3):
            value = jnp.concatenate(
                [
                    field[turn, c, pl.ds(length_z - 1, length_x, stride=length_z), :],
                    field[turn, c, pl.ds(0, length_x, stride=length_z), :],
                    field[turn, c, pl.ds(rows - length_z, length_z), :],
                    field[turn, c, pl.ds(0, length_z), :],
                ],
                axis=0,
            )
            lines_of.append(jnp.concatenate(split(value), axis=1))
        weight = columns[2 * rows : 2 * rows + edges, :]
        send_faces(turn, image(rows, edges, lines_of, weight))
        for c, value in enumerate(image(0, rows, packed, column(1))):
            field[turn + 1, c] = value

    slots = {(0, 0): 0, (0, 1): 1, (1, 1): 2, (0, 2): 3, (1, 2): 4, (2, 2): 5}

    def inner_products(newest):
        for c in range(3):
            weighted = field[newest, c] * column(2)
            for other in range(newest + 1):
                inner(slots[(other, newest)], c, weighted * field[other, c])

    operate(0)
    parts[...] = jnp.zeros_like(parts)

    loaded("coords", "points")
    points = owner.shape[1]
    row_x = lagrange_rows(coords[0:1, :])
    row_z = lagrange_rows(coords[1:2, :])
    row_y = lagrange_rows(coords[2:3, :])
    cross = jnp.concatenate([row_x[a : a + 1] * row_z for a in range(8)], axis=0)
    distance = lax.rem(owner[...] - w + n_wall, n_wall)
    from_next = distance == 1
    from_prev = distance == n_wall - 1
    own = jnp.logical_not(jnp.logical_or(from_next, from_prev))
    spread = jnp.concatenate(
        [jnp.where(mask, cross, 0.0) for mask in (own, from_prev, from_next)], axis=0
    )
    half = points // 2
    n_row = lax.broadcasted_iota(jnp.int32, (groups * depth, points), 0)
    side_of = lax.broadcasted_iota(jnp.int32, (groups * depth, points), 1) // half
    layer_y = (n_row % depth) // 8 + side_of * (count_y - NEAR)
    wanted = (n_row // depth) * count_y + layer_y == element[...]
    along = jnp.where(wanted, jnp.concatenate([row_y] * (groups * NEAR), axis=0), 0.0)
    spread = split(spread)
    drag = karman / jnp.log(sample_height / roughness[...])
    drag = drag * drag * (-1.0 / viscosity)

    sampled = []
    for wall_side in range(2):
        settle(near_rs.at[wall_side], near_got.at[wall_side])
        sources = jnp.concatenate(
            [near[wall_side], near_got[wall_side, 0], near_got[wall_side, 1]], axis=0
        )
        here = slice(wall_side * half, (wall_side + 1) * half)
        values = dot3(split(sources), tuple(part[:, here] for part in spread), TN)
        total = []
        for index in range(2):
            strip_rows = [
                (place - wall_side) % strips * depth
                for place in range(index * groups, (index + 1) * groups)
            ]
            own_rows = jnp.concatenate([values[k : k + depth] for k in strip_rows], axis=0)
            total.append(jnp.sum(own_rows * along[:, here], axis=0, keepdims=True))
        sampled.append(total)
    stream, spanwise = [jnp.concatenate(both, axis=1) for both in zip(*sampled)]
    speed = jnp.sqrt(stream * stream + spanwise * spanwise + speed_floor)
    factor = drag * speed
    gradient = (factor * stream, factor * spanwise)
    neumann[0:1, :] = gradient[0]
    neumann[1:2, :] = gradient[1]

    planes = []
    for index in range(2):
        pull = viscosity * gradient[index]
        planes += [pull[:, :rows], pull[:, rows:]]
    tiles = 4 * length_x // 8
    tile_lane = lax.broadcasted_iota(jnp.int32, (8, 128), 1)
    tile_row = lax.broadcasted_iota(jnp.int32, (8, 128), 0)
    block_of = tile_lane // length_z
    bundle = jnp.zeros((8, 128), F32)
    fringe = jnp.zeros((8, 128), F32)
    for tile in range(tiles):
        part = planes[tile // 2][:, 128 * (tile % 2) : 128 * (tile % 2) + 128]
        part = jnp.broadcast_to(part, (8, 128))
        spread_rows = pltpu.roll(part, 0, 1, stride=length_z, stride_axis=0)
        spread_rows = pltpu.roll(spread_rows, (8 - tile) % 8, 0)
        bundle = jnp.where(block_of == tile, spread_rows, bundle)
        for end in range(2):
            slanted = pltpu.roll(part, 7 * (1 - end), 1, stride=length_z - 1, stride_axis=0)
            wanted_lane = tile * length_z + 8 * end + 7 - tile_row
            fringe = jnp.where(tile_lane == wanted_lane, slanted, fringe)
    pull_send[...] = bundle
    edge_send[0:1, :] = jnp.sum(fringe, axis=0, keepdims=True)
    edge_send[1:2, :] = jnp.where(block_of[0:1] % 2 == 0, bundle[0:1], bundle[1:2])
    if stepwise:
        pl.semaphore_wait(step_two, len(across_wall))
    reach = 2 * REACH + 1
    offsets = [
        (dx, dz)
        for dx in range(-REACH, REACH + 1)
        for dz in range(-REACH, REACH + 1)
        if (dx, dz) != (0, 0)
    ]
    nearby = [place for place in offsets if max(abs(place[0]), abs(place[1])) < REACH]
    remaining = [place for place in offsets if place not in nearby]
    pull_rows = {place: pl.ds(8 * index, 8) for index, place in enumerate(nearby)}
    for index, place in enumerate(remaining):
        pull_rows[place] = pl.ds(8 * len(nearby) + index, 1)
    for dx, dz in sorted(offsets, key=lambda pair: -abs(pair[0]) - abs(pair[1])):
        if (dx, dz) in nearby:
            source = pull_send
        else:
            source = edge_send.at[pl.ds(0 if abs(dz) == REACH else 1, 1), :]
        remote(
            source, pull_got.at[pull_rows[(-dx, -dz)], :], sent, pull_rs, at(dx, dz)
        ).start()

    add_faces(0)
    operate(1)
    loaded("words")
    lines_rows = jnp.concatenate([lines_mass, lines_stiff], axis=1)
    ends = [lines_rows[0:1], lines_rows[length_y - 1 : length_y]]
    once = [(end[:, :length_y], end[:, length_y:]) for end in ends]
    twice = dot3(
        split(jnp.concatenate([once[0][0], once[0][1], once[1][0], once[1][1]] * 2, axis=0)),
        split(lines_rows),
        NN,
    )
    one_lane = lax.broadcasted_iota(jnp.int32, (1, length_y), 1)
    zero = jnp.zeros((1, length_y), F32)
    images = []
    for side in range(2):
        by_mass, by_stiff = twice[2 * side : 2 * side + 1], twice[2 * side + 1 : 2 * side + 2]
        moved_tip = jnp.where(one_lane == length_y // 2 - side, 1.0, 0.0)
        rows_of = [
            (zero, moved_tip),
            (zero, once[side][0]),
            (zero, once[side][1]),
            (by_mass[:, :length_y], zero),
            (by_stiff[:, :length_y], zero),
            (by_mass[:, length_y:], zero),
            (by_stiff[:, length_y:], zero),
        ]
        for entry in rows_of:
            image = jnp.concatenate(entry, axis=1)
            images.append(jnp.broadcast_to(image, (length_z, 2 * length_y)))
        images.append(jnp.zeros((128 - 7 * length_z, 2 * length_y), F32))
    images = split(jnp.concatenate(images, axis=0))
    low_half = tile_lane & 8 == 0
    low_rows = tile_row & 1 == 0
    diagonal_of = (tile_lane + tile_row) & 7

    def halves(value):
        return split(value)

    def both_tiles(pair, mask_of):
        masks = [jnp.where(mask_of(tile), 1.0, 0.0) for tile in (2 * pair, 2 * pair + 1)]
        return jnp.concatenate(masks, axis=0).astype(BF16)

    block_masks = [both_tiles(pair, lambda tile: block_of == tile) for pair in range(tiles // 2)]
    end_masks = [
        both_tiles(
            pair,
            lambda tile: jnp.logical_and(block_of == tile, diagonal_of == (7 - tile) % 8),
        )
        for pair in range(tiles // 2)
    ]
    settle(pull_rs, pull_got)

    def edge(dx, dz):
        return jnp.broadcast_to(pull_got[pull_rows[(dx, dz)], :], (8, 128))

    def both_ends(dx):
        return jnp.where(low_half, edge(dx, REACH), edge(dx, -REACH))

    middle = range(-REACH + 1, REACH)

    def doubled(part):
        return [jnp.concatenate([half, half], axis=0) for half in (part[0], part[1])]

    spans = ([], [])
    for dx in middle:
        parts_z = [bundle if (dx, dz) == (0, 0) else pull_got[pull_rows[(dx, dz)], :] for dz in middle]
        pairs = [doubled(halves(part)) for part in parts_z]
        ends = doubled(halves(both_ends(dx)))
        for pair in range(tiles // 2):
            for out, which in zip(spans, range(2)):
                pieces = [part[which] * block_masks[pair] for part in pairs]
                pieces.append(ends[which] * end_masks[pair])
                out.append(jnp.concatenate(pieces, axis=1))
    pieces = [
        jnp.where(block_of == tile_row, jnp.where(low_rows, edge(REACH, dz), edge(-REACH, dz)), 0.0)
        for dz in middle
    ]
    kept = jnp.logical_and(
        block_of == tile_row, (tile_lane + tile_row + (tile_row & 1)) & 7 == 7
    )
    ends = jnp.where(low_rows, both_ends(REACH), both_ends(-REACH))
    pieces.append(jnp.where(kept, ends, 0.0))
    last = jnp.concatenate([jnp.concatenate(pieces, axis=1), jnp.zeros((8, 512), F32)], axis=0)
    for out, half in zip(spans, split(last)):
        out.append(half)
    spans_hi, spans_lo = [jnp.concatenate(out, axis=0) for out in spans]
    reached = jnp.dot(spans_hi, along_z[...], preferred_element_type=F32)
    reached = (reached[:, :128] + reached[:, 128:]) + jnp.dot(
        spans_lo, along_z[:, :128], preferred_element_type=F32
    )
    by_plane = []
    for plane in range(4):
        kept = [
            reached[ix * 64 + plane * length_x : ix * 64 + (plane + 1) * length_x]
            for ix in range(len(middle))
        ]
        last = reached[64 * len(middle) : 64 * len(middle) + 8]
        kept.append(jnp.where(tile_row // 2 == plane, last, 0.0))
        kept.append(jnp.zeros((8, 128), F32))
        by_plane.append(jnp.concatenate(kept, axis=0))
    stacked_hi, stacked_lo = split(jnp.concatenate(by_plane, axis=1))
    both_ways = jnp.dot(
        along_x[:, : 3 * stacked_hi.shape[0]],
        jnp.concatenate([stacked_hi, stacked_lo, stacked_hi], axis=0),
        preferred_element_type=F32,
    )
    block_lane = lax.broadcasted_iota(jnp.int32, (length_x, 128), 1) // length_z
    keep_row = lax.rem(lax.broadcasted_iota(jnp.int32, (rows, 256), 0), length_z)
    keep_lane = lax.rem(lax.broadcasted_iota(jnp.int32, (rows, 256), 1), length_z)
    wall_lane = lax.broadcasted_iota(jnp.int32, (rows, length_y), 1)
    tractions = []
    for index in range(2):
        blocks = []
        for side in range(2):
            plane = index * 2 + side
            total = jnp.zeros((length_x, 128), F32)
            for block, word_x, word_z in TERMS:
                piece = both_ways[
                    word_x * length_x : (word_x + 1) * length_x, plane * 128 : plane * 128 + 128
                ]
                shift = ((block - word_z) * length_z) % 128
                moved = pltpu.roll(piece, shift, 1) if shift else piece
                total = total + jnp.where(block_lane == block, moved, 0.0)
            blocks.append(total)
        wide = jnp.concatenate(blocks, axis=1)
        tall = jnp.concatenate(
            [jnp.broadcast_to(wide[x : x + 1], (length_z, 256)) for x in range(length_x)], axis=0
        )
        tall = jnp.where(keep_row == keep_lane, tall, 0.0)
        deep = dot3(split(tall), images, NN)
        level_two, shallow = deep[:, :length_y], deep[:, length_y:]
        tip = jnp.logical_or(wall_lane == 0, wall_lane == length_y - 1)
        level_zero = jnp.where(tip, pltpu.roll(shallow, length_y // 2, 1), 0.0)
        outside = jnp.logical_or(wall_lane < length_y // 4, wall_lane >= 3 * length_y // 4)
        level_one = jnp.where(outside, shallow, 0.0)
        tractions.append((level_zero, level_one, level_two))
    t1, t2 = shifts
    for c in range(3):
        chain = [field[level, c] for level in range(3)]
        if c != 1:
            taus = tractions[c // 2]
            chain = [chain[level] + taus[level] for level in range(3)]
        v1 = chain[1] - t1 * chain[0]
        field[0, c] = chain[0]
        field[1, c] = v1
        field[2, c] = chain[2] - t1 * chain[1] - t2 * v1
    for newest in range(2):
        inner_products(newest)
    add_faces(1)
    highs = [field[2, c].astype(BF16) for c in range(3)]
    along_y = jnp.dot(
        jnp.concatenate(highs, axis=0), lines_packed[:length_y], preferred_element_type=F32
    )
    wide = jnp.concatenate(highs, axis=1)
    across = jnp.dot(sheet[0, :rows], wide, preferred_element_type=F32)
    across_low = jnp.dot(sheet[1, :rows], wide, preferred_element_type=F32)
    inner_products(2)
    for c in range(3):
        here = slice(c * length_y, (c + 1) * length_y)
        tall = along_y[c * rows : (c + 1) * rows]
        tall = tall[:, :length_y] + tall[:, length_y:]
        image = (across[:, here] + across_low[:, here]) * mass_row + tall * column(1)
        value = field[2, c]
        partner = value + (value - highs[c].astype(F32))
        inner(6, c, partner * column(3) * image)

    total_rows = parts.shape[0]
    r_iota = lax.broadcasted_iota(jnp.int32, (total_rows, 128), 0)
    l_iota = lax.broadcasted_iota(jnp.int32, (total_rows, 128), 1)
    diagonal = r_iota == l_iota
    end_lane = lax.broadcasted_iota(jnp.int32, (total_rows, 128), 1)
    shared = jnp.logical_or(end_lane % 8 == 0, end_lane % 8 == 7)
    tips = jnp.logical_or(end_lane == 0, end_lane == length_y - 1)
    weight_y = jnp.where(jnp.logical_and(shared, jnp.logical_not(tips)), 0.5, 1.0)
    summed = jnp.sum(parts[...] * weight_y, axis=1, keepdims=True)
    row = jnp.sum(jnp.where(diagonal, summed, 0.0), axis=0, keepdims=True)

    def gather_sum(stage, row, count, got, rs, place):
        sum_send[stage : stage + 1, :] = row
        def ring(place, size):
            return min(place % size, -place % size)

        def reach_of(k):
            if count != n_wall * n_span:
                return ring(k, count)
            return ring(k // n_span, n_wall) + ring(k % n_span, n_span)

        for k in sorted(range(1, count), key=reach_of, reverse=True):
            remote(
                sum_send.at[pl.ds(stage, 1), :], got.at[pl.ds(k - 1, 1), :], sent, rs, place(k)
            ).start()
        settle(rs, got)
        return row + jnp.sum(got[...], axis=0, keepdims=True)

    sum_rows = 0
    if single:
        every = n_wall * n_span
        row = gather_sum(0, row, every, wall_got, wall_rs, lambda k: at(k // n_span, k % n_span))
        sum_rows = every - 1
    else:
        row = gather_sum(0, row, n_wall, wall_got, wall_rs, lambda k: at(k, 0))
        row = gather_sum(1, row, n_span, span_got, span_rs[0], lambda k: at(0, k))
        sum_rows = n_wall + n_span - 2
    sent_rows = 2 * 2 * 64 + pull_got.shape[0] + ROUNDS * face_total + sum_rows
    settle(sent, everything.at[pl.ds(0, sent_rows), :])
    totals = jnp.sum(jnp.where(diagonal, row, 0.0), axis=1, keepdims=True)
    m00, m01, m11, m02, m12, m22, e22 = [totals[q * 8 : q * 8 + 8, :] for q in range(7)]
    t1, t2 = shifts
    a00 = m01 + t1 * m00
    a01 = m11 + t1 * m01
    a02 = m12 + t1 * m02
    a11 = m12 + t2 * m11
    a12 = m22 + t2 * m12
    l10 = a01 / a00
    l20 = a02 / a00
    d1 = a11 - l10 * a01
    u12 = a12 - l10 * a02
    l21 = u12 / d1
    d2 = e22 - l20 * a02 - l21 * u12
    y1 = m01 - l10 * m00
    y2 = m02 - l20 * m00 - l21 * y1
    x2 = y2 / d2
    x1 = y1 / d1 - l21 * x2
    x0 = m00 / a00 - l10 * x1 - l20 * x2
    for index, value in enumerate((x0, x1, x2)):
        factors[index] = jnp.broadcast_to(value, (8, 128))


def combine(field, factors, neumann_in, out, neumann, stage, sems):
    small = pltpu.make_async_copy(neumann_in, neumann, sems.at[1])
    small.start()
    length_x, length_z, length_y = stage.shape[1:]
    half = length_x // 2
    for c in range(3):
        for first in (0, half):
            here = slice(first * length_z, (first + half) * length_z)
            result = factors[0, c : c + 1] * field[0, c, here]
            for level in range(1, 3):
                result += factors[level, c : c + 1] * field[level, c, here]
            stage[c, first : first + half] = result.reshape(half, length_z, length_y)
            part = (c, pl.ds(first, half))
            pltpu.make_async_copy(stage.at[part], out.at[part], sems.at[0]).start()
    pltpu.make_async_copy(stage, out, sems.at[0]).wait()
    small.wait()


def body(n_wall, n_span, velocity_old, heights, owner_device, owner_element, ref_coords, roughness):
    sizes = velocity_old.shape[1:]
    length_x, length_z, length_y = sizes
    rows = length_x * length_z
    points = owner_device.shape[0]
    plane, lines, columns, along_x, along_z = tables(*sizes)
    along_x_hi, along_x_lo = split_np(along_x)
    every = n_wall * n_span
    first = every if every <= SINGLE_STAGE else n_wall
    faces = -(-(6 * (length_x + length_z) + 12) // 8) * 8
    vmem = pl.BlockSpec(memory_space=pltpu.VMEM)
    hbm = pl.BlockSpec(memory_space=pltpu.HBM)
    operands = (
        velocity_old,
        heights.reshape(1, -1),
        owner_device.reshape(1, -1),
        owner_element.reshape(1, -1),
        ref_coords,
        roughness.reshape(1, -1),
        jnp.stack(split_np(plane)),
        jnp.asarray(lines, F32),
        jnp.asarray(columns, F32),
        jnp.pad(jnp.concatenate([along_x_hi, along_x_hi, along_x_lo], axis=1), ((0, 0), (0, 64))),
        jnp.concatenate(split_np(along_z), axis=1),
    )
    dma = pltpu.SemaphoreType.DMA
    field, factors, neumann = pl.pallas_call(
        functools.partial(kernel, n_wall, n_span, sizes),
        out_shape=(
            pltpu.VMEM((3, 3, rows, length_y), F32),
            pltpu.VMEM((3, 8, 128), F32),
            pltpu.VMEM((2, points), F32),
        ),
        in_specs=[hbm] * 11,
        out_specs=(vmem, vmem, vmem),
        scratch_shapes=[pltpu.VMEM(value.shape, value.dtype) for value in operands]
        + [
            dma((6,)),
            pltpu.VMEM((2, 64, length_y), F32),
            pltpu.VMEM((2, 2, 64, length_y), F32),
            pltpu.VMEM((ROUNDS, faces, length_y), F32),
            pltpu.VMEM((ROUNDS, faces, length_y), F32),
            pltpu.VMEM((56, length_y), F32),
            pltpu.VMEM((2, 128), F32),
            pltpu.VMEM((first - 1, 128), F32),
            pltpu.VMEM((n_span - 1, 128), F32),
            pltpu.VMEM((8, 128), F32),
            pltpu.VMEM((8, 128), F32),
            pltpu.VMEM((80, 128), F32),
            pltpu.VMEM((1536, length_y), F32),
            dma,
            dma((2,)),
            dma,
            dma((ROUNDS,)),
            dma,
            pltpu.SemaphoreType.REGULAR,
            pltpu.SemaphoreType.REGULAR,
        ]
        + ([] if every <= SINGLE_STAGE else [dma]),
        compiler_params=pltpu.CompilerParams(
            collective_id=0, has_side_effects=True, vmem_limit_bytes=VMEM_LIMIT
        ),
    )(*[pltpu.with_memory_space_constraint(value, pltpu.HBM) for value in operands])
    return pl.pallas_call(
        combine,
        out_shape=(
            jax.ShapeDtypeStruct(velocity_old.shape, F32),
            jax.ShapeDtypeStruct((2, points), F32),
        ),
        in_specs=[vmem] * 3,
        out_specs=(hbm, hbm),
        scratch_shapes=[pltpu.VMEM(velocity_old.shape, F32), dma((2,))],
        compiler_params=pltpu.CompilerParams(vmem_limit_bytes=VMEM_LIMIT),
    )(field, factors, neumann)


def solution(mesh):
    placed = (
        P(None, "wall", "span", None),
        P(),
        P(("wall", "span"), None),
        P(("wall", "span"), None),
        P(None, ("wall", "span")),
        P(("wall", "span")),
    )
    return jax.shard_map(
        functools.partial(body, mesh.shape["wall"], mesh.shape["span"]),
        mesh=mesh,
        in_specs=placed,
        out_specs=(P(None, "wall", "span", None), P(None, ("wall", "span"))),
        check_vma=False,
    )
```
